256 devices in a mesh: section: 8 (over z), dp: 32 (over x, y, core).
Axes of the slice: x: 4, y: 4, z: 8, core: 2. Of those that a mesh axis runs over, the one named last changes fastest.
Arguments:
- entry: bfloat16 [6144, 3584], P('dp'), may hold values from -6 to 6
- norm_gain: float32 [8, 3584], P('section'), may hold values from 0.5 to 1.5
- w_qkv: bfloat16 [8, 3584, 1152], P('section', 'dp'), may hold values from -0.09375 to 0.09375
- w_out: bfloat16 [8, 896, 3584], P('section', 'dp'), may hold values from -0.1875 to 0.1875
- final_gain: float32 [3584], replicated, may hold values from 0.5 to 1.5
- lengths: int32 [128], P('dp'), may hold values from 24 to 48
- positive: int32 [64], P('dp'), may hold values from 0 to 63, each once
Outputs:
- section_grads: bfloat16 [8, 6144, 3584], P('section', 'dp')
The draws below stay inside these ranges and needn't reach their ends.
Inputs may be any that keep to these rules, and one draw needn't show every extreme that they name: lengths[j] is the count of tokens of sequence j; its last token is pooled. Each document index is the positive of exactly one query.
All inputs are finite; a program needn't handle non-finite values.
Results may differ from the reference program's by a relative error of at most 0.022.
Values may be sent and summed in bfloat16 or wider, within the bound.
A program may use at most 192 MiB of HBM per device.

```python
import jax
import jax.numpy as jnp
from jax import lax

D = 3584
HEAD_DIM = 64
GROUP_HEADS = 7
KV_GROUPS = 2
LEN = 48
QW = 896
QUERIES = 64
SEQS = 128
TOKENS = 6144
N_SECTION = 8


def place_ends(values, rng, smallest, high):
    index_at = [jax.random.randint(jax.random.fold_in(rng, axis), (), 0, length) for axis, length in enumerate(values.shape)]
    main_axis = values.shape.index(max(values.shape))
    next_to = index_at[:main_axis] + [(index_at[main_axis] + 1) % values.shape[main_axis]] + index_at[main_axis + 1:]
    return values.at[tuple(index_at)].set(smallest).at[tuple(next_to)].set(high)


def shard_levels(rng, dims, shards, smallest, high):
    def one(axis_at, shards_of):
        steps = jax.random.uniform(jax.random.fold_in(jax.random.fold_in(rng, 6), axis_at), (shards_of,), jnp.float32, smallest / len(shards), high / len(shards))
        return jnp.repeat(jnp.exp(steps), dims[axis_at] // shards_of).reshape((-1,) + (1,) * (len(dims) - axis_at - 1))

    level = one(*shards[0])
    for cut in shards[1:]:
        level = level * one(*cut)
    return level


def noise(rng, dims, deviation, reach, shards=(), kind=jnp.bfloat16):
    drawn = jax.random.normal(rng, dims, jnp.float32) * deviation
    if len(shards) > 0:
        drawn = shard_levels(rng, dims, shards, -0.22, 0.18) * drawn
    return jnp.clip(drawn, min=-reach, max=reach).astype(kind)


def setup_inputs(seed: int = 0) -> dict:
    arg_keys = jax.random.split(jax.random.key(seed), 8)
    return {
        "entry": noise(arg_keys[0], (TOKENS, D), 1.0, 6.0, ((0, 32),)),
        "norm_gain": jnp.clip(1.0 + 0.1 * jax.random.normal(arg_keys[1], (N_SECTION, D), jnp.float32), 0.5, 1.5),
        "w_qkv": noise(arg_keys[2], (N_SECTION, D, QW + 2 * KV_GROUPS * HEAD_DIM), D ** -0.5, 0.09375, ((0, 8), (1, 32))),
        "w_out": noise(arg_keys[3], (N_SECTION, QW, D), QW ** -0.5, 0.1875, ((0, 8), (1, 32))),
        "final_gain": jnp.clip(1.0 + 0.1 * jax.random.normal(arg_keys[4], (D,), jnp.float32), 0.5, 1.5),
        "lengths": place_ends(jax.random.randint(arg_keys[5], (SEQS,), LEN // 2, LEN + 1), jax.random.fold_in(arg_keys[5], 1), LEN // 2, LEN).astype(jnp.int32),
        "positive": jax.random.permutation(arg_keys[6], QUERIES).astype(jnp.int32),
    }


rope_base = 1000000.0
norm_eps = 1e-06
sharpness_divisor = 0.05
objective_coefficient = 256.0

def rotary(values, positions):
    half_dim = values.shape[-1] // 2
    frequency = rope_base ** (-jnp.arange(half_dim, dtype=jnp.float32) * (2.0 / values.shape[-1]))
    angles = positions.astype(jnp.float32)[:, None] * frequency[None, :]
    cosine = jnp.cos(angles)[:, None, :]
    sine_part = jnp.sin(angles)[:, None, :]
    first_half = values[..., :half_dim]
    second_half = values[..., half_dim:]
    return jnp.concatenate([first_half * cosine - second_half * sine_part, second_half * cosine + first_half * sine_part], axis=-1)

def rms_scale(values, gain_row):
    return values * lax.rsqrt(lax.optimization_barrier(jnp.mean(values * values, axis=-1, keepdims=True)) + norm_eps) * gain_row

def attention_layer(hidden, seq_lengths, gain_row, weight_qkv, weight_out):
    row_count, row_width = hidden.shape
    seq_count = seq_lengths.shape[0]
    length = row_count // seq_count
    q_width = weight_out.shape[0]
    kv_width = KV_GROUPS * HEAD_DIM
    wide_in = hidden.astype(jnp.float32)
    normed = rms_scale(wide_in, gain_row).astype(jnp.bfloat16)
    projected = jnp.dot(normed, weight_qkv, preferred_element_type=jnp.float32)
    positions = jnp.arange(length, dtype=jnp.int32)
    query_rot = rotary(projected[:, :q_width].reshape(seq_count, length, KV_GROUPS * GROUP_HEADS, HEAD_DIM), positions).astype(jnp.bfloat16)
    key_rot = rotary(projected[:, q_width:q_width + kv_width].reshape(seq_count, length, KV_GROUPS, HEAD_DIM), positions).astype(jnp.bfloat16)
    value_rows = projected[:, q_width + kv_width:].reshape(seq_count, length, KV_GROUPS, HEAD_DIM).astype(jnp.bfloat16)
    query_grid = query_rot.reshape(seq_count, length, KV_GROUPS, GROUP_HEADS, HEAD_DIM)
    scores = jnp.einsum('sqgzd,skgd->sgzqk', query_grid.astype(jnp.float32), key_rot.astype(jnp.float32)) * HEAD_DIM ** (-0.5)
    key_live = positions[None, :] < seq_lengths[:, None]
    weights = jnp.where(key_live[:, None, None, None, :], jnp.exp(scores), 0.0)
    prob_low = (weights / lax.optimization_barrier(jnp.sum(weights, axis=-1, keepdims=True))).astype(jnp.bfloat16)
    context = jnp.einsum('sgzqk,skgd->sqgzd', prob_low.astype(jnp.float32), value_rows.astype(jnp.float32)).astype(jnp.bfloat16)
    branch = jnp.dot(context.reshape(row_count, q_width), weight_out, preferred_element_type=jnp.float32)
    return (wide_in + branch).astype(jnp.bfloat16)

def embed_rows(rows_in, final_gain):
    pooled = rms_scale(rows_in.astype(jnp.float32), final_gain)
    return pooled * lax.rsqrt(lax.optimization_barrier(jnp.sum(pooled * pooled, axis=-1, keepdims=True)))

def pair_terms(question_representation, passage_representation, positive):
    match_raw_scores = jnp.dot(question_representation, passage_representation.T, preferred_element_type=jnp.float32) * (1.0 / sharpness_divisor)
    weights = jnp.exp(match_raw_scores)
    normalized_exponential_odds = weights / lax.optimization_barrier(jnp.sum(weights, axis=-1, keepdims=True))
    correct_target_column = (positive[:, None] == jnp.arange(passage_representation.shape[0], dtype=jnp.int32)[None, :]).astype(jnp.float32)
    return (normalized_exponential_odds - correct_target_column) * (objective_coefficient / sharpness_divisor)

def reference(entry, norm_gain, w_qkv, w_out, final_gain, lengths, positive):
    section_count = norm_gain.shape[0]
    seq_count = lengths.shape[0]
    length = entry.shape[0] // seq_count
    row_width = entry.shape[1]
    hidden = entry
    inputs = []
    for layer_id in range(section_count):
        inputs.append(hidden)
        hidden = attention_layer(hidden, lengths, norm_gain[layer_id], w_qkv[layer_id], w_out[layer_id])
    seq_grid = hidden.reshape(seq_count, length, row_width)
    last_rows = jnp.take_along_axis(seq_grid, (lengths - 1)[:, None, None], axis=1)[:, 0]
    embedding, back_embed = jax.vjp(lambda rows_in: embed_rows(rows_in, final_gain), last_rows)
    emb_low = embedding.astype(jnp.bfloat16)
    question_representation = emb_low[0::2]
    passage_representation = emb_low[1::2]
    pair_coef = pair_terms(question_representation, passage_representation, positive)
    grad_query = jnp.dot(pair_coef, passage_representation.astype(jnp.float32), precision=lax.Precision.HIGHEST)
    grad_doc = jnp.dot(pair_coef.T, question_representation.astype(jnp.float32), precision=lax.Precision.HIGHEST)
    grad_emb = jnp.stack([grad_query, grad_doc], axis=1).reshape(seq_count, row_width)
    grad_last = back_embed(grad_emb)[0]
    slot_hit = jnp.arange(length, dtype=jnp.int32)[None, :] == (lengths - 1)[:, None]
    seed_grad = jnp.where(slot_hit[:, :, None], grad_last[:, None, :], 0).astype(jnp.bfloat16).reshape(-1, row_width)
    cotangent = seed_grad
    collected = []
    for layer_id in reversed(range(section_count)):
        _, pull_back = jax.vjp(lambda values: attention_layer(values, lengths, norm_gain[layer_id], w_qkv[layer_id], w_out[layer_id]), inputs[layer_id])
        cotangent = pull_back(cotangent)[0]
        collected.append(cotangent)
    return jnp.stack(collected[::-1])
```

```python
import functools

import jax
import jax.numpy as jnp
from jax import lax
from jax.experimental import pallas as pl
from jax.experimental.pallas import tpu as pltpu
from jax.sharding import Mesh
from jax.sharding import PartitionSpec as P

HEAD_DIM = 64
GROUP_HEADS = 7
KV_GROUPS = 2
DP = ("dp_0", "dp_1", "dp_2")

rope_base = 1000000.0
norm_eps = 1e-06
sharpness_divisor = 0.05
objective_coefficient = 256.0

LENGTH = 48
PAIRS = 7
F32 = jnp.float32
BF16 = jnp.bfloat16


def nn(a, b):
    return lax.dot_general(a, b, (((1,), (0,)), ((), ())), preferred_element_type=F32)


def nt(a, b):
    return lax.dot_general(a, b, (((1,), (1,)), ((), ())), preferred_element_type=F32)


def tn(a, b):
    return lax.dot_general(a, b, (((0,), (0,)), ((), ())), preferred_element_type=F32)


def lanes_of(shape):
    return lax.broadcasted_iota(jnp.int32, shape, 1)


def turned(block, cosine, sine, roll):
    lane = lanes_of(block.shape)
    swapped = jnp.where(lane % 64 < 32, roll(block, 96), roll(block, 32))
    return block * cosine + swapped * sine


def paired(rows, roll):
    lane = lanes_of(rows.shape)
    other = roll(rows, 64)
    zero = jnp.zeros_like(rows)
    low = lane < 64
    first = jnp.where(low, rows, zero)
    second = jnp.where(low, zero, rows)
    return tuple(
        jnp.concatenate(two, axis=0).astype(BF16)
        for two in (
            (first, jnp.where(low, zero, other)),
            (first, second),
            (jnp.where(low, other, zero), second),
        )
    )


SPANS = ((0, 3), (3, 4), (4, 7))


def stacked(blocks, span):
    chosen = blocks[span[0] : span[1]]
    return chosen[0] if len(chosen) == 1 else jnp.concatenate(chosen, axis=0)


def layer_forward(hidden, gain, wq, wo, cosine, sine, key_mask, roll):
    wide = hidden.astype(F32)
    inverse = lax.rsqrt(jnp.mean(wide * wide, axis=-1, keepdims=True) + norm_eps)
    normed = (wide * inverse * gain).astype(BF16)
    projected = nn(normed, wq[...])
    blocks = [projected[:, 128 * b : 128 * (b + 1)] for b in range(9)]
    turned_blocks = [turned(b, cosine, sine, roll) for b in blocks[:8]]
    queries = [b.astype(BF16) for b in turned_blocks[:PAIRS]]
    keys = turned_blocks[PAIRS].astype(BF16)
    values = blocks[8].astype(BF16)
    key_forms = paired(keys.astype(F32), roll)
    value_forms = paired(values.astype(F32), roll)
    probabilities = []
    context = []
    for span, key_form, value_form in zip(SPANS, key_forms, value_forms):
        scores = nt(stacked(queries, span), key_form) * HEAD_DIM ** (-0.5)
        weights = jnp.where(key_mask > 0, jnp.exp(scores), 0.0)
        low = lanes_of(weights.shape) < LENGTH
        sum_low = jnp.sum(jnp.where(low, weights, 0.0), axis=-1, keepdims=True)
        sum_high = jnp.sum(jnp.where(low, 0.0, weights), axis=-1, keepdims=True)
        probability = (weights / jnp.where(low, sum_low, sum_high)).astype(BF16)
        probabilities.append(probability)
        result = nn(probability, value_form).astype(BF16)
        for i in range(span[1] - span[0]):
            context.append(result[LENGTH * i : LENGTH * (i + 1)])
    branch = nn(jnp.concatenate(context, axis=1), wo[...])
    following = (wide + branch).astype(BF16)
    saved = jnp.concatenate(queries + [keys, values], axis=1)
    return following, saved, jnp.concatenate(probabilities, axis=0)


def layer_backward(grad, hidden, saved, probabilities, gain, wq, wo, cosine, sine, roll):
    queries = [saved[:, 128 * b : 128 * (b + 1)] for b in range(PAIRS)]
    key_forms = paired(saved[:, 896:1024].astype(F32), roll)
    value_forms = paired(saved[:, 1024:1152].astype(F32), roll)
    context_grad_t = nt(wo[...], grad)
    context_grads = [
        context_grad_t[128 * b : 128 * (b + 1)].T.astype(BF16) for b in range(PAIRS)
    ]
    query_grads = []
    key_parts = []
    value_parts = []
    for span, key_form, value_form in zip(SPANS, key_forms, value_forms):
        chosen = stacked(context_grads, span)
        probability = probabilities[LENGTH * span[0] : LENGTH * span[1]]
        wide_p = probability.astype(F32)
        prob_grad = nt(chosen, value_form)
        product = prob_grad * wide_p
        low = lanes_of(product.shape) < LENGTH
        sum_low = jnp.sum(jnp.where(low, product, 0.0), axis=-1, keepdims=True)
        sum_high = jnp.sum(jnp.where(low, 0.0, product), axis=-1, keepdims=True)
        score_grad = (
            wide_p * (prob_grad - jnp.where(low, sum_low, sum_high)) * HEAD_DIM ** (-0.5)
        ).astype(BF16)
        query_grad = nn(score_grad, key_form)
        for i in range(span[1] - span[0]):
            query_grads.append(query_grad[LENGTH * i : LENGTH * (i + 1)])
        key_parts.append(tn(score_grad, stacked(queries, span)))
        value_parts.append(tn(probability, chosen))

    def folded(parts):
        both, mixed, last = parts
        low_part = both[:LENGTH] + roll(both[LENGTH:], 64) + mixed[:LENGTH]
        high_part = mixed[LENGTH:] + last[LENGTH:] + roll(last[:LENGTH], 64)
        return jnp.where(lanes_of(low_part.shape) < 64, low_part, high_part)

    turned_back = [
        turned(block.astype(BF16).astype(F32), cosine, -sine, roll).astype(BF16)
        for block in query_grads + [folded(key_parts)]
    ]
    projected_grad = jnp.concatenate(turned_back + [folded(value_parts).astype(BF16)], axis=1)
    normed_grad = nt(wq[...], projected_grad).T
    wide = hidden.astype(F32)
    inverse = lax.rsqrt(jnp.mean(wide * wide, axis=-1, keepdims=True) + norm_eps)
    gained = normed_grad * gain
    inner = jnp.mean(gained * wide, axis=-1, keepdims=True)
    return (
        grad.astype(F32) + gained * inverse - wide * (inverse * inverse * inverse * inner)
    ).astype(BF16)


def tpu_roll(x, shift):
    return pltpu.roll(x, shift, axis=1)


def meet(axis):
    me = lax.axis_index(axis)
    count = lax.axis_size(axis)
    barrier = pltpu.get_barrier_semaphore()
    for step in (1, count - 1):
        pl.semaphore_signal(
            barrier,
            inc=1,
            device_id={axis: lax.rem(me + step, count)},
            device_id_type=pl.DeviceIdType.MESH,
        )
    pl.semaphore_wait(barrier, 2)


def forward_kernel(
    entry, gain, wq, wo, cosine, sine, key_mask, last_mask,
    hidden_out, saved_out, prob_out, last_out,
    inbox, outbox, send_sem, recv_sem,
):
    me = lax.axis_index("section")
    count = lax.axis_size("section")
    micros = entry.shape[0]
    meet("section")

    def hop(m):
        return pltpu.make_async_remote_copy(
            src_ref=outbox.at[m],
            dst_ref=inbox.at[m],
            send_sem=send_sem.at[m],
            recv_sem=recv_sem.at[m],
            device_id={"section": lax.rem(me + 1, count)},
            device_id_type=pl.DeviceIdType.MESH,
        )

    def step(m, carry):
        @pl.when(me == 0)
        def _():
            hidden_out[m] = entry[m]

        @pl.when(me > 0)
        def _():
            hop(m).wait_recv()
            hidden_out[m] = inbox[m]

        following, saved, probabilities = layer_forward(
            hidden_out[m], gain[...], wq, wo, cosine[...], sine[...], key_mask[m], tpu_roll
        )
        outbox[m] = following

        @pl.when(me < count - 1)
        def _():
            hop(m).start()

        saved_out[m] = saved
        prob_out[m] = probabilities
        last_out[m] = jnp.sum(following.astype(F32) * last_mask[m], axis=0, keepdims=True)
        return carry

    lax.fori_loop(0, micros, step, 0)

    @pl.when(me < count - 1)
    def _():
        for m in range(micros):
            hop(m).wait_send()


def backward_kernel(
    last_grad, hidden_in, saved_in, prob_in, gain, wq, wo, cosine, sine, last_mask,
    grad_out,
    inbox, outbox, send_sem, recv_sem,
):
    me = lax.axis_index("section")
    count = lax.axis_size("section")
    micros = hidden_in.shape[0]
    meet("section")

    def hop(m):
        return pltpu.make_async_remote_copy(
            src_ref=outbox.at[m],
            dst_ref=inbox.at[m],
            send_sem=send_sem.at[m],
            recv_sem=recv_sem.at[m],
            device_id={"section": lax.rem(me + count - 1, count)},
            device_id_type=pl.DeviceIdType.MESH,
        )

    def step(m, carry):
        @pl.when(me == count - 1)
        def _():
            outbox[m] = jnp.where(last_mask[m] > 0, last_grad[m], 0.0).astype(BF16)

        @pl.when(me < count - 1)
        def _():
            hop(m).wait_recv()
            outbox[m] = inbox[m]

        downstream = layer_backward(
            outbox[m], hidden_in[m], saved_in[m], prob_in[m],
            gain[...], wq, wo, cosine[...], sine[...], tpu_roll,
        )
        outbox[m] = downstream

        @pl.when(me > 0)
        def _():
            hop(m).start()

        grad_out[m] = downstream
        return carry

    lax.fori_loop(0, micros, step, 0)

    @pl.when(me > 0)
    def _():
        for m in range(micros):
            hop(m).wait_send()


def whole():
    return pl.BlockSpec(memory_space=pltpu.VMEM)


def run_kernel(body, out_shapes, scratch, ident, args):
    return pl.pallas_call(
        body,
        out_shape=out_shapes,
        in_specs=[whole()] * len(args),
        out_specs=jax.tree.map(lambda _: whole(), out_shapes),
        scratch_shapes=scratch,
        compiler_params=pltpu.CompilerParams(
            collective_id=ident, has_side_effects=True, vmem_limit_bytes=64000 * 1024
        ),
    )(*args)


def rms_scale(values, gain_row):
    return (
        values * lax.rsqrt(jnp.mean(values * values, axis=-1, keepdims=True) + norm_eps) * gain_row
    )


def embed_rows(rows_in, final_gain):
    pooled = rms_scale(rows_in.astype(F32), final_gain)
    return pooled * lax.rsqrt(jnp.sum(pooled * pooled, axis=-1, keepdims=True))


def pair_terms(question, passage, positive):
    scores = jnp.dot(question, passage.T, preferred_element_type=F32) * (1.0 / sharpness_divisor)
    weights = jnp.exp(scores)
    odds = weights / jnp.sum(weights, axis=-1, keepdims=True)
    target = (
        positive[:, None] == jnp.arange(passage.shape[0], dtype=jnp.int32)[None, :]
    ).astype(F32)
    return (odds - target) * (objective_coefficient / sharpness_divisor)


def turning(length):
    half = HEAD_DIM // 2
    frequency = rope_base ** (-jnp.arange(half, dtype=F32) * (2.0 / HEAD_DIM))
    angles = jnp.arange(length, dtype=jnp.int32).astype(F32)[:, None] * frequency[None, :]
    cosine, sine = jnp.cos(angles), jnp.sin(angles)
    return (
        jnp.concatenate([cosine] * 4, axis=1),
        jnp.concatenate([-sine, sine] * 2, axis=1),
    )


def per_device(entry, norm_gain, w_qkv, w_out, final_gain, lengths, positive):
    width = entry.shape[1]
    seqs = lengths.shape[0]
    length = entry.shape[0] // seqs
    pairs = positive.shape[0]
    pair_all = lax.all_gather(positive, DP, axis=0, tiled=True)
    full_out = lax.all_gather(w_out[0], DP, axis=0, tiled=True)
    full_qkv = lax.all_gather(w_qkv[0], DP, axis=0, tiled=True)
    cosine, sine = turning(length)
    spots = jnp.arange(length, dtype=jnp.int32)
    live = (spots[None, :] < lengths[:, None]).astype(F32)
    key_mask = jnp.concatenate([live, live], axis=1)[:, None, :]
    last_mask = (spots[None, :] == lengths[:, None] - 1).astype(F32)[:, :, None]
    block = jax.ShapeDtypeStruct((seqs, length, width), BF16)
    buffers = [
        pltpu.VMEM(block.shape, BF16),
        pltpu.VMEM(block.shape, BF16),
        pltpu.SemaphoreType.DMA((seqs,)),
        pltpu.SemaphoreType.DMA((seqs,)),
    ]
    hidden, saved, probabilities, last_rows = run_kernel(
        forward_kernel,
        [
            block,
            jax.ShapeDtypeStruct((seqs, length, 1152), BF16),
            jax.ShapeDtypeStruct((seqs, PAIRS * length, 2 * length), BF16),
            jax.ShapeDtypeStruct((seqs, 1, width), F32),
        ],
        buffers,
        0,
        (entry.reshape(block.shape), norm_gain, full_qkv, full_out, cosine, sine,
         key_mask, last_mask),
    )
    last_rows = last_rows[:, 0]
    embedding, back_embed = jax.vjp(lambda rows: embed_rows(rows, final_gain), last_rows)
    low = lax.all_gather(embedding.astype(BF16), DP, axis=0, tiled=True)
    low = low.reshape(-1, 2, width)
    question, passage = low[:, 0], low[:, 1]
    replica = lax.axis_index(DP)
    coefficient = pair_terms(question, passage, pair_all)
    mine_q = lax.dynamic_slice_in_dim(coefficient, replica * pairs, pairs, 0)
    mine_d = lax.dynamic_slice_in_dim(coefficient.T, replica * pairs, pairs, 0)
    grad_q = jnp.dot(mine_q, passage.astype(F32), precision=lax.Precision.HIGHEST)
    grad_d = jnp.dot(mine_d, question.astype(F32), precision=lax.Precision.HIGHEST)
    grad_emb = jnp.stack([grad_q, grad_d], axis=1).reshape(seqs, width)
    last_grad = back_embed(grad_emb)[0]
    grads = run_kernel(
        backward_kernel,
        block,
        buffers,
        1,
        (last_grad[:, None, :], hidden, saved, probabilities, norm_gain, full_qkv, full_out,
         cosine, sine, last_mask),
    )
    return grads.reshape(1, seqs * length, width)


def solution(mesh):
    finer = Mesh(
        mesh.devices.reshape(mesh.shape["section"], 4, 4, 2), ("section", "dp_0", "dp_1", "dp_2")
    )
    in_specs = (
        P(DP, None),
        P("section", None),
        P("section", DP, None),
        P("section", DP, None),
        P(),
        P(DP),
        P(DP),
    )
    return jax.shard_map(
        per_device, mesh=finer, in_specs=in_specs, out_specs=P("section", DP, None),
        check_vma=False,
    )
```

```python
import functools

import jax
import jax.numpy as jnp
from jax import lax
from jax.experimental import pallas as pl
from jax.experimental.pallas import tpu as pltpu
from jax.sharding import Mesh
from jax.sharding import PartitionSpec as P

HEAD_DIM = 64
GROUP_HEADS = 7
KV_GROUPS = 2
DP = ("dp_0", "dp_1", "dp_2")

rope_base = 1000000.0
norm_eps = 1e-06
sharpness_divisor = 0.05
objective_coefficient = 256.0

LENGTH = 48
PAIRS = 7
F32 = jnp.float32
BF16 = jnp.bfloat16


def nn(a, b):
    return lax.dot_general(a, b, (((1,), (0,)), ((), ())), preferred_element_type=F32)


def nt(a, b):
    return lax.dot_general(a, b, (((1,), (1,)), ((), ())), preferred_element_type=F32)


def tn(a, b):
    return lax.dot_general(a, b, (((0,), (0,)), ((), ())), preferred_element_type=F32)


def lanes_of(shape):
    return lax.broadcasted_iota(jnp.int32, shape, 1)


def turned(block, cosine, sine, roll):
    lane = lanes_of(block.shape)
    swapped = jnp.where(lane % 64 < 32, roll(block, 96), roll(block, 32))
    return block * cosine + swapped * sine


def paired(rows, roll):
    lane = lanes_of(rows.shape)
    other = roll(rows, 64)
    zero = jnp.zeros_like(rows)
    low = lane < 64
    first = jnp.where(low, rows, zero)
    second = jnp.where(low, zero, rows)
    return tuple(
        jnp.concatenate(two, axis=0).astype(BF16)
        for two in (
            (first, jnp.where(low, zero, other)),
            (first, second),
            (jnp.where(low, other, zero), second),
        )
    )


SPANS = ((0, 3), (3, 4), (4, 7))


def stacked(blocks, span):
    chosen = blocks[span[0] : span[1]]
    return chosen[0] if len(chosen) == 1 else jnp.concatenate(chosen, axis=0)


def layer_forward(hidden, gain, wq, wo, cosine, sine, key_mask, roll):
    wide = hidden.astype(F32)
    inverse = lax.rsqrt(jnp.mean(wide * wide, axis=-1, keepdims=True) + norm_eps)
    normed = (wide * inverse * gain).astype(BF16)
    projected = nn(normed, wq[...])
    blocks = [projected[:, 128 * b : 128 * (b + 1)] for b in range(9)]
    turned_blocks = [turned(b, cosine, sine, roll) for b in blocks[:8]]
    queries = [b.astype(BF16) for b in turned_blocks[:PAIRS]]
    keys = turned_blocks[PAIRS].astype(BF16)
    values = blocks[8].astype(BF16)
    key_forms = paired(keys.astype(F32), roll)
    value_forms = paired(values.astype(F32), roll)
    probabilities = []
    context = []
    for span, key_form, value_form in zip(SPANS, key_forms, value_forms):
        scores = nt(stacked(queries, span), key_form) * HEAD_DIM ** (-0.5)
        weights = jnp.where(key_mask > 0, jnp.exp(scores), 0.0)
        low = lanes_of(weights.shape) < LENGTH
        sum_low = jnp.sum(jnp.where(low, weights, 0.0), axis=-1, keepdims=True)
        sum_high = jnp.sum(jnp.where(low, 0.0, weights), axis=-1, keepdims=True)
        probability = (weights / jnp.where(low, sum_low, sum_high)).astype(BF16)
        probabilities.append(probability)
        result = nn(probability, value_form).astype(BF16)
        for i in range(span[1] - span[0]):
            context.append(result[LENGTH * i : LENGTH * (i + 1)])
    branch = nn(jnp.concatenate(context, axis=1), wo[...])
    following = (wide + branch).astype(BF16)
    saved = jnp.concatenate(queries + [keys, values], axis=1)
    return following, saved, jnp.concatenate(probabilities, axis=0)


def layer_backward(grad, hidden, saved, probabilities, gain, wq, wo, cosine, sine, roll):
    queries = [saved[:, 128 * b : 128 * (b + 1)] for b in range(PAIRS)]
    key_forms = paired(saved[:, 896:1024].astype(F32), roll)
    value_forms = paired(saved[:, 1024:1152].astype(F32), roll)
    context_grad_t = nt(wo[...], grad)
    context_grads = [
        context_grad_t[128 * b : 128 * (b + 1)].T.astype(BF16) for b in range(PAIRS)
    ]
    query_grads = []
    key_parts = []
    value_parts = []
    for span, key_form, value_form in zip(SPANS, key_forms, value_forms):
        chosen = stacked(context_grads, span)
        probability = probabilities[LENGTH * span[0] : LENGTH * span[1]]
        wide_p = probability.astype(F32)
        prob_grad = nt(chosen, value_form)
        product = prob_grad * wide_p
        low = lanes_of(product.shape) < LENGTH
        sum_low = jnp.sum(jnp.where(low, product, 0.0), axis=-1, keepdims=True)
        sum_high = jnp.sum(jnp.where(low, 0.0, product), axis=-1, keepdims=True)
        score_grad = (
            wide_p * (prob_grad - jnp.where(low, sum_low, sum_high)) * HEAD_DIM ** (-0.5)
        ).astype(BF16)
        query_grad = nn(score_grad, key_form)
        for i in range(span[1] - span[0]):
            query_grads.append(query_grad[LENGTH * i : LENGTH * (i + 1)])
        key_parts.append(tn(score_grad, stacked(queries, span)))
        value_parts.append(tn(probability, chosen))

    def folded(parts):
        both, mixed, last = parts
        low_part = both[:LENGTH] + roll(both[LENGTH:], 64) + mixed[:LENGTH]
        high_part = mixed[LENGTH:] + last[LENGTH:] + roll(last[:LENGTH], 64)
        return jnp.where(lanes_of(low_part.shape) < 64, low_part, high_part)

    turned_back = [
        turned(block.astype(BF16).astype(F32), cosine, -sine, roll).astype(BF16)
        for block in query_grads + [folded(key_parts)]
    ]
    projected_grad = jnp.concatenate(turned_back + [folded(value_parts).astype(BF16)], axis=1)
    normed_grad = nt(wq[...], projected_grad).T
    wide = hidden.astype(F32)
    inverse = lax.rsqrt(jnp.mean(wide * wide, axis=-1, keepdims=True) + norm_eps)
    gained = normed_grad * gain
    inner = jnp.mean(gained * wide, axis=-1, keepdims=True)
    return (
        grad.astype(F32) + gained * inverse - wide * (inverse * inverse * inverse * inner)
    ).astype(BF16)


def tpu_roll(x, shift):
    return pltpu.roll(x, shift, axis=1)


def remote(source, target, send, receive, place):
    return pltpu.make_async_remote_copy(
        src_ref=source,
        dst_ref=target,
        send_sem=send,
        recv_sem=receive,
        device_id=place,
        device_id_type=pl.DeviceIdType.MESH,
    )


class Plane:
    def __init__(self):
        self.x = lax.axis_index("dp_0")
        self.y = lax.axis_index("dp_1")
        self.core = lax.axis_index("dp_2")

    def spot(self, first, second):
        other = 1 - self.core
        return (
            lax.rem(self.x + first * other + second * self.core, 4),
            lax.rem(self.y + first * self.core + second * other, 4),
        )

    def slot(self, first, second, mine=True):
        x, y = self.spot(first % 4, second % 4)
        core = self.core if mine else 1 - self.core
        return (x * 4 + y) * 2 + core

    def device(self, first, second):
        x, y = self.spot(first % 4, second % 4)
        return {"dp_0": x, "dp_1": y}

    def partner_slot(self, x, y):
        return (x * 4 + y) * 2 + (1 - self.core)

    def partner(self):
        return {"dp_2": 1 - self.core}


def start_meeting(plane):
    me = lax.axis_index("section")
    count = lax.axis_size("section")
    barrier = pltpu.get_barrier_semaphore()
    places = [{"section": lax.rem(me + step, count)} for step in (1, count - 1)]
    places.append(plane.partner())
    places += [plane.device(a, b) for a in range(4) for b in range(4) if a or b]
    for place in places:
        pl.semaphore_signal(
            barrier, inc=1, device_id=place, device_id_type=pl.DeviceIdType.MESH
        )
    pl.semaphore_wait(barrier, len(places))


class Gather:
    def __init__(self, plane, own, whole, rows, cut, sends, receives, partner_receives):
        self.plane, self.own, self.whole = plane, own, whole
        self.rows, self.cut = rows, cut
        self.sends, self.receives = sends, receives
        self.partner_receives = partner_receives
        self.started = []

    def part(self, slot, half):
        low, size = ((0, self.rows), (0, self.cut), (self.cut, self.rows - self.cut))[half]
        return self.whole.at[pl.ds(pl.multiple_of(slot * self.rows + low, 16), size)]

    def send(self, slot, half, place, receives=None, own=False):
        target = self.part(slot, half)
        receives = self.receives.at[slot // 2, max(half - 1, 0)] if receives is None else receives
        copy = remote(
            self.own if own else target,
            target,
            self.sends.at[len(self.started)],
            receives,
            place,
        )
        copy.start()
        self.started.append(copy)

    def hand_over(self, slot, own=False):
        self.send(
            slot, 0, self.plane.partner(), self.partner_receives.at[slot // 2], own=own
        )

    def arrived(self, slot, half):
        part = self.part(slot, half)
        remote(
            part, part, self.sends.at[0], self.receives.at[slot // 2, max(half - 1, 0)],
            self.plane.partner(),
        ).wait_recv()

    def begin(self):
        plane = self.plane
        slot = plane.slot(0, 0)
        for step in (1, -1):
            self.send(slot, 0, plane.device(step, 0), own=True)
            self.send(slot, 0, plane.device(0, step), own=True)
        self.hand_over(slot, own=True)
        self.whole[pl.ds(pl.multiple_of(slot * self.rows, 16), self.rows)] = self.own[...]

    def first_ring(self):
        plane = self.plane
        for step, half in ((-1, 1), (1, 2)):
            slot = plane.slot(step, 0)
            self.arrived(slot, 0)
            self.send(slot, half, plane.device(-step, 0))
            self.spread(slot)
        slot = plane.slot(2, 0)
        self.arrived(slot, 1)
        self.arrived(slot, 2)
        self.spread(slot)

    def spread(self, slot):
        for step in (1, -1):
            self.send(slot, 0, self.plane.device(0, step))
        self.hand_over(slot)

    def second_ring(self):
        plane = self.plane
        for first in (0, -1, 1, 2):
            for step, half in ((-1, 1), (1, 2)):
                slot = plane.slot(first, step)
                self.arrived(slot, 0)
                self.send(slot, half, plane.device(0, -step))
                self.hand_over(slot)
        for first in (0, -1, 1, 2):
            slot = plane.slot(first, 2)
            self.arrived(slot, 1)
            self.arrived(slot, 2)
            self.hand_over(slot)

    def from_partner(self):
        for at in range(16):
            part = self.part(self.plane.partner_slot(at // 4, at % 4), 0)
            remote(
                part, part, self.sends.at[0], self.partner_receives.at[at],
                self.plane.partner(),
            ).wait_recv()

    def drain(self):
        for copy in self.started:
            copy.wait_send()


GATHER_SENDS = 36


def contrast(plane, last_rows, final_gain, positive, gathered, outgoing, sends, receives,
             partner_receives, last_grad):
    rows = jnp.concatenate([last_rows[m] for m in range(4)], axis=0)
    gain = final_gain[...]
    inverse = lax.rsqrt(jnp.mean(rows * rows, axis=-1, keepdims=True) + norm_eps)
    pooled = rows * inverse * gain
    scale = lax.rsqrt(jnp.sum(pooled * pooled, axis=-1, keepdims=True))
    embedding = pooled * scale
    tail = jnp.broadcast_to(positive[...], (4, 128))
    packed = jnp.concatenate(
        [
            jnp.concatenate([embedding[:, 896 * k : 896 * (k + 1)], tail], axis=1)
            for k in range(4)
        ],
        axis=0,
    ).astype(BF16)
    outgoing[...] = packed
    mine = plane.slot(0, 0)
    gathered[mine] = packed
    started = []

    def send(source, slot, receive, place):
        copy = remote(source, gathered.at[slot], sends.at[len(started)], receive, place)
        copy.start()
        started.append(copy)

    others = [(a, b) for a in range(4) for b in range(4) if a or b]
    others.sort(key=lambda ab: min(ab[0], 4 - ab[0]) + min(ab[1], 4 - ab[1]))
    for a, b in reversed(others):
        send(outgoing, mine, receives.at[mine // 2], plane.device(a, b))
    send(outgoing, mine, partner_receives.at[mine // 2], plane.partner())
    for a, b in others:
        slot = plane.slot(a, b)
        remote(
            outgoing, gathered.at[slot], sends.at[0], receives.at[slot // 2], plane.partner()
        ).wait_recv()
        send(gathered.at[slot], slot, partner_receives.at[slot // 2], plane.partner())
    for at in range(16):
        slot = plane.partner_slot(at // 4, at % 4)
        remote(
            outgoing, gathered.at[slot], sends.at[0], partner_receives.at[at], plane.partner()
        ).wait_recv()
    for copy in started:
        copy.wait_send()

    flat = jnp.concatenate([gathered[i] for i in range(32)], axis=0)
    at = lax.broadcasted_iota(jnp.int32, (128, 512), 0)
    lane = lanes_of((128, 512))
    number = at & 63
    row = (number >> 1) * 16 + (number & 1) * 2 + (at >> 6)
    pieces = []
    for k in range(4):
        chosen = jnp.where(lane == row + 4 * k, 1.0, 0.0).astype(BF16)
        pieces.append(nn(chosen, flat))
    everyone = jnp.concatenate([p[:, :896] for p in pieces], axis=1).astype(BF16)
    target = pieces[0][:64, 896:960]
    logits = nt(everyone[:64], everyone[64:]) * (1.0 / sharpness_divisor)
    weights = jnp.exp(logits)
    odds = weights / jnp.sum(weights, axis=-1, keepdims=True)
    column = lanes_of((64, 64))
    hit = jnp.where(target == column.astype(F32), 1.0, 0.0)
    coefficient = (odds - hit) * (objective_coefficient / sharpness_divisor)
    turned_coefficient = coefficient.T
    line = lax.broadcasted_iota(jnp.int32, (64, 64), 0)
    blank = jnp.zeros((1, 64), F32)
    replica = mine
    chosen_rows = []
    for m in range(4):
        source = turned_coefficient if m % 2 else coefficient
        one = jnp.sum(
            jnp.where(line == replica * 2 + m // 2, source, 0.0), axis=0, keepdims=True
        )
        chosen_rows.append(jnp.concatenate([one, blank] if m % 2 else [blank, one], axis=1))
    exact = jnp.concatenate(chosen_rows, axis=0)
    top = exact.astype(BF16)
    rest = exact - top.astype(F32)
    middle = rest.astype(BF16)
    low = (rest - middle.astype(F32)).astype(BF16)
    embed_grad = nn(top, everyone) + nn(middle, everyone) + nn(low, everyone)
    pooled_grad = embed_grad * scale - pooled * (
        scale * scale * scale * jnp.sum(embed_grad * pooled, axis=-1, keepdims=True)
    )
    gained = pooled_grad * gain
    row_grad = gained * inverse - rows * (
        inverse * inverse * inverse * jnp.mean(gained * rows, axis=-1, keepdims=True)
    )
    for m in range(4):
        last_grad[m] = row_grad[m : m + 1]


def step_kernel(
    entry, gain, wq_own, wo_own, cosine, sine, key_mask, last_mask, final_gain, positive,
    spread_rows,
    grad_out,
    wq, wo_spaced, wo, hidden, saved, prob, last_rows, last_grad, embeds, embed_own,
    inbox, outbox, back_inbox, back_outbox,
    wq_send, wq_recv, wq_cross, wo_send, wo_recv, wo_cross, e_send, e_recv, e_cross,
    f_send, f_recv, b_send, b_recv,
):
    me = lax.axis_index("section")
    count = lax.axis_size("section")
    micros = entry.shape[0]
    plane = Plane()
    start_meeting(plane)
    gathers = (
        Gather(plane, wq_own, wq, 112, 64, wq_send, wq_recv, wq_cross),
        Gather(plane, wo_own, wo_spaced, 32, 16, wo_send, wo_recv, wo_cross),
    )
    for gather in gathers:
        gather.begin()
    for gather in gathers:
        gather.first_ring()
    for gather in gathers:
        gather.second_ring()
    for gather in gathers:
        gather.from_partner()
    for gather in gathers:
        gather.drain()

    def pack(b, carry):
        spaced = wo_spaced[pl.ds(pl.multiple_of(b * 256, 256), 256)]
        wo[pl.ds(pl.multiple_of(b * 224, 16), 224)] = nn(spread_rows[...], spaced).astype(BF16)
        return carry

    lax.fori_loop(0, 4, pack, 0)

    def hop(m):
        return remote(
            outbox.at[m], inbox.at[m], f_send.at[m], f_recv.at[m],
            {"section": lax.rem(me + 1, count)},
        )

    def forward(m, carry):
        @pl.when(me == 0)
        def _():
            hidden[m] = entry[m]

        @pl.when(me > 0)
        def _():
            hop(m).wait_recv()
            hidden[m] = inbox[m]

        following, kept, probabilities = layer_forward(
            hidden[m], gain[...], wq, wo, cosine[...], sine[...], key_mask[m], tpu_roll
        )
        outbox[m] = following

        @pl.when(me < count - 1)
        def _():
            hop(m).start()

        saved[m] = kept
        prob[m] = probabilities
        last_rows[m] = jnp.sum(following.astype(F32) * last_mask[m], axis=0, keepdims=True)
        return carry

    lax.fori_loop(0, micros, forward, 0)

    @pl.when(me < count - 1)
    def _():
        for m in range(micros):
            hop(m).wait_send()

    @pl.when(me == count - 1)
    def _():
        contrast(plane, last_rows, final_gain, positive, embeds, embed_own, e_send, e_recv,
                 e_cross, last_grad)

    def back_hop(m):
        return remote(
            back_outbox.at[m], back_inbox.at[m], b_send.at[m], b_recv.at[m],
            {"section": lax.rem(me + count - 1, count)},
        )

    def backward(m, carry):
        @pl.when(me == count - 1)
        def _():
            grad_out[m] = jnp.where(last_mask[m] > 0, last_grad[m], 0.0).astype(BF16)

        @pl.when(me < count - 1)
        def _():
            back_hop(m).wait_recv()
            grad_out[m] = back_inbox[m]

        downstream = layer_backward(
            grad_out[m], hidden[m], saved[m], prob[m],
            gain[...], wq, wo, cosine[...], sine[...], tpu_roll,
        )
        back_outbox[m] = downstream

        @pl.when(me > 0)
        def _():
            back_hop(m).start()

        grad_out[m] = downstream
        return carry

    lax.fori_loop(0, micros, backward, 0)

    @pl.when(me > 0)
    def _():
        for m in range(micros):
            back_hop(m).wait_send()


def whole():
    return pl.BlockSpec(memory_space=pltpu.VMEM)


def turning(length):
    half = HEAD_DIM // 2
    frequency = rope_base ** (-jnp.arange(half, dtype=F32) * (2.0 / HEAD_DIM))
    angles = jnp.arange(length, dtype=jnp.int32).astype(F32)[:, None] * frequency[None, :]
    cosine, sine = jnp.cos(angles), jnp.sin(angles)
    return (
        jnp.concatenate([cosine] * 4, axis=1),
        jnp.concatenate([-sine, sine] * 2, axis=1),
    )


def per_device(entry, norm_gain, w_qkv, w_out, final_gain, lengths, positive):
    width = entry.shape[1]
    seqs = lengths.shape[0]
    length = entry.shape[0] // seqs
    cosine, sine = turning(length)
    spots = jnp.arange(length, dtype=jnp.int32)
    live = (spots[None, :] < lengths[:, None]).astype(F32)
    key_mask = jnp.concatenate([live, live], axis=1)[:, None, :]
    last_mask = (spots[None, :] == lengths[:, None] - 1).astype(F32)[:, :, None]
    target = jnp.repeat(positive, 2).astype(F32)[:, None]
    packed = jnp.arange(224)
    spread_rows = (
        jnp.arange(256)[None, :] == (packed // 28 * 32 + packed % 28)[:, None]
    ).astype(BF16)
    block = (seqs, length, width)
    dma = pltpu.SemaphoreType.DMA
    args = (
        entry.reshape(block), norm_gain, w_qkv[0], jnp.pad(w_out[0], ((0, 4), (0, 0))),
        cosine, sine, key_mask, last_mask, final_gain[None, :], target, spread_rows,
    )
    grads = pl.pallas_call(
        step_kernel,
        out_shape=jax.ShapeDtypeStruct(block, BF16),
        in_specs=[whole()] * len(args),
        out_specs=whole(),
        scratch_shapes=[
            pltpu.VMEM((width, 1152), BF16),
            pltpu.VMEM((1024, width), BF16),
            pltpu.VMEM((896, width), BF16),
            pltpu.VMEM(block, BF16),
            pltpu.VMEM((seqs, length, 1152), BF16),
            pltpu.VMEM((seqs, PAIRS * length, 2 * length), BF16),
            pltpu.VMEM((seqs, 1, width), F32),
            pltpu.VMEM((seqs, 1, width), F32),
            pltpu.VMEM((32, 16, 1024), BF16),
            pltpu.VMEM((16, 1024), BF16),
            pltpu.VMEM(block, BF16),
            pltpu.VMEM(block, BF16),
            pltpu.VMEM(block, BF16),
            pltpu.VMEM(block, BF16),
            dma((GATHER_SENDS,)), dma((16, 2)), dma((16,)),
            dma((GATHER_SENDS,)), dma((16, 2)), dma((16,)),
            dma((31,)), dma((16,)), dma((16,)),
            dma((seqs,)), dma((seqs,)), dma((seqs,)), dma((seqs,)),
        ],
        compiler_params=pltpu.CompilerParams(
            collective_id=0, has_side_effects=True, vmem_limit_bytes=64000 * 1024
        ),
    )(*args)
    return grads.reshape(1, seqs * length, width)


def solution(mesh):
    finer = Mesh(
        mesh.devices.reshape(mesh.shape["section"], 4, 4, 2), ("section", "dp_0", "dp_1", "dp_2")
    )
    in_specs = (
        P(DP, None),
        P("section", None),
        P("section", DP, None),
        P("section", DP, None),
        P(),
        P(DP),
        P(DP),
    )
    return jax.shard_map(
        per_device, mesh=finer, in_specs=in_specs, out_specs=P("section", DP, None),
        check_vma=False,
    )
```

```python
import jax
import jax.numpy as jnp
import numpy as np
from jax import lax
from jax.experimental import pallas as pl
from jax.experimental.pallas import tpu as pltpu
from jax.sharding import Mesh
from jax.sharding import PartitionSpec as P

HEAD_DIM = 64
GROUP_HEADS = 7
KV_GROUPS = 2
DP = ("dp_0", "dp_1", "dp_2")

rope_base = 1000000.0
norm_eps = 1e-06
sharpness_divisor = 0.05
objective_coefficient = 256.0

LENGTH = 48
PAIRS = 7
F32 = jnp.float32
BF16 = jnp.bfloat16


def nn(a, b):
    return lax.dot_general(a, b, (((1,), (0,)), ((), ())), preferred_element_type=F32)


def nt(a, b):
    return lax.dot_general(a, b, (((1,), (1,)), ((), ())), preferred_element_type=F32)


def tn(a, b):
    return lax.dot_general(a, b, (((0,), (0,)), ((), ())), preferred_element_type=F32)


def lanes_of(shape):
    return lax.broadcasted_iota(jnp.int32, shape, 1)


def turned(block, cosine, sine, roll):
    lane = lanes_of(block.shape)
    swapped = jnp.where(lane % 64 < 32, roll(block, 96), roll(block, 32))
    return block * cosine + swapped * sine


def paired(rows, roll):
    lane = lanes_of(rows.shape)
    other = roll(rows, 64)
    zero = jnp.zeros_like(rows)
    low = lane < 64
    first = jnp.where(low, rows, zero)
    second = jnp.where(low, zero, rows)
    return tuple(
        jnp.concatenate(two, axis=0).astype(BF16)
        for two in (
            (first, jnp.where(low, zero, other)),
            (first, second),
            (jnp.where(low, other, zero), second),
        )
    )


SPANS = ((0, 3), (3, 4), (4, 7))


def stacked(blocks, span):
    chosen = blocks[span[0] : span[1]]
    return chosen[0] if len(chosen) == 1 else jnp.concatenate(chosen, axis=0)


CHUNKS = ((0, 1024), (1024, 1024), (2048, 1024), (3072, 512))


def live_lanes(shape, length):
    lane = lanes_of(shape)
    return jnp.where(lane < LENGTH, lane, lane - LENGTH) < length


def is_last(length):
    return lax.broadcasted_iota(jnp.int32, (LENGTH, 1), 0) == length - 1


def project(chunk_of, gain, wq):
    squares, projected = 0.0, 0.0
    for low, size in CHUNKS:
        wide = chunk_of(low, size).astype(F32)
        squares = squares + jnp.sum(wide * wide, axis=-1, keepdims=True)
        gained = (wide * gain[:, low : low + size]).astype(BF16)
        projected = projected + nn(gained, wq[low : low + size, :])
    inverse = lax.rsqrt(squares * (1.0 / 3584) + norm_eps)
    return projected * inverse, inverse


def attend(projected, length, cosine, sine, roll):
    blocks = [projected[:, 128 * b : 128 * (b + 1)] for b in range(9)]
    turned_blocks = [turned(b, cosine, sine, roll) for b in blocks[:8]]
    queries = [b.astype(BF16) for b in turned_blocks[:PAIRS]]
    keys = turned_blocks[PAIRS].astype(BF16)
    values = blocks[8].astype(BF16)
    key_forms = paired(keys.astype(F32), roll)
    value_forms = paired(values.astype(F32), roll)
    probabilities = []
    context = []
    for span, key_form, value_form in zip(SPANS, key_forms, value_forms):
        scores = nt(stacked(queries, span), key_form) * HEAD_DIM ** (-0.5)
        weights = jnp.where(live_lanes(scores.shape, length), jnp.exp(scores), 0.0)
        low = lanes_of(weights.shape) < LENGTH
        sum_low = jnp.sum(jnp.where(low, weights, 0.0), axis=-1, keepdims=True)
        sum_high = jnp.sum(jnp.where(low, 0.0, weights), axis=-1, keepdims=True)
        probability = (weights / jnp.where(low, sum_low, sum_high)).astype(BF16)
        probabilities.append(probability)
        result = nn(probability, value_form).astype(BF16)
        for i in range(span[1] - span[0]):
            context.append(result[LENGTH * i : LENGTH * (i + 1)])
    saved = jnp.concatenate(queries + [keys, values], axis=1)
    return jnp.concatenate(context, axis=1), saved, jnp.concatenate(probabilities, axis=0)


def context_gradient(chunk_of, wo):
    total = 0.0
    for low, size in CHUNKS:
        total = total + nt(chunk_of(low, size), wo[:, low : low + size])
    return total.astype(BF16)


def attend_back(context_grad, saved, probabilities, cosine, sine, roll):
    context_grads = [context_grad[:, 128 * b : 128 * (b + 1)] for b in range(PAIRS)]
    queries = [saved[:, 128 * b : 128 * (b + 1)] for b in range(PAIRS)]
    key_forms = paired(saved[:, 896:1024].astype(F32), roll)
    value_forms = paired(saved[:, 1024:1152].astype(F32), roll)
    query_grads = []
    key_parts = []
    value_parts = []
    for span, key_form, value_form in zip(SPANS, key_forms, value_forms):
        chosen = stacked(context_grads, span)
        probability = probabilities[LENGTH * span[0] : LENGTH * span[1]]
        wide_p = probability.astype(F32)
        prob_grad = nt(chosen, value_form)
        product = prob_grad * wide_p
        low = lanes_of(product.shape) < LENGTH
        sum_low = jnp.sum(jnp.where(low, product, 0.0), axis=-1, keepdims=True)
        sum_high = jnp.sum(jnp.where(low, 0.0, product), axis=-1, keepdims=True)
        score_grad = (
            wide_p * (prob_grad - jnp.where(low, sum_low, sum_high)) * HEAD_DIM ** (-0.5)
        ).astype(BF16)
        query_grad = nn(score_grad, key_form)
        for i in range(span[1] - span[0]):
            query_grads.append(query_grad[LENGTH * i : LENGTH * (i + 1)])
        key_parts.append(tn(score_grad, stacked(queries, span)))
        value_parts.append(tn(probability, chosen))

    def folded(parts):
        both, mixed, last = parts
        low_part = both[:LENGTH] + roll(both[LENGTH:], 64) + mixed[:LENGTH]
        high_part = mixed[LENGTH:] + last[LENGTH:] + roll(last[:LENGTH], 64)
        return jnp.where(lanes_of(low_part.shape) < 64, low_part, high_part)

    grads = [
        block.astype(BF16).astype(F32)
        for block in query_grads + [folded(key_parts), folded(value_parts)]
    ]
    product = 0.0
    for b, block in enumerate(grads):
        product = product + block * saved[:, 128 * b : 128 * (b + 1)].astype(F32)
    turned_back = [turned(block, cosine, -sine, roll).astype(BF16) for block in grads[:8]]
    projected_grad = jnp.concatenate(turned_back + [grads[8].astype(BF16)], axis=1)
    return projected_grad, jnp.sum(product, axis=-1, keepdims=True)


def tpu_roll(x, shift):
    return pltpu.roll(x, shift, axis=1)


def remote(source, target, send, receive, place):
    return pltpu.make_async_remote_copy(
        src_ref=source,
        dst_ref=target,
        send_sem=send,
        recv_sem=receive,
        device_id=place,
        device_id_type=pl.DeviceIdType.MESH,
    )


class Plane:
    def __init__(self):
        self.x = lax.axis_index("dp_0")
        self.y = lax.axis_index("dp_1")
        self.core = lax.axis_index("dp_2")

    def spot(self, first, second):
        other = 1 - self.core
        return (
            lax.rem(self.x + first * other + second * self.core, 4),
            lax.rem(self.y + first * self.core + second * other, 4),
        )

    def slot(self, first, second, mine=True):
        x, y = self.spot(first % 4, second % 4)
        core = self.core if mine else 1 - self.core
        return (x * 4 + y) * 2 + core

    def device(self, first, second):
        x, y = self.spot(first % 4, second % 4)
        return {"dp_0": x, "dp_1": y}

    def partner_slot(self, x, y):
        return (x * 4 + y) * 2 + (1 - self.core)

    def partner(self):
        return {"dp_2": 1 - self.core}


def start_meeting(plane):
    me = lax.axis_index("section")
    count = lax.axis_size("section")
    barrier = pltpu.get_barrier_semaphore()
    places = [{"section": lax.rem(me + step, count)} for step in (1, count - 1)]
    places.append(plane.partner())
    places += [plane.device(a, b) for a in range(4) for b in range(4) if a or b]
    for place in places:
        pl.semaphore_signal(
            barrier, inc=1, device_id=place, device_id_type=pl.DeviceIdType.MESH
        )
    pl.semaphore_wait(barrier, len(places))


class Gather:
    def __init__(self, plane, whole, rows, cut, sends, receives, partner_receives):
        self.plane, self.whole = plane, whole
        self.rows, self.cut = rows, cut
        self.sends, self.receives = sends, receives
        self.partner_receives = partner_receives
        self.started = []

    def part(self, slot, half):
        low, size = ((0, self.rows), (0, self.cut), (self.cut, self.rows - self.cut))[half]
        return self.whole.at[pl.ds(pl.multiple_of(slot * self.rows + low, 16), size)]

    def send(self, slot, half, place, receives=None):
        target = self.part(slot, half)
        receives = self.receives.at[slot // 2, max(half - 1, 0)] if receives is None else receives
        copy = remote(
            target,
            target,
            self.sends.at[len(self.started)],
            receives,
            place,
        )
        copy.start()
        self.started.append(copy)

    def hand_over(self, slot):
        self.send(slot, 0, self.plane.partner(), self.partner_receives.at[slot // 2])

    def arrived(self, slot, half):
        part = self.part(slot, half)
        remote(
            part, part, self.sends.at[0], self.receives.at[slot // 2, max(half - 1, 0)],
            self.plane.partner(),
        ).wait_recv()

    def begin(self):
        plane = self.plane
        slot = plane.slot(0, 0)
        for step in (1, -1):
            self.send(slot, 0, plane.device(step, 0))
            self.send(slot, 0, plane.device(0, step))
        self.hand_over(slot)

    def first_near(self):
        plane = self.plane
        for step, half in ((-1, 1), (1, 2)):
            slot = plane.slot(step, 0)
            self.arrived(slot, 0)
            self.send(slot, half, plane.device(-step, 0))
            self.spread(slot)

    def first_far(self):
        slot = self.plane.slot(2, 0)
        self.arrived(slot, 1)
        self.arrived(slot, 2)
        self.spread(slot)

    def spread(self, slot):
        for step in (1, -1):
            self.send(slot, 0, self.plane.device(0, step))
        self.hand_over(slot)

    def second_near(self, first):
        plane = self.plane
        for step, half in ((-1, 1), (1, 2)):
            slot = plane.slot(first, step)
            self.arrived(slot, 0)
            self.send(slot, half, plane.device(0, -step))
            self.hand_over(slot)

    def second_far(self, first):
        slot = self.plane.slot(first, 2)
        self.arrived(slot, 1)
        self.arrived(slot, 2)
        self.hand_over(slot)

    def from_partner(self):
        for at in range(16):
            part = self.part(self.plane.partner_slot(at // 4, at % 4), 0)
            remote(
                part, part, self.sends.at[0], self.partner_receives.at[at],
                self.plane.partner(),
            ).wait_recv()

    def drain(self):
        for copy in self.started:
            copy.wait_send()


GATHER_SENDS = 36


def contrast(plane, last_rows, final_gain, positive, gathered, outgoing, sends, receives,
             partner_receives, last_grad):
    rows = jnp.concatenate([last_rows[m] for m in range(4)], axis=0)
    gain = final_gain[...].reshape(1, -1)
    inverse = lax.rsqrt(jnp.mean(rows * rows, axis=-1, keepdims=True) + norm_eps)
    pooled = rows * inverse * gain
    scale = lax.rsqrt(jnp.sum(pooled * pooled, axis=-1, keepdims=True))
    embedding = pooled * scale
    spot = lax.broadcasted_iota(jnp.int32, (4, 128), 0)
    tail = jnp.where(spot < 2, positive[0], positive[1]).astype(F32)
    packed = jnp.concatenate(
        [
            jnp.concatenate([embedding[:, 896 * k : 896 * (k + 1)], tail], axis=1)
            for k in range(4)
        ],
        axis=0,
    ).astype(BF16)
    outgoing[...] = packed
    mine = plane.slot(0, 0)
    gathered[mine] = packed
    started = []

    def send(source, slot, receive, place):
        copy = remote(source, gathered.at[slot], sends.at[len(started)], receive, place)
        copy.start()
        started.append(copy)

    others = [(a, b) for a in range(4) for b in range(4) if a or b]
    others.sort(key=lambda ab: min(ab[0], 4 - ab[0]) + min(ab[1], 4 - ab[1]))
    for a, b in reversed(others):
        send(outgoing, mine, receives.at[mine // 2], plane.device(a, b))
    send(outgoing, mine, partner_receives.at[mine // 2], plane.partner())
    for a, b in others:
        slot = plane.slot(a, b)
        remote(
            outgoing, gathered.at[slot], sends.at[0], receives.at[slot // 2], plane.partner()
        ).wait_recv()
        send(gathered.at[slot], slot, partner_receives.at[slot // 2], plane.partner())
    for at in range(16):
        slot = plane.partner_slot(at // 4, at % 4)
        remote(
            outgoing, gathered.at[slot], sends.at[0], partner_receives.at[at], plane.partner()
        ).wait_recv()
    for copy in started:
        copy.wait_send()

    flat = jnp.concatenate([gathered[i] for i in range(32)], axis=0)
    at = lax.broadcasted_iota(jnp.int32, (128, 512), 0)
    lane = lanes_of((128, 512))
    number = at & 63
    row = (number >> 1) * 16 + (number & 1) * 2 + (at >> 6)
    pieces = []
    for k in range(4):
        chosen = jnp.where(lane == row + 4 * k, 1.0, 0.0).astype(BF16)
        pieces.append(nn(chosen, flat))
    everyone = jnp.concatenate([p[:, :896] for p in pieces], axis=1).astype(BF16)
    target = pieces[0][:64, 896:960]
    logits = nt(everyone[:64], everyone[64:]) * (1.0 / sharpness_divisor)
    weights = jnp.exp(logits)
    odds = weights / jnp.sum(weights, axis=-1, keepdims=True)
    column = lanes_of((64, 64))
    hit = jnp.where(target == column.astype(F32), 1.0, 0.0)
    coefficient = (odds - hit) * (objective_coefficient / sharpness_divisor)
    turned_coefficient = coefficient.T
    line = lax.broadcasted_iota(jnp.int32, (64, 64), 0)
    blank = jnp.zeros((1, 64), F32)
    replica = mine
    chosen_rows = []
    for m in range(4):
        source = turned_coefficient if m % 2 else coefficient
        one = jnp.sum(
            jnp.where(line == replica * 2 + m // 2, source, 0.0), axis=0, keepdims=True
        )
        chosen_rows.append(jnp.concatenate([one, blank] if m % 2 else [blank, one], axis=1))
    exact = jnp.concatenate(chosen_rows, axis=0)
    top = exact.astype(BF16)
    rest = exact - top.astype(F32)
    middle = rest.astype(BF16)
    low = (rest - middle.astype(F32)).astype(BF16)
    embed_grad = nn(top, everyone) + nn(middle, everyone) + nn(low, everyone)
    pooled_grad = embed_grad * scale - pooled * (
        scale * scale * scale * jnp.sum(embed_grad * pooled, axis=-1, keepdims=True)
    )
    gained = pooled_grad * gain
    row_grad = gained * inverse - rows * (
        inverse * inverse * inverse * jnp.mean(gained * rows, axis=-1, keepdims=True)
    )
    for m in range(4):
        last_grad[m] = row_grad[m : m + 1]


def step_kernel(
    lengths, positive, entry, gain, wq_own, wo_own, cosine, sine, final_gain, spread_rows,
    grad_out,
    wq, wo_spaced, wo, hidden, saved, prob, inverses, last_rows, last_grad, embeds, embed_own,
    outbox, grads,
    wq_send, wq_recv, wq_cross, wo_send, wo_recv, wo_cross, e_send, e_recv, e_cross,
    f_send, f_recv, b_send, b_recv, f_turn, b_turn,
):
    me = lax.axis_index("section")
    count = lax.axis_size("section")
    micros = entry.shape[0]
    plane = Plane()
    mine = plane.slot(0, 0)
    wq[pl.ds(pl.multiple_of(mine * 112, 16), 112)] = wq_own[...]
    wo_spaced[pl.ds(pl.multiple_of(mine * 32, 16), 32)] = jnp.concatenate(
        [wo_own[...], jnp.zeros((4, wo_own.shape[1]), BF16)], axis=0
    )
    start_meeting(plane)
    gathers = (
        Gather(plane, wq, 112, 64, wq_send, wq_recv, wq_cross),
        Gather(plane, wo_spaced, 32, 16, wo_send, wo_recv, wo_cross),
    )
    for gather in gathers:
        gather.begin()

    @pl.when(me == 0)
    def _():
        hidden[...] = entry[...]

    for gather in gathers:
        gather.first_near()
    for gather in gathers:
        gather.second_near(0)
    for gather in gathers:
        gather.first_far()
    for first in (-1, 1, 2):
        for gather in gathers:
            gather.second_near(first)
    for gather in gathers:
        for first in (0, -1, 1, 2):
            gather.second_far(first)
    for gather in gathers:
        gather.from_partner()
    for gather in gathers:
        gather.drain()

    def pack(b, carry):
        spaced = wo_spaced[pl.ds(pl.multiple_of(b * 256, 256), 256)]
        wo[pl.ds(pl.multiple_of(b * 224, 16), 224)] = nn(spread_rows[...], spaced).astype(BF16)
        return carry

    lax.fori_loop(0, 4, pack, 0)

    def hop(m, k):
        low, size = CHUNKS[k]
        return remote(
            outbox.at[m, :, pl.ds(low, size)], hidden.at[m, :, pl.ds(low, size)],
            f_send.at[m, k], f_recv.at[m, k], {"section": lax.rem(me + 1, count)},
        )

    def back_hop(m, k):
        low, size = CHUNKS[k]
        return remote(
            grad_out.at[m, :, pl.ds(low, size)], grads.at[m, :, pl.ds(low, size)],
            b_send.at[m, k], b_recv.at[m, k], {"section": lax.rem(me + count - 1, count)},
        )

    def take_turn(first, turn, m):
        @pl.when(jnp.logical_and(me == first, plane.core + m > 0))
        def _():
            pl.semaphore_wait(turn, 1)

    def give_turn(first, turn, m, copies):
        @pl.when(me == first)
        def _():
            for k in range(len(CHUNKS)):
                copies(m, k).wait_send()

        @pl.when(jnp.logical_and(me == first, m + plane.core < micros))
        def _():
            pl.semaphore_signal(
                turn, inc=1, device_id=plane.partner(), device_id_type=pl.DeviceIdType.MESH
            )

    def forward(m, carry):
        length = lengths[m]

        def chunk_of(low, size):
            k = [c[0] for c in CHUNKS].index(low)

            @pl.when(me > 0)
            def _():
                hop(m, k).wait_recv()

            return hidden[m, :, low : low + size]

        projected, inverse = project(chunk_of, gain, wq)
        inverses[m] = inverse
        context, kept, probabilities = attend(
            projected, length, cosine[...], sine[...], tpu_roll
        )
        last = is_last(length)
        for k, (low, size) in enumerate(CHUNKS):
            wide = hidden[m, :, low : low + size].astype(F32)
            following = (wide + nn(context, wo[:, low : low + size])).astype(BF16)
            outbox[m, :, low : low + size] = following
            if k == 0:
                take_turn(0, f_turn, m)

            @pl.when(me < count - 1)
            def _():
                hop(m, k).start()

            last_rows[m, :, low : low + size] = jnp.sum(
                jnp.where(last, following.astype(F32), 0.0), axis=0, keepdims=True
            )
        saved[m] = kept
        prob[m] = probabilities
        give_turn(0, f_turn, m, hop)
        return carry

    lax.fori_loop(0, micros, forward, 0)

    @pl.when(jnp.logical_and(me > 0, me < count - 1))
    def _():
        for m in range(micros):
            for k in range(len(CHUNKS)):
                hop(m, k).wait_send()

    @pl.when(me == count - 1)
    def _():
        contrast(plane, last_rows, final_gain, positive, embeds, embed_own, e_send, e_recv,
                 e_cross, last_grad)
        for m in range(micros):
            grads[m] = jnp.where(is_last(lengths[m]), last_grad[m], 0.0).astype(BF16)

    def backward(m, carry):
        def chunk_of(low, size):
            k = [c[0] for c in CHUNKS].index(low)

            @pl.when(me < count - 1)
            def _():
                back_hop(m, k).wait_recv()

            return grads[m, :, low : low + size]

        context_grad = context_gradient(chunk_of, wo)
        projected_grad, product = attend_back(
            context_grad, saved[m], prob[m], cosine[...], sine[...], tpu_roll
        )
        inverse = inverses[m]
        lean = inverse * inverse * product * (1.0 / 3584)
        for k, (low, size) in enumerate(CHUNKS):
            normed_grad = nt(projected_grad, wq[low : low + size, :])
            grad_out[m, :, low : low + size] = (
                grads[m, :, low : low + size].astype(F32)
                + normed_grad * gain[:, low : low + size] * inverse
                - hidden[m, :, low : low + size].astype(F32) * lean
            ).astype(BF16)
            if k == 0:
                take_turn(count - 1, b_turn, m)

            @pl.when(me > 0)
            def _():
                back_hop(m, k).start()

        give_turn(count - 1, b_turn, m, back_hop)
        return carry

    lax.fori_loop(0, micros, backward, 0)

    @pl.when(jnp.logical_and(me > 0, me < count - 1))
    def _():
        for m in range(micros):
            for k in range(len(CHUNKS)):
                back_hop(m, k).wait_send()


def whole():
    return pl.BlockSpec(memory_space=pltpu.VMEM)


def turning(length):
    half = HEAD_DIM // 2
    frequency = rope_base ** (-np.arange(half, dtype=np.float32) * np.float32(2.0 / HEAD_DIM))
    angles = np.arange(length, dtype=np.float32)[:, None] * frequency[None, :].astype(np.float32)
    cosine, sine = np.cos(angles), np.sin(angles)
    return (
        np.concatenate([cosine] * 4, axis=1).astype(np.float32),
        np.concatenate([-sine, sine] * 2, axis=1).astype(np.float32),
    )


def per_device(entry, norm_gain, w_qkv, w_out, final_gain, lengths, positive):
    width = entry.shape[1]
    seqs = lengths.shape[0]
    length = entry.shape[0] // seqs
    cosine, sine = turning(length)
    packed = np.arange(224)
    spread_rows = np.arange(256)[None, :] == (packed // 28 * 32 + packed % 28)[:, None]
    block = (seqs, length, width)
    dma = pltpu.SemaphoreType.DMA
    args = (
        lengths, positive,
        entry.reshape(block), norm_gain, w_qkv[0], w_out[0],
        jnp.asarray(cosine), jnp.asarray(sine), final_gain,
        jnp.asarray(spread_rows.astype(np.float32), dtype=BF16),
    )
    small = pl.BlockSpec(memory_space=pltpu.SMEM)
    chunks = len(CHUNKS)
    grads = pl.pallas_call(
        step_kernel,
        out_shape=jax.ShapeDtypeStruct(block, BF16),
        in_specs=[small] * 2 + [whole()] * (len(args) - 2),
        out_specs=whole(),
        scratch_shapes=[
            pltpu.VMEM((width, 1152), BF16),
            pltpu.VMEM((1024, width), BF16),
            pltpu.VMEM((896, width), BF16),
            pltpu.VMEM(block, BF16),
            pltpu.VMEM((seqs, length, 1152), BF16),
            pltpu.VMEM((seqs, PAIRS * length, 2 * length), BF16),
            pltpu.VMEM((seqs, length, 1), F32),
            pltpu.VMEM((seqs, 1, width), F32),
            pltpu.VMEM((seqs, 1, width), F32),
            pltpu.VMEM((32, 16, 1024), BF16),
            pltpu.VMEM((16, 1024), BF16),
            pltpu.VMEM(block, BF16),
            pltpu.VMEM(block, BF16),
            dma((GATHER_SENDS,)), dma((16, 2)), dma((16,)),
            dma((GATHER_SENDS,)), dma((16, 2)), dma((16,)),
            dma((31,)), dma((16,)), dma((16,)),
            dma((seqs, chunks)), dma((seqs, chunks)), dma((seqs, chunks)), dma((seqs, chunks)),
            pltpu.SemaphoreType.REGULAR, pltpu.SemaphoreType.REGULAR,
        ],
        compiler_params=pltpu.CompilerParams(
            collective_id=0, has_side_effects=True, vmem_limit_bytes=64000 * 1024
        ),
    )(*args)
    return grads.reshape(1, seqs * length, width)


def solution(mesh):
    finer = Mesh(
        mesh.devices.reshape(mesh.shape["section"], 4, 4, 2), ("section", "dp_0", "dp_1", "dp_2")
    )
    in_specs = (
        P(DP, None),
        P("section", None),
        P("section", DP, None),
        P("section", DP, None),
        P(),
        P(DP),
        P(DP),
    )
    return jax.shard_map(
        per_device, mesh=finer, in_specs=in_specs, out_specs=P("section", DP, None),
        check_vma=False,
    )
```

```python
import jax
import jax.numpy as jnp
import numpy as np
from jax import lax
from jax.experimental import pallas as pl
from jax.experimental.pallas import tpu as pltpu
from jax.sharding import Mesh
from jax.sharding import PartitionSpec as P

HEAD_DIM = 64
GROUP_HEADS = 7
KV_GROUPS = 2
DP = ("dp_0", "dp_1", "dp_2")

rope_base = 1000000.0
norm_eps = 1e-06
sharpness_divisor = 0.05
objective_coefficient = 256.0

LENGTH = 48
PAIRS = 7
F32 = jnp.float32
BF16 = jnp.bfloat16


def nn(a, b):
    return lax.dot_general(a, b, (((1,), (0,)), ((), ())), preferred_element_type=F32)


def nt(a, b):
    return lax.dot_general(a, b, (((1,), (1,)), ((), ())), preferred_element_type=F32)


def tn(a, b):
    return lax.dot_general(a, b, (((0,), (0,)), ((), ())), preferred_element_type=F32)


def lanes_of(shape):
    return lax.broadcasted_iota(jnp.int32, shape, 1)


def turned(block, cosine, sine, roll):
    lane = lanes_of(block.shape)
    swapped = jnp.where(lane % 64 < 32, roll(block, 96), roll(block, 32))
    return block * cosine + swapped * sine


def paired(rows, roll):
    lane = lanes_of(rows.shape)
    other = roll(rows, 64)
    zero = jnp.zeros_like(rows)
    low = lane < 64
    first = jnp.where(low, rows, zero)
    second = jnp.where(low, zero, rows)
    return tuple(
        jnp.concatenate(two, axis=0).astype(BF16)
        for two in (
            (first, jnp.where(low, zero, other)),
            (first, second),
            (jnp.where(low, other, zero), second),
        )
    )


SPANS = ((0, 3), (3, 4), (4, 7))


def stacked(blocks, span):
    chosen = blocks[span[0] : span[1]]
    return chosen[0] if len(chosen) == 1 else jnp.concatenate(chosen, axis=0)


CHUNKS = ((0, 512), (512, 1024), (1536, 1024), (2560, 512), (3072, 512))


def live_lanes(shape, length):
    lane = lanes_of(shape)
    return jnp.where(lane < LENGTH, lane, lane - LENGTH) < length


def is_last(length):
    return lax.broadcasted_iota(jnp.int32, (LENGTH, 1), 0) == length - 1


def project(chunk_of, gain, wq):
    squares, projected = 0.0, 0.0
    for low, size in CHUNKS:
        wide = chunk_of(low, size).astype(F32)
        squares = squares + jnp.sum(wide * wide, axis=-1, keepdims=True)
        gained = (wide * gain[:, low : low + size]).astype(BF16)
        projected = projected + nn(gained, wq[low : low + size, :])
    inverse = lax.rsqrt(squares * (1.0 / 3584) + norm_eps)
    return projected * inverse, inverse


def attend(projected, length, cosine, sine, roll):
    blocks = [projected[:, 128 * b : 128 * (b + 1)] for b in range(9)]
    turned_blocks = [turned(b, cosine, sine, roll) for b in blocks[:8]]
    queries = [b.astype(BF16) for b in turned_blocks[:PAIRS]]
    keys = turned_blocks[PAIRS].astype(BF16)
    values = blocks[8].astype(BF16)
    key_forms = paired(keys.astype(F32), roll)
    value_forms = paired(values.astype(F32), roll)
    probabilities = []
    context = []
    for span, key_form, value_form in zip(SPANS, key_forms, value_forms):
        scores = nt(stacked(queries, span), key_form) * HEAD_DIM ** (-0.5)
        weights = jnp.where(live_lanes(scores.shape, length), jnp.exp(scores), 0.0)
        low = lanes_of(weights.shape) < LENGTH
        sum_low = jnp.sum(jnp.where(low, weights, 0.0), axis=-1, keepdims=True)
        sum_high = jnp.sum(jnp.where(low, 0.0, weights), axis=-1, keepdims=True)
        probability = (weights * jnp.where(low, 1.0 / sum_low, 1.0 / sum_high)).astype(BF16)
        probabilities.append(probability)
        result = nn(probability, value_form).astype(BF16)
        for i in range(span[1] - span[0]):
            context.append(result[LENGTH * i : LENGTH * (i + 1)])
    saved = jnp.concatenate(queries + [keys, values], axis=1)
    return jnp.concatenate(context, axis=1), saved, jnp.concatenate(probabilities, axis=0)


def context_gradient(chunk_of, wo):
    total = 0.0
    for low, size in CHUNKS:
        total = total + nt(chunk_of(low, size), wo[:, low : low + size])
    return total.astype(BF16)


def attend_back(context_grad, saved, probabilities, cosine, sine, roll):
    context_grads = [context_grad[:, 128 * b : 128 * (b + 1)] for b in range(PAIRS)]
    queries = [saved[:, 128 * b : 128 * (b + 1)] for b in range(PAIRS)]
    key_forms = paired(saved[:, 896:1024].astype(F32), roll)
    value_forms = paired(saved[:, 1024:1152].astype(F32), roll)
    query_grads = []
    key_parts = []
    value_parts = []
    for span, key_form, value_form in zip(SPANS, key_forms, value_forms):
        chosen = stacked(context_grads, span)
        probability = probabilities[LENGTH * span[0] : LENGTH * span[1]]
        wide_p = probability.astype(F32)
        prob_grad = nt(chosen, value_form)
        product = prob_grad * wide_p
        low = lanes_of(product.shape) < LENGTH
        sum_low = jnp.sum(jnp.where(low, product, 0.0), axis=-1, keepdims=True)
        sum_high = jnp.sum(jnp.where(low, 0.0, product), axis=-1, keepdims=True)
        score_grad = (
            wide_p * (prob_grad - jnp.where(low, sum_low, sum_high)) * HEAD_DIM ** (-0.5)
        ).astype(BF16)
        query_grad = nn(score_grad, key_form)
        for i in range(span[1] - span[0]):
            query_grads.append(query_grad[LENGTH * i : LENGTH * (i + 1)])
        key_parts.append(tn(score_grad, stacked(queries, span)))
        value_parts.append(tn(probability, chosen))

    def folded(parts):
        both, mixed, last = parts
        low_part = both[:LENGTH] + roll(both[LENGTH:], 64) + mixed[:LENGTH]
        high_part = mixed[LENGTH:] + last[LENGTH:] + roll(last[:LENGTH], 64)
        return jnp.where(lanes_of(low_part.shape) < 64, low_part, high_part)

    grads = [
        block.astype(BF16).astype(F32)
        for block in query_grads + [folded(key_parts), folded(value_parts)]
    ]
    product = 0.0
    for b, block in enumerate(grads):
        product = product + block * saved[:, 128 * b : 128 * (b + 1)].astype(F32)
    turned_back = [turned(block, cosine, -sine, roll).astype(BF16) for block in grads[:8]]
    projected_grad = jnp.concatenate(turned_back + [grads[8].astype(BF16)], axis=1)
    return projected_grad, jnp.sum(product, axis=-1, keepdims=True)


def tpu_roll(x, shift):
    return pltpu.roll(x, shift, axis=1)


def remote(source, target, send, receive, place):
    return pltpu.make_async_remote_copy(
        src_ref=source,
        dst_ref=target,
        send_sem=send,
        recv_sem=receive,
        device_id=place,
        device_id_type=pl.DeviceIdType.MESH,
    )


class Plane:
    def __init__(self, flipped=False):
        self.x = lax.axis_index("dp_0")
        self.y = lax.axis_index("dp_1")
        self.core = lax.axis_index("dp_2")
        self.turned = 1 - self.core if flipped else self.core

    def spot(self, first, second):
        other = 1 - self.turned
        return (
            lax.rem(self.x + first * other + second * self.turned, 4),
            lax.rem(self.y + first * self.turned + second * other, 4),
        )

    def slot(self, first, second, mine=True):
        x, y = self.spot(first % 4, second % 4)
        core = self.core if mine else 1 - self.core
        return (x * 4 + y) * 2 + core

    def device(self, first, second):
        x, y = self.spot(first % 4, second % 4)
        return {"dp_0": x, "dp_1": y}

    def partner_slot(self, x, y):
        return (x * 4 + y) * 2 + (1 - self.core)

    def partner(self):
        return {"dp_2": 1 - self.core}


def start_meeting(plane):
    me = lax.axis_index("section")
    count = lax.axis_size("section")
    barrier = pltpu.get_barrier_semaphore()
    places = [{"section": lax.rem(me + step, count)} for step in (1, count - 1)]
    places.append(plane.partner())
    places += [plane.device(a, b) for a in range(4) for b in range(4) if a or b]
    for place in places:
        pl.semaphore_signal(
            barrier, inc=1, device_id=place, device_id_type=pl.DeviceIdType.MESH
        )
    return barrier, len(places)


class Gather:
    def __init__(self, plane, whole, rows, cut, sends, receives, partner_receives):
        self.plane, self.whole = plane, whole
        self.rows, self.cut = rows, cut
        self.sends, self.receives = sends, receives
        self.partner_receives = partner_receives
        self.started = []

    def part(self, slot, half):
        low, size = ((0, self.rows), (0, self.cut), (self.cut, self.rows - self.cut))[half]
        return self.whole.at[pl.ds(pl.multiple_of(slot * self.rows + low, 16), size)]

    def send(self, slot, half, place, receives=None):
        target = self.part(slot, half)
        receives = self.receives.at[slot // 2, max(half - 1, 0)] if receives is None else receives
        copy = remote(
            target,
            target,
            self.sends.at[len(self.started)],
            receives,
            place,
        )
        copy.start()
        self.started.append(copy)

    def hand_over(self, slot):
        self.send(slot, 0, self.plane.partner(), self.partner_receives.at[slot // 2])

    def arrived(self, slot, half):
        part = self.part(slot, half)
        remote(
            part, part, self.sends.at[0], self.receives.at[slot // 2, max(half - 1, 0)],
            self.plane.partner(),
        ).wait_recv()

    def begin(self):
        plane = self.plane
        slot = plane.slot(0, 0)
        for step in (1, -1):
            self.send(slot, 0, plane.device(step, 0))
            self.send(slot, 0, plane.device(0, step))
        self.hand_over(slot)

    def first_near(self):
        plane = self.plane
        for step, half in ((-1, 1), (1, 2)):
            slot = plane.slot(step, 0)
            self.arrived(slot, 0)
            self.send(slot, half, plane.device(-step, 0))
            self.spread(slot)

    def first_far(self):
        slot = self.plane.slot(2, 0)
        self.arrived(slot, 1)
        self.arrived(slot, 2)
        self.spread(slot)

    def spread(self, slot):
        for step in (1, -1):
            self.send(slot, 0, self.plane.device(0, step))
        self.hand_over(slot)

    def second_near(self, first):
        plane = self.plane
        for step, half in ((-1, 1), (1, 2)):
            slot = plane.slot(first, step)
            self.arrived(slot, 0)
            self.send(slot, half, plane.device(0, -step))
            self.hand_over(slot)

    def second_far(self, first):
        slot = self.plane.slot(first, 2)
        self.arrived(slot, 1)
        self.arrived(slot, 2)
        self.hand_over(slot)

    def from_partner(self, b):
        for at in range(4 * b, 4 * b + 4):
            part = self.part(self.plane.partner_slot(at // 4, at % 4), 0)
            remote(
                part, part, self.sends.at[0], self.partner_receives.at[at],
                self.plane.partner(),
            ).wait_recv()

    def drain(self):
        for copy in self.started:
            copy.wait_send()


GATHER_SENDS = 36


def contrast(plane, last_rows, final_gain, positive, gathered, outgoing, sends, receives,
             partner_receives, last_grad):
    rows = jnp.concatenate([last_rows[m] for m in range(4)], axis=0)
    gain = final_gain[...].reshape(1, -1)
    inverse = lax.rsqrt(jnp.mean(rows * rows, axis=-1, keepdims=True) + norm_eps)
    pooled = rows * inverse * gain
    scale = lax.rsqrt(jnp.sum(pooled * pooled, axis=-1, keepdims=True))
    embedding = pooled * scale
    spot = lax.broadcasted_iota(jnp.int32, (4, 128), 0)
    tail = jnp.where(spot < 2, positive[0], positive[1]).astype(F32)
    packed = jnp.concatenate(
        [
            jnp.concatenate([embedding[:, 896 * k : 896 * (k + 1)], tail], axis=1)
            for k in range(4)
        ],
        axis=0,
    ).astype(BF16)
    outgoing[...] = packed
    mine = plane.slot(0, 0)
    gathered[mine] = packed
    started = []

    def send(source, slot, receive, place):
        copy = remote(source, gathered.at[slot], sends.at[len(started)], receive, place)
        copy.start()
        started.append(copy)

    others = [(a, b) for a in range(4) for b in range(4) if a or b]
    others.sort(key=lambda ab: min(ab[0], 4 - ab[0]) + min(ab[1], 4 - ab[1]))
    for a, b in reversed(others):
        send(outgoing, mine, receives.at[mine // 2], plane.device(a, b))
    send(outgoing, mine, partner_receives.at[mine // 2], plane.partner())
    for a, b in others:
        slot = plane.slot(a, b)
        remote(
            outgoing, gathered.at[slot], sends.at[0], receives.at[slot // 2], plane.partner()
        ).wait_recv()
        send(gathered.at[slot], slot, partner_receives.at[slot // 2], plane.partner())
    for at in range(16):
        slot = plane.partner_slot(at // 4, at % 4)
        remote(
            outgoing, gathered.at[slot], sends.at[0], partner_receives.at[at], plane.partner()
        ).wait_recv()
    for copy in started:
        copy.wait_send()

    flat = jnp.concatenate([gathered[i] for i in range(32)], axis=0)
    at = lax.broadcasted_iota(jnp.int32, (128, 512), 0)
    lane = lanes_of((128, 512))
    number = at & 63
    row = (number >> 1) * 16 + (number & 1) * 2 + (at >> 6)
    pieces = []
    for k in range(4):
        chosen = jnp.where(lane == row + 4 * k, 1.0, 0.0).astype(BF16)
        pieces.append(nn(chosen, flat))
    everyone = jnp.concatenate([p[:, :896] for p in pieces], axis=1).astype(BF16)
    target = pieces[0][:64, 896:960]
    logits = nt(everyone[:64], everyone[64:]) * (1.0 / sharpness_divisor)
    weights = jnp.exp(logits)
    odds = weights / jnp.sum(weights, axis=-1, keepdims=True)
    column = lanes_of((64, 64))
    hit = jnp.where(target == column.astype(F32), 1.0, 0.0)
    coefficient = (odds - hit) * (objective_coefficient / sharpness_divisor)
    turned_coefficient = coefficient.T
    line = lax.broadcasted_iota(jnp.int32, (64, 64), 0)
    blank = jnp.zeros((1, 64), F32)
    replica = mine
    chosen_rows = []
    for m in range(4):
        source = turned_coefficient if m % 2 else coefficient
        one = jnp.sum(
            jnp.where(line == replica * 2 + m // 2, source, 0.0), axis=0, keepdims=True
        )
        chosen_rows.append(jnp.concatenate([one, blank] if m % 2 else [blank, one], axis=1))
    exact = jnp.concatenate(chosen_rows, axis=0)
    top = exact.astype(BF16)
    rest = exact - top.astype(F32)
    middle = rest.astype(BF16)
    low = (rest - middle.astype(F32)).astype(BF16)
    embed_grad = nn(top, everyone) + nn(middle, everyone) + nn(low, everyone)
    pooled_grad = embed_grad * scale - pooled * (
        scale * scale * scale * jnp.sum(embed_grad * pooled, axis=-1, keepdims=True)
    )
    gained = pooled_grad * gain
    row_grad = gained * inverse - rows * (
        inverse * inverse * inverse * jnp.mean(gained * rows, axis=-1, keepdims=True)
    )
    for m in range(4):
        last_grad[m] = row_grad[m : m + 1]


def step_kernel(
    lengths, positive, entry, gain, wq_own, wo_own, cosine, sine, final_gain, spread_rows,
    grad_out,
    wq, wo_spaced, wo, hidden, saved, prob, inverses, last_rows, last_grad, embeds, embed_own,
    outbox, grads,
    wq_send, wq_recv, wq_cross, wo_send, wo_recv, wo_cross, e_send, e_recv, e_cross,
    f_send, f_recv, b_send, b_recv,
):
    me = lax.axis_index("section")
    count = lax.axis_size("section")
    micros = entry.shape[0]
    plane = Plane()
    mine = plane.slot(0, 0)
    barrier, greetings = start_meeting(plane)
    wq[pl.ds(pl.multiple_of(mine * 112, 16), 112)] = wq_own[...]
    wo_spaced[pl.ds(pl.multiple_of(mine * 32, 16), 32)] = jnp.concatenate(
        [wo_own[...], jnp.zeros((4, wo_own.shape[1]), BF16)], axis=0
    )
    pl.semaphore_wait(barrier, greetings)
    gathers = (
        Gather(plane, wq, 112, 64, wq_send, wq_recv, wq_cross),
        Gather(Plane(flipped=True), wo_spaced, 32, 16, wo_send, wo_recv, wo_cross),
    )
    for gather in gathers:
        gather.begin()

    @pl.when(me == 0)
    def _():
        hidden[...] = entry[...]

    for gather in gathers:
        gather.first_near()
    for gather in gathers:
        gather.second_near(0)
    for gather in gathers:
        gather.first_far()
    for first in (-1, 1, 2):
        for gather in gathers:
            gather.second_near(first)
    for gather in gathers:
        for first in (0, -1, 1, 2):
            gather.second_far(first)
    for b in range(4):
        gathers[1].from_partner(b)
        spaced = wo_spaced[256 * b : 256 * (b + 1)]
        wo[224 * b : 224 * (b + 1)] = nn(spread_rows[...], spaced).astype(BF16)
    for b in range(4):
        gathers[0].from_partner(b)
    for gather in gathers:
        gather.drain()

    def hop(m, k):
        low, size = CHUNKS[k]
        return remote(
            outbox.at[m, :, pl.ds(low, size)], hidden.at[m, :, pl.ds(low, size)],
            f_send.at[m, k], f_recv.at[m, k], {"section": lax.rem(me + 1, count)},
        )

    def back_hop(m, k):
        low, size = CHUNKS[k]
        return remote(
            grad_out.at[m, :, pl.ds(low, size)], grads.at[m, :, pl.ds(low, size)],
            b_send.at[m, k], b_recv.at[m, k], {"section": lax.rem(me + count - 1, count)},
        )

    def forward(m, carry):
        length = lengths[m]

        def chunk_of(low, size):
            k = [c[0] for c in CHUNKS].index(low)

            @pl.when(me > 0)
            def _():
                hop(m, k).wait_recv()

            return hidden[m, :, low : low + size]

        projected, inverse = project(chunk_of, gain, wq)
        inverses[m] = inverse
        context, kept, probabilities = attend(
            projected, length, cosine[...], sine[...], tpu_roll
        )
        last = is_last(length)
        for k, (low, size) in enumerate(CHUNKS):
            wide = hidden[m, :, low : low + size].astype(F32)
            following = (wide + nn(context, wo[:, low : low + size])).astype(BF16)
            outbox[m, :, low : low + size] = following

            @pl.when(me < count - 1)
            def _():
                hop(m, k).start()

            last_rows[m, :, low : low + size] = jnp.sum(
                jnp.where(last, following.astype(F32), 0.0), axis=0, keepdims=True
            )
        saved[m] = kept
        prob[m] = probabilities
        return carry

    lax.fori_loop(0, micros, forward, 0)

    @pl.when(me < count - 1)
    def _():
        for m in range(micros):
            for k in range(len(CHUNKS)):
                hop(m, k).wait_send()

    @pl.when(me == count - 1)
    def _():
        contrast(plane, last_rows, final_gain, positive, embeds, embed_own, e_send, e_recv,
                 e_cross, last_grad)
        for m in range(micros):
            grads[m] = jnp.where(is_last(lengths[m]), last_grad[m], 0.0).astype(BF16)

    def backward(m, carry):
        def chunk_of(low, size):
            k = [c[0] for c in CHUNKS].index(low)

            @pl.when(me < count - 1)
            def _():
                back_hop(m, k).wait_recv()

            return grads[m, :, low : low + size]

        context_grad = context_gradient(chunk_of, wo)
        projected_grad, product = attend_back(
            context_grad, saved[m], prob[m], cosine[...], sine[...], tpu_roll
        )
        inverse = inverses[m]
        lean = inverse * inverse * product * (1.0 / 3584)
        for k, (low, size) in enumerate(CHUNKS):
            normed_grad = nt(projected_grad, wq[low : low + size, :])
            grad_out[m, :, low : low + size] = (
                grads[m, :, low : low + size].astype(F32)
                + normed_grad * gain[:, low : low + size] * inverse
                - hidden[m, :, low : low + size].astype(F32) * lean
            ).astype(BF16)

            @pl.when(me > 0)
            def _():
                back_hop(m, k).start()

        return carry

    lax.fori_loop(0, micros, backward, 0)

    @pl.when(me > 0)
    def _():
        for m in range(micros):
            for k in range(len(CHUNKS)):
                back_hop(m, k).wait_send()


def whole():
    return pl.BlockSpec(memory_space=pltpu.VMEM)


def turning(length):
    half = HEAD_DIM // 2
    frequency = rope_base ** (-np.arange(half, dtype=np.float32) * np.float32(2.0 / HEAD_DIM))
    angles = np.arange(length, dtype=np.float32)[:, None] * frequency[None, :].astype(np.float32)
    cosine, sine = np.cos(angles), np.sin(angles)
    return (
        np.concatenate([cosine] * 4, axis=1).astype(np.float32),
        np.concatenate([-sine, sine] * 2, axis=1).astype(np.float32),
    )


def per_device(entry, norm_gain, w_qkv, w_out, final_gain, lengths, positive):
    width = entry.shape[1]
    seqs = lengths.shape[0]
    length = entry.shape[0] // seqs
    cosine, sine = turning(length)
    packed = np.arange(224)
    spread_rows = np.arange(256)[None, :] == (packed // 28 * 32 + packed % 28)[:, None]
    block = (seqs, length, width)
    dma = pltpu.SemaphoreType.DMA
    args = (
        lengths, positive,
        entry.reshape(block), norm_gain, w_qkv[0], w_out[0],
        jnp.asarray(cosine), jnp.asarray(sine), final_gain,
        jnp.asarray(spread_rows.astype(np.float32), dtype=BF16),
    )
    small = pl.BlockSpec(memory_space=pltpu.SMEM)
    chunks = len(CHUNKS)
    grads = pl.pallas_call(
        step_kernel,
        out_shape=jax.ShapeDtypeStruct(block, BF16),
        in_specs=[small] * 2 + [whole()] * (len(args) - 2),
        out_specs=whole(),
        scratch_shapes=[
            pltpu.VMEM((width, 1152), BF16),
            pltpu.VMEM((1024, width), BF16),
            pltpu.VMEM((896, width), BF16),
            pltpu.VMEM(block, BF16),
            pltpu.VMEM((seqs, length, 1152), BF16),
            pltpu.VMEM((seqs, PAIRS * length, 2 * length), BF16),
            pltpu.VMEM((seqs, length, 1), F32),
            pltpu.VMEM((seqs, 1, width), F32),
            pltpu.VMEM((seqs, 1, width), F32),
            pltpu.VMEM((32, 16, 1024), BF16),
            pltpu.VMEM((16, 1024), BF16),
            pltpu.VMEM(block, BF16),
            pltpu.VMEM(block, BF16),
            dma((GATHER_SENDS,)), dma((16, 2)), dma((16,)),
            dma((GATHER_SENDS,)), dma((16, 2)), dma((16,)),
            dma((31,)), dma((16,)), dma((16,)),
            dma((seqs, chunks)), dma((seqs, chunks)), dma((seqs, chunks)), dma((seqs, chunks)),
        ],
        compiler_params=pltpu.CompilerParams(
            collective_id=0, has_side_effects=True, vmem_limit_bytes=64000 * 1024
        ),
    )(*args)
    return grads.reshape(1, seqs * length, width)


def solution(mesh):
    finer = Mesh(
        mesh.devices.reshape(mesh.shape["section"], 4, 4, 2), ("section", "dp_0", "dp_1", "dp_2")
    )
    in_specs = (
        P(DP, None),
        P("section", None),
        P("section", DP, None),
        P("section", DP, None),
        P(),
        P(DP),
        P(DP),
    )
    return jax.shard_map(
        per_device, mesh=finer, in_specs=in_specs, out_specs=P("section", DP, None),
        check_vma=False,
    )
```

```python
import jax
import jax.numpy as jnp
import numpy as np
from jax import lax
from jax.experimental import pallas as pl
from jax.experimental.pallas import tpu as pltpu
from jax.sharding import Mesh
from jax.sharding import PartitionSpec as P

HEAD_DIM = 64
GROUP_HEADS = 7
KV_GROUPS = 2
DP = ("dp_0", "dp_1", "dp_2")

rope_base = 1000000.0
norm_eps = 1e-06
sharpness_divisor = 0.05
objective_coefficient = 256.0

LENGTH = 48
EARLY = 2
PAIRS = 7
F32 = jnp.float32
BF16 = jnp.bfloat16


def nn(a, b):
    return lax.dot_general(a, b, (((1,), (0,)), ((), ())), preferred_element_type=F32)


def nt(a, b):
    return lax.dot_general(a, b, (((1,), (1,)), ((), ())), preferred_element_type=F32)


def tn(a, b):
    return lax.dot_general(a, b, (((0,), (0,)), ((), ())), preferred_element_type=F32)


def lanes_of(shape):
    return lax.broadcasted_iota(jnp.int32, shape, 1)


def turned(block, cosine, sine, roll):
    lane = lanes_of(block.shape)
    swapped = jnp.where(lane % 64 < 32, roll(block, 96), roll(block, 32))
    return block * cosine + swapped * sine


def paired(rows, roll):
    lane = lanes_of(rows.shape)
    other = roll(rows, 64)
    zero = jnp.zeros_like(rows)
    low = lane < 64
    first = jnp.where(low, rows, zero)
    second = jnp.where(low, zero, rows)
    return tuple(
        jnp.concatenate(two, axis=0).astype(BF16)
        for two in (
            (first, jnp.where(low, zero, other)),
            (first, second),
            (jnp.where(low, other, zero), second),
        )
    )


SPANS = ((0, 3), (3, 4), (4, 7))


def stacked(blocks, span):
    chosen = blocks[span[0] : span[1]]
    return chosen[0] if len(chosen) == 1 else jnp.concatenate(chosen, axis=0)


CHUNKS = ((0, 512), (512, 2048), (2560, 1024))
BACK_CHUNKS = ((0, 512), (512, 1024), (1536, 1280), (2816, 768))


def live_lanes(shape, length):
    lane = lanes_of(shape)
    return jnp.where(lane < LENGTH, lane, lane - LENGTH) < length


def is_last(length):
    return lax.broadcasted_iota(jnp.int32, (LENGTH, 1), 0) == length - 1


def project(chunk_of, gain, wq):
    squares, projected = 0.0, 0.0
    for low, size in CHUNKS:
        wide = chunk_of(low, size).astype(F32)
        squares = squares + jnp.sum(wide * wide, axis=-1, keepdims=True)
        gained = (wide * gain[:, low : low + size]).astype(BF16)
        projected = projected + nn(gained, wq[low : low + size, :])
    inverse = lax.rsqrt(squares * (1.0 / 3584) + norm_eps)
    return projected * inverse, inverse


def attend(projected, length, cosine, sine, roll):
    blocks = [projected[:, 128 * b : 128 * (b + 1)] for b in range(9)]
    turned_blocks = [turned(b, cosine, sine, roll) for b in blocks[:8]]
    queries = [b.astype(BF16) for b in turned_blocks[:PAIRS]]
    keys = turned_blocks[PAIRS].astype(BF16)
    values = blocks[8].astype(BF16)
    key_forms = paired(keys.astype(F32), roll)
    value_forms = paired(values.astype(F32), roll)
    probabilities = []
    context = []
    for span, key_form, value_form in zip(SPANS, key_forms, value_forms):
        scores = nt(stacked(queries, span), key_form) * HEAD_DIM ** (-0.5)
        weights = jnp.where(live_lanes(scores.shape, length), jnp.exp(scores), 0.0)
        low = lanes_of(weights.shape) < LENGTH
        sum_low = jnp.sum(jnp.where(low, weights, 0.0), axis=-1, keepdims=True)
        sum_high = jnp.sum(jnp.where(low, 0.0, weights), axis=-1, keepdims=True)
        probability = (weights * jnp.where(low, 1.0 / sum_low, 1.0 / sum_high)).astype(BF16)
        probabilities.append(probability)
        result = nn(probability, value_form).astype(BF16)
        for i in range(span[1] - span[0]):
            context.append(result[LENGTH * i : LENGTH * (i + 1)])
    saved = jnp.concatenate(queries + [keys, values], axis=1)
    return jnp.concatenate(context, axis=1), saved, jnp.concatenate(probabilities, axis=0)


def context_gradient(chunk_of, wo):
    total = 0.0
    for low, size in BACK_CHUNKS:
        total = total + nt(chunk_of(low, size), wo[:, low : low + size])
    return total.astype(BF16)


def attend_back(context_grad, saved, probabilities, cosine, sine, roll):
    context_grads = [context_grad[:, 128 * b : 128 * (b + 1)] for b in range(PAIRS)]
    queries = [saved[:, 128 * b : 128 * (b + 1)] for b in range(PAIRS)]
    key_forms = paired(saved[:, 896:1024].astype(F32), roll)
    value_forms = paired(saved[:, 1024:1152].astype(F32), roll)
    query_grads = []
    key_parts = []
    value_parts = []
    for span, key_form, value_form in zip(SPANS, key_forms, value_forms):
        chosen = stacked(context_grads, span)
        probability = probabilities[LENGTH * span[0] : LENGTH * span[1]]
        wide_p = probability.astype(F32)
        prob_grad = nt(chosen, value_form)
        product = prob_grad * wide_p
        low = lanes_of(product.shape) < LENGTH
        sum_low = jnp.sum(jnp.where(low, product, 0.0), axis=-1, keepdims=True)
        sum_high = jnp.sum(jnp.where(low, 0.0, product), axis=-1, keepdims=True)
        score_grad = (
            wide_p * (prob_grad - jnp.where(low, sum_low, sum_high)) * HEAD_DIM ** (-0.5)
        ).astype(BF16)
        query_grad = nn(score_grad, key_form)
        for i in range(span[1] - span[0]):
            query_grads.append(query_grad[LENGTH * i : LENGTH * (i + 1)])
        key_parts.append(tn(score_grad, stacked(queries, span)))
        value_parts.append(tn(probability, chosen))

    def folded(parts):
        both, mixed, last = parts
        low_part = both[:LENGTH] + roll(both[LENGTH:], 64) + mixed[:LENGTH]
        high_part = mixed[LENGTH:] + last[LENGTH:] + roll(last[:LENGTH], 64)
        return jnp.where(lanes_of(low_part.shape) < 64, low_part, high_part)

    grads = [
        block.astype(BF16).astype(F32)
        for block in query_grads + [folded(key_parts), folded(value_parts)]
    ]
    product = 0.0
    for b, block in enumerate(grads):
        product = product + block * saved[:, 128 * b : 128 * (b + 1)].astype(F32)
    turned_back = [turned(block, cosine, -sine, roll).astype(BF16) for block in grads[:8]]
    projected_grad = jnp.concatenate(turned_back + [grads[8].astype(BF16)], axis=1)
    return projected_grad, jnp.sum(product, axis=-1, keepdims=True)


def tpu_roll(x, shift):
    return pltpu.roll(x, shift, axis=1)


def remote(source, target, send, receive, place):
    return pltpu.make_async_remote_copy(
        src_ref=source,
        dst_ref=target,
        send_sem=send,
        recv_sem=receive,
        device_id=place,
        device_id_type=pl.DeviceIdType.MESH,
    )


class Plane:
    def __init__(self, flipped=False):
        self.x = lax.axis_index("dp_0")
        self.y = lax.axis_index("dp_1")
        self.core = lax.axis_index("dp_2")
        self.turned = 1 - self.core if flipped else self.core

    def spot(self, first, second):
        other = 1 - self.turned
        return (
            lax.rem(self.x + first * other + second * self.turned, 4),
            lax.rem(self.y + first * self.turned + second * other, 4),
        )

    def slot(self, first, second, mine=True):
        x, y = self.spot(first % 4, second % 4)
        core = self.core if mine else 1 - self.core
        return (x * 4 + y) * 2 + core

    def device(self, first, second):
        x, y = self.spot(first % 4, second % 4)
        return {"dp_0": x, "dp_1": y}

    def partner_slot(self, x, y):
        return (x * 4 + y) * 2 + (1 - self.core)

    def partner(self):
        return {"dp_2": 1 - self.core}


def start_meeting(plane):
    me = lax.axis_index("section")
    count = lax.axis_size("section")
    barrier = pltpu.get_barrier_semaphore()
    places = [{"section": lax.rem(me + step, count)} for step in (1, count - 1)]
    places.append(plane.partner())
    places += [plane.device(a, b) for a in range(4) for b in range(4) if a or b]
    for place in places:
        pl.semaphore_signal(
            barrier, inc=1, device_id=place, device_id_type=pl.DeviceIdType.MESH
        )
    return barrier, len(places)


class Gather:
    def __init__(self, plane, whole, rows, cut, sends, receives, partner_receives):
        self.plane, self.whole = plane, whole
        self.rows, self.cut = rows, cut
        self.sends, self.receives = sends, receives
        self.partner_receives = partner_receives
        self.started = []

    def part(self, slot, half):
        low, size = ((0, self.rows), (0, self.cut), (self.cut, self.rows - self.cut))[half]
        return self.whole.at[pl.ds(pl.multiple_of(slot * self.rows + low, 16), size)]

    def send(self, slot, half, place, receives=None):
        target = self.part(slot, half)
        receives = self.receives.at[slot // 2, max(half - 1, 0)] if receives is None else receives
        copy = remote(
            target,
            target,
            self.sends.at[len(self.started)],
            receives,
            place,
        )
        copy.start()
        self.started.append(copy)

    def hand_over(self, slot):
        self.send(slot, 0, self.plane.partner(), self.partner_receives.at[slot // 2])

    def arrived(self, slot, half):
        part = self.part(slot, half)
        remote(
            part, part, self.sends.at[0], self.receives.at[slot // 2, max(half - 1, 0)],
            self.plane.partner(),
        ).wait_recv()

    def begin(self):
        plane = self.plane
        slot = plane.slot(0, 0)
        for step in (1, -1):
            self.send(slot, 0, plane.device(step, 0))
            self.send(slot, 0, plane.device(0, step))
        self.hand_over(slot)

    def first_near(self):
        plane = self.plane
        for step, half in ((-1, 1), (1, 2)):
            slot = plane.slot(step, 0)
            self.arrived(slot, 0)
            self.send(slot, half, plane.device(-step, 0))
            self.spread(slot)

    def first_far(self):
        slot = self.plane.slot(2, 0)
        self.arrived(slot, 1)
        self.arrived(slot, 2)
        self.spread(slot)

    def spread(self, slot):
        for step in (1, -1):
            self.send(slot, 0, self.plane.device(0, step))
        self.hand_over(slot)

    def second_near(self, first):
        plane = self.plane
        for step, half in ((-1, 1), (1, 2)):
            slot = plane.slot(first, step)
            self.arrived(slot, 0)
            self.send(slot, half, plane.device(0, -step))
            self.hand_over(slot)

    def second_far(self, first):
        slot = self.plane.slot(first, 2)
        self.arrived(slot, 1)
        self.arrived(slot, 2)
        self.hand_over(slot)

    def from_partner(self, b):
        for at in range(4 * b, 4 * b + 4):
            part = self.part(self.plane.partner_slot(at // 4, at % 4), 0)
            remote(
                part, part, self.sends.at[0], self.partner_receives.at[at],
                self.plane.partner(),
            ).wait_recv()

    def drain(self):
        for copy in self.started:
            copy.wait_send()


GATHER_SENDS = 36


def contrast(plane, last_rows, final_gain, positive, gathered, outgoing, sends, receives,
             partner_receives, last_grad):
    rows = jnp.concatenate([last_rows[m] for m in range(4)], axis=0)
    gain = final_gain[...].reshape(1, -1)
    inverse = lax.rsqrt(jnp.mean(rows * rows, axis=-1, keepdims=True) + norm_eps)
    pooled = rows * inverse * gain
    scale = lax.rsqrt(jnp.sum(pooled * pooled, axis=-1, keepdims=True))
    embedding = pooled * scale
    spot = lax.broadcasted_iota(jnp.int32, (4, 128), 0)
    tail = jnp.where(spot < 2, positive[0], positive[1]).astype(F32)
    packed = jnp.concatenate(
        [
            jnp.concatenate([embedding[:, 896 * k : 896 * (k + 1)], tail], axis=1)
            for k in range(4)
        ],
        axis=0,
    ).astype(BF16)
    outgoing[...] = packed
    mine = plane.slot(0, 0)
    gathered[mine] = packed
    started = []

    def send(source, slot, receive, place):
        copy = remote(source, gathered.at[slot], sends.at[len(started)], receive, place)
        copy.start()
        started.append(copy)

    others = [(a, b) for a in range(4) for b in range(4) if a or b]
    others.sort(key=lambda ab: min(ab[0], 4 - ab[0]) + min(ab[1], 4 - ab[1]))
    for a, b in reversed(others):
        send(outgoing, mine, receives.at[mine // 2], plane.device(a, b))
    send(outgoing, mine, partner_receives.at[mine // 2], plane.partner())
    for a, b in others:
        slot = plane.slot(a, b)
        remote(
            outgoing, gathered.at[slot], sends.at[0], receives.at[slot // 2], plane.partner()
        ).wait_recv()
        send(gathered.at[slot], slot, partner_receives.at[slot // 2], plane.partner())
    for at in range(16):
        slot = plane.partner_slot(at // 4, at % 4)
        remote(
            outgoing, gathered.at[slot], sends.at[0], partner_receives.at[at], plane.partner()
        ).wait_recv()
    flat = jnp.concatenate([gathered[i] for i in range(32)], axis=0)
    at = lax.broadcasted_iota(jnp.int32, (128, 512), 0)
    lane = lanes_of((128, 512))
    number = at & 63
    row = (number >> 1) * 16 + (number & 1) * 2 + (at >> 6)
    pieces = []
    for k in range(4):
        chosen = jnp.where(lane == row + 4 * k, 1.0, 0.0).astype(BF16)
        pieces.append(nn(chosen, flat))
    everyone = jnp.concatenate([p[:, :896] for p in pieces], axis=1).astype(BF16)
    target = pieces[0][:64, 896:960]
    logits = nt(everyone[:64], everyone[64:]) * (1.0 / sharpness_divisor)
    weights = jnp.exp(logits)
    odds = weights / jnp.sum(weights, axis=-1, keepdims=True)
    column = lanes_of((64, 64))
    hit = jnp.where(target == column.astype(F32), 1.0, 0.0)
    coefficient = (odds - hit) * (objective_coefficient / sharpness_divisor)
    turned_coefficient = coefficient.T
    line = lax.broadcasted_iota(jnp.int32, (64, 64), 0)
    blank = jnp.zeros((1, 64), F32)
    replica = mine
    chosen_rows = []
    for m in range(4):
        source = turned_coefficient if m % 2 else coefficient
        one = jnp.sum(
            jnp.where(line == replica * 2 + m // 2, source, 0.0), axis=0, keepdims=True
        )
        chosen_rows.append(jnp.concatenate([one, blank] if m % 2 else [blank, one], axis=1))
    exact = jnp.concatenate(chosen_rows, axis=0)
    top = exact.astype(BF16)
    rest = exact - top.astype(F32)
    middle = rest.astype(BF16)
    low = (rest - middle.astype(F32)).astype(BF16)
    embed_grad = nn(top, everyone) + nn(middle, everyone) + nn(low, everyone)
    pooled_grad = embed_grad * scale - pooled * (
        scale * scale * scale * jnp.sum(embed_grad * pooled, axis=-1, keepdims=True)
    )
    gained = pooled_grad * gain
    row_grad = gained * inverse - rows * (
        inverse * inverse * inverse * jnp.mean(gained * rows, axis=-1, keepdims=True)
    )
    for m in range(4):
        last_grad[m] = row_grad[m : m + 1]
    for copy in started:
        copy.wait_send()


def step_kernel(
    lengths, positive, entry, gain, wq_own, wo_own, cosine, sine, final_gain, spread_rows,
    grad_out,
    wq, wo_spaced, wo, hidden, saved, prob, inverses, last_rows, last_grad, embeds, embed_own,
    outbox, grads,
    wq_send, wq_recv, wq_cross, wo_send, wo_recv, wo_cross, e_send, e_recv, e_cross,
    f_send, f_recv, b_send, b_recv, f_turn, b_turn,
):
    me = lax.axis_index("section")
    count = lax.axis_size("section")
    micros = entry.shape[0]
    plane = Plane()
    mine = plane.slot(0, 0)
    barrier, greetings = start_meeting(plane)
    wq[pl.ds(pl.multiple_of(mine * 112, 16), 112)] = wq_own[...]
    wo_spaced[pl.ds(pl.multiple_of(mine * 32, 16), 32)] = jnp.concatenate(
        [wo_own[...], jnp.zeros((4, wo_own.shape[1]), BF16)], axis=0
    )
    pl.semaphore_wait(barrier, greetings)
    gathers = (
        Gather(plane, wq, 112, 64, wq_send, wq_recv, wq_cross),
        Gather(Plane(flipped=True), wo_spaced, 32, 16, wo_send, wo_recv, wo_cross),
    )
    for gather in gathers:
        gather.begin()

    @pl.when(me == 0)
    def _():
        hidden[...] = entry[...]

    for gather in gathers:
        gather.first_near()
    for gather in gathers:
        gather.second_near(0)
    for gather in gathers:
        gather.first_far()
    for first in (-1, 1, 2):
        for gather in gathers:
            gather.second_near(first)
    for gather in gathers:
        for first in (0, -1, 1, 2):
            gather.second_far(first)
    for b in range(4):
        gathers[1].from_partner(b)
        spaced = wo_spaced[256 * b : 256 * (b + 1)]
        wo[224 * b : 224 * (b + 1)] = nn(spread_rows[...], spaced).astype(BF16)
    for b in range(4):
        gathers[0].from_partner(b)
    for gather in gathers:
        gather.drain()

    def hop(m, k):
        low, size = CHUNKS[k]
        return remote(
            outbox.at[m, :, pl.ds(low, size)], hidden.at[m, :, pl.ds(low, size)],
            f_send.at[m, k], f_recv.at[m, k], {"section": lax.rem(me + 1, count)},
        )

    def back_hop(m, k):
        low, size = BACK_CHUNKS[k]
        return remote(
            grad_out.at[m, :, pl.ds(low, size)], grads.at[m, :, pl.ds(low, size)],
            b_send.at[m, k], b_recv.at[m, k], {"section": lax.rem(me + count - 1, count)},
        )

    def take_turn(sending, turn, m):
        @pl.when(jnp.logical_and(sending, plane.core + m > 0))
        def _():
            pl.semaphore_wait(turn, 1)

    def give_turn(sending, turn, m, copies):
        @pl.when(sending)
        def _():
            for k in range(EARLY):
                copies(m, k).wait_send()

        @pl.when(jnp.logical_and(sending, m + plane.core < micros))
        def _():
            pl.semaphore_signal(
                turn, inc=1, device_id=plane.partner(), device_id_type=pl.DeviceIdType.MESH
            )

    def forward(m, carry):
        length = lengths[m]

        def chunk_of(low, size):
            k = [c[0] for c in CHUNKS].index(low)

            @pl.when(me > 0)
            def _():
                hop(m, k).wait_recv()

            return hidden[m, :, low : low + size]

        projected, inverse = project(chunk_of, gain, wq)
        inverses[m] = inverse
        context, kept, probabilities = attend(
            projected, length, cosine[...], sine[...], tpu_roll
        )
        last = is_last(length)
        for k, (low, size) in enumerate(CHUNKS):
            wide = hidden[m, :, low : low + size].astype(F32)
            following = (wide + nn(context, wo[:, low : low + size])).astype(BF16)
            outbox[m, :, low : low + size] = following
            if k == 0:
                take_turn(me < count - 1, f_turn, m)

            @pl.when(me < count - 1)
            def _():
                hop(m, k).start()

            last_rows[m, :, low : low + size] = jnp.sum(
                jnp.where(last, following.astype(F32), 0.0), axis=0, keepdims=True
            )
        saved[m] = kept
        prob[m] = probabilities
        give_turn(me < count - 1, f_turn, m, hop)
        return carry

    lax.fori_loop(0, micros, forward, 0)

    @pl.when(me < count - 1)
    def _():
        for m in range(micros):
            for k in range(EARLY, len(CHUNKS)):
                hop(m, k).wait_send()

    @pl.when(me == count - 1)
    def _():
        contrast(plane, last_rows, final_gain, positive, embeds, embed_own, e_send, e_recv,
                 e_cross, last_grad)
        for m in range(micros):
            grads[m] = jnp.where(is_last(lengths[m]), last_grad[m], 0.0).astype(BF16)

    def backward(m, carry):
        def chunk_of(low, size):
            k = [c[0] for c in BACK_CHUNKS].index(low)

            @pl.when(me < count - 1)
            def _():
                back_hop(m, k).wait_recv()

            return grads[m, :, low : low + size]

        context_grad = context_gradient(chunk_of, wo)
        projected_grad, product = attend_back(
            context_grad, saved[m], prob[m], cosine[...], sine[...], tpu_roll
        )
        inverse = inverses[m]
        lean = inverse * inverse * product * (1.0 / 3584)
        for k, (low, size) in enumerate(BACK_CHUNKS):
            normed_grad = nt(projected_grad, wq[low : low + size, :])
            grad_out[m, :, low : low + size] = (
                grads[m, :, low : low + size].astype(F32)
                + normed_grad * gain[:, low : low + size] * inverse
                - hidden[m, :, low : low + size].astype(F32) * lean
            ).astype(BF16)
            if k == 0:
                take_turn(me > 0, b_turn, m)

            @pl.when(me > 0)
            def _():
                back_hop(m, k).start()

        give_turn(me > 0, b_turn, m, back_hop)
        return carry

    lax.fori_loop(0, micros, backward, 0)

    @pl.when(me > 0)
    def _():
        for m in range(micros):
            for k in range(EARLY, len(BACK_CHUNKS)):
                back_hop(m, k).wait_send()


def whole():
    return pl.BlockSpec(memory_space=pltpu.VMEM)


def turning(length):
    half = HEAD_DIM // 2
    frequency = rope_base ** (-np.arange(half, dtype=np.float32) * np.float32(2.0 / HEAD_DIM))
    angles = np.arange(length, dtype=np.float32)[:, None] * frequency[None, :].astype(np.float32)
    cosine, sine = np.cos(angles), np.sin(angles)
    return (
        np.concatenate([cosine] * 4, axis=1).astype(np.float32),
        np.concatenate([-sine, sine] * 2, axis=1).astype(np.float32),
    )


def per_device(entry, norm_gain, w_qkv, w_out, final_gain, lengths, positive):
    width = entry.shape[1]
    seqs = lengths.shape[0]
    length = entry.shape[0] // seqs
    cosine, sine = turning(length)
    packed = np.arange(224)
    spread_rows = np.arange(256)[None, :] == (packed // 28 * 32 + packed % 28)[:, None]
    block = (seqs, length, width)
    dma = pltpu.SemaphoreType.DMA
    args = (
        lengths, positive,
        entry.reshape(block), norm_gain, w_qkv[0], w_out[0],
        jnp.asarray(cosine), jnp.asarray(sine), final_gain,
        jnp.asarray(spread_rows.astype(np.float32), dtype=BF16),
    )
    small = pl.BlockSpec(memory_space=pltpu.SMEM)
    chunks, back_chunks = len(CHUNKS), len(BACK_CHUNKS)
    grads = pl.pallas_call(
        step_kernel,
        out_shape=jax.ShapeDtypeStruct(block, BF16),
        in_specs=[small] * 2 + [whole()] * (len(args) - 2),
        out_specs=whole(),
        scratch_shapes=[
            pltpu.VMEM((width, 1152), BF16),
            pltpu.VMEM((1024, width), BF16),
            pltpu.VMEM((896, width), BF16),
            pltpu.VMEM(block, BF16),
            pltpu.VMEM((seqs, length, 1152), BF16),
            pltpu.VMEM((seqs, PAIRS * length, 2 * length), BF16),
            pltpu.VMEM((seqs, length, 1), F32),
            pltpu.VMEM((seqs, 1, width), F32),
            pltpu.VMEM((seqs, 1, width), F32),
            pltpu.VMEM((32, 16, 1024), BF16),
            pltpu.VMEM((16, 1024), BF16),
            pltpu.VMEM(block, BF16),
            pltpu.VMEM(block, BF16),
            dma((GATHER_SENDS,)), dma((16, 2)), dma((16,)),
            dma((GATHER_SENDS,)), dma((16, 2)), dma((16,)),
            dma((31,)), dma((16,)), dma((16,)),
            dma((seqs, chunks)), dma((seqs, chunks)),
            dma((seqs, back_chunks)), dma((seqs, back_chunks)),
            pltpu.SemaphoreType.REGULAR, pltpu.SemaphoreType.REGULAR,
        ],
        compiler_params=pltpu.CompilerParams(
            collective_id=0, has_side_effects=True, vmem_limit_bytes=64000 * 1024
        ),
    )(*args)
    return grads.reshape(1, seqs * length, width)


def solution(mesh):
    finer = Mesh(
        mesh.devices.reshape(mesh.shape["section"], 4, 4, 2), ("section", "dp_0", "dp_1", "dp_2")
    )
    in_specs = (
        P(DP, None),
        P("section", None),
        P("section", DP, None),
        P("section", DP, None),
        P(),
        P(DP),
        P(DP),
    )
    return jax.shard_map(
        per_device, mesh=finer, in_specs=in_specs, out_specs=P("section", DP, None),
        check_vma=False,
    )
```

```python
import jax
import jax.numpy as jnp
import numpy as np
from jax import lax
from jax.experimental import pallas as pl
from jax.experimental.pallas import tpu as pltpu
from jax.sharding import Mesh
from jax.sharding import PartitionSpec as P

HEAD_DIM = 64
GROUP_HEADS = 7
KV_GROUPS = 2
DP = ("dp_0", "dp_1", "dp_2")

rope_base = 1000000.0
norm_eps = 1e-06
sharpness_divisor = 0.05
objective_coefficient = 256.0

LENGTH = 48
EARLY = 2
PAIRS = 7
F32 = jnp.float32
BF16 = jnp.bfloat16


def nn(a, b):
    return lax.dot_general(a, b, (((1,), (0,)), ((), ())), preferred_element_type=F32)


def nt(a, b):
    return lax.dot_general(a, b, (((1,), (1,)), ((), ())), preferred_element_type=F32)


def tn(a, b):
    return lax.dot_general(a, b, (((0,), (0,)), ((), ())), preferred_element_type=F32)


def lanes_of(shape):
    return lax.broadcasted_iota(jnp.int32, shape, 1)


def turned(block, cosine, sine, roll):
    lane = lanes_of(block.shape)
    swapped = jnp.where(lane % 64 < 32, roll(block, 96), roll(block, 32))
    return block * cosine + swapped * sine


def paired(rows, roll):
    lane = lanes_of(rows.shape)
    other = roll(rows, 64)
    zero = jnp.zeros_like(rows)
    low = lane < 64
    first = jnp.where(low, rows, zero)
    second = jnp.where(low, zero, rows)
    return tuple(
        jnp.concatenate(two, axis=0).astype(BF16)
        for two in (
            (first, jnp.where(low, zero, other)),
            (first, second),
            (jnp.where(low, other, zero), second),
        )
    )


SPANS = ((0, 3), (3, 4), (4, 7))


def stacked(blocks, span):
    chosen = blocks[span[0] : span[1]]
    return chosen[0] if len(chosen) == 1 else jnp.concatenate(chosen, axis=0)


CHUNKS = ((0, 512), (512, 2048), (2560, 1024))
BACK_CHUNKS = ((0, 512), (512, 1024), (1536, 1280), (2816, 768))


def live_lanes(shape, length):
    lane = lanes_of(shape)
    return jnp.where(lane < LENGTH, lane, lane - LENGTH) < length


def is_last(length):
    return lax.broadcasted_iota(jnp.int32, (LENGTH, 1), 0) == length - 1


def project(chunk_of, gain, wq):
    squares, projected = 0.0, 0.0
    for low, size in CHUNKS:
        wide = chunk_of(low, size).astype(F32)
        squares = squares + jnp.sum(wide * wide, axis=-1, keepdims=True)
        gained = (wide * gain[:, low : low + size]).astype(BF16)
        projected = projected + nn(gained, wq[low : low + size, :])
    inverse = lax.rsqrt(squares * (1.0 / 3584) + norm_eps)
    return projected * inverse, inverse


def attend(projected, length, cosine, sine, roll):
    blocks = [projected[:, 128 * b : 128 * (b + 1)] for b in range(9)]
    turned_blocks = [turned(b, cosine, sine, roll) for b in blocks[:8]]
    queries = [b.astype(BF16) for b in turned_blocks[:PAIRS]]
    keys = turned_blocks[PAIRS].astype(BF16)
    values = blocks[8].astype(BF16)
    key_forms = paired(keys.astype(F32), roll)
    value_forms = paired(values.astype(F32), roll)
    probabilities = []
    context = []
    for span, key_form, value_form in zip(SPANS, key_forms, value_forms):
        scores = nt(stacked(queries, span), key_form) * HEAD_DIM ** (-0.5)
        weights = jnp.where(live_lanes(scores.shape, length), jnp.exp(scores), 0.0)
        low = lanes_of(weights.shape) < LENGTH
        sum_low = jnp.sum(jnp.where(low, weights, 0.0), axis=-1, keepdims=True)
        sum_high = jnp.sum(jnp.where(low, 0.0, weights), axis=-1, keepdims=True)
        probability = (weights / jnp.where(low, sum_low, sum_high)).astype(BF16)
        probabilities.append(probability)
        result = nn(probability, value_form).astype(BF16)
        for i in range(span[1] - span[0]):
            context.append(result[LENGTH * i : LENGTH * (i + 1)])
    saved = jnp.concatenate(queries + [keys, values], axis=1)
    return jnp.concatenate(context, axis=1), saved, jnp.concatenate(probabilities, axis=0)


def context_gradient(chunk_of, wo):
    total = 0.0
    for low, size in BACK_CHUNKS:
        total = total + nt(chunk_of(low, size), wo[:, low : low + size])
    return total.astype(BF16)


def forms_of(saved, roll):
    return (
        paired(saved[:, 896:1024].astype(F32), roll),
        paired(saved[:, 1024:1152].astype(F32), roll),
    )


def attend_back(context_grad, saved, forms, probabilities, cosine, sine, roll):
    context_grads = [context_grad[:, 128 * b : 128 * (b + 1)] for b in range(PAIRS)]
    queries = [saved[:, 128 * b : 128 * (b + 1)] for b in range(PAIRS)]
    key_forms, value_forms = forms
    query_grads = []
    key_parts = []
    value_parts = []
    for span, key_form, value_form in zip(SPANS, key_forms, value_forms):
        chosen = stacked(context_grads, span)
        probability = probabilities[LENGTH * span[0] : LENGTH * span[1]]
        wide_p = probability.astype(F32)
        prob_grad = nt(chosen, value_form)
        product = prob_grad * wide_p
        low = lanes_of(product.shape) < LENGTH
        sum_low = jnp.sum(jnp.where(low, product, 0.0), axis=-1, keepdims=True)
        sum_high = jnp.sum(jnp.where(low, 0.0, product), axis=-1, keepdims=True)
        score_grad = (
            wide_p * (prob_grad - jnp.where(low, sum_low, sum_high)) * HEAD_DIM ** (-0.5)
        ).astype(BF16)
        query_grad = nn(score_grad, key_form)
        for i in range(span[1] - span[0]):
            query_grads.append(query_grad[LENGTH * i : LENGTH * (i + 1)])
        key_parts.append(tn(score_grad, stacked(queries, span)))
        value_parts.append(tn(probability, chosen))

    def folded(parts):
        both, mixed, last = parts
        low_part = both[:LENGTH] + roll(both[LENGTH:], 64) + mixed[:LENGTH]
        high_part = mixed[LENGTH:] + last[LENGTH:] + roll(last[:LENGTH], 64)
        return jnp.where(lanes_of(low_part.shape) < 64, low_part, high_part)

    grads = [
        block.astype(BF16).astype(F32)
        for block in query_grads + [folded(key_parts), folded(value_parts)]
    ]
    product = 0.0
    for b, block in enumerate(grads):
        product = product + block * saved[:, 128 * b : 128 * (b + 1)].astype(F32)
    turned_back = [turned(block, cosine, -sine, roll).astype(BF16) for block in grads[:8]]
    projected_grad = jnp.concatenate(turned_back + [grads[8].astype(BF16)], axis=1)
    return projected_grad, jnp.sum(product, axis=-1, keepdims=True)


def tpu_roll(x, shift):
    return pltpu.roll(x, shift, axis=1)


def remote(source, target, send, receive, place):
    return pltpu.make_async_remote_copy(
        src_ref=source,
        dst_ref=target,
        send_sem=send,
        recv_sem=receive,
        device_id=place,
        device_id_type=pl.DeviceIdType.MESH,
    )


class Plane:
    def __init__(self, flipped=False):
        self.x = lax.axis_index("dp_0")
        self.y = lax.axis_index("dp_1")
        self.core = lax.axis_index("dp_2")
        self.turned = 1 - self.core if flipped else self.core

    def spot(self, first, second):
        other = 1 - self.turned
        return (
            lax.rem(self.x + first * other + second * self.turned, 4),
            lax.rem(self.y + first * self.turned + second * other, 4),
        )

    def slot(self, first, second, mine=True):
        x, y = self.spot(first % 4, second % 4)
        core = self.core if mine else 1 - self.core
        return (x * 4 + y) * 2 + core

    def device(self, first, second):
        x, y = self.spot(first % 4, second % 4)
        return {"dp_0": x, "dp_1": y}

    def partner_slot(self, x, y):
        return (x * 4 + y) * 2 + (1 - self.core)

    def partner(self):
        return {"dp_2": 1 - self.core}


def start_meeting(plane):
    me = lax.axis_index("section")
    count = lax.axis_size("section")
    barrier = pltpu.get_barrier_semaphore()
    places = [{"section": lax.rem(me + step, count)} for step in (1, count - 1)]
    places.append(plane.partner())
    places += [plane.device(a, b) for a, b in ((1, 0), (3, 0), (0, 1), (0, 3))]
    for place in places:
        pl.semaphore_signal(
            barrier, inc=1, device_id=place, device_id_type=pl.DeviceIdType.MESH
        )
    return barrier, len(places)


class Gather:
    def __init__(self, plane, whole, rows, cut, sends, receives, partner_receives):
        self.plane, self.whole = plane, whole
        self.rows, self.cut = rows, cut
        self.sends, self.receives = sends, receives
        self.partner_receives = partner_receives
        self.started = []

    def part(self, slot, half):
        low, size = ((0, self.rows), (0, self.cut), (self.cut, self.rows - self.cut))[half]
        return self.whole.at[pl.ds(pl.multiple_of(slot * self.rows + low, 16), size)]

    def send(self, slot, half, place, receives=None):
        target = self.part(slot, half)
        receives = self.receives.at[slot // 2, max(half - 1, 0)] if receives is None else receives
        copy = remote(
            target,
            target,
            self.sends.at[len(self.started)],
            receives,
            place,
        )
        copy.start()
        self.started.append(copy)

    def hand_over(self, slot):
        self.send(slot, 0, self.plane.partner(), self.partner_receives.at[slot // 2])

    def arrived(self, slot, half):
        part = self.part(slot, half)
        remote(
            part, part, self.sends.at[0], self.receives.at[slot // 2, max(half - 1, 0)],
            self.plane.partner(),
        ).wait_recv()

    def begin(self):
        plane = self.plane
        slot = plane.slot(0, 0)
        for step in (1, -1):
            self.send(slot, 0, plane.device(step, 0))
            self.send(slot, 0, plane.device(0, step))
        self.hand_over(slot)

    def first_near(self):
        plane = self.plane
        for step, half in ((-1, 1), (1, 2)):
            slot = plane.slot(step, 0)
            self.arrived(slot, 0)
            self.send(slot, half, plane.device(-step, 0))
            self.spread(slot)

    def first_far(self):
        slot = self.plane.slot(2, 0)
        self.arrived(slot, 1)
        self.arrived(slot, 2)
        self.spread(slot)

    def spread(self, slot):
        for step in (1, -1):
            self.send(slot, 0, self.plane.device(0, step))
        self.hand_over(slot)

    def second_near(self, first):
        plane = self.plane
        for step, half in ((-1, 1), (1, 2)):
            slot = plane.slot(first, step)
            self.arrived(slot, 0)
            self.send(slot, half, plane.device(0, -step))
            self.hand_over(slot)

    def second_far(self, first):
        slot = self.plane.slot(first, 2)
        self.arrived(slot, 1)
        self.arrived(slot, 2)
        self.hand_over(slot)

    def from_partner(self, b):
        for at in range(4 * b, 4 * b + 4):
            part = self.part(self.plane.partner_slot(at // 4, at % 4), 0)
            remote(
                part, part, self.sends.at[0], self.partner_receives.at[at],
                self.plane.partner(),
            ).wait_recv()

    def drain(self):
        for copy in self.started:
            copy.wait_send()


GATHER_SENDS = 36


def contrast(plane, last_rows, final_gain, positive, gathered, outgoing, sends, receives,
             partner_receives, last_grad):
    rows = jnp.concatenate([last_rows[m] for m in range(4)], axis=0)
    gain = final_gain[...].reshape(1, -1)
    inverse = lax.rsqrt(jnp.mean(rows * rows, axis=-1, keepdims=True) + norm_eps)
    pooled = rows * inverse * gain
    scale = lax.rsqrt(jnp.sum(pooled * pooled, axis=-1, keepdims=True))
    embedding = pooled * scale
    spot = lax.broadcasted_iota(jnp.int32, (4, 128), 0)
    tail = jnp.where(spot < 2, positive[0], positive[1]).astype(F32)
    packed = jnp.concatenate(
        [
            jnp.concatenate([embedding[:, 896 * k : 896 * (k + 1)], tail], axis=1)
            for k in range(4)
        ],
        axis=0,
    ).astype(BF16)
    outgoing[...] = packed
    mine = plane.slot(0, 0)
    gathered[mine] = packed
    started = []

    def send(source, slot, receive, place):
        copy = remote(source, gathered.at[slot], sends.at[len(started)], receive, place)
        copy.start()
        started.append(copy)

    others = [(a, b) for a in range(4) for b in range(4) if a or b]
    others.sort(key=lambda ab: min(ab[0], 4 - ab[0]) + min(ab[1], 4 - ab[1]))
    for a, b in reversed(others):
        send(outgoing, mine, receives.at[mine // 2], plane.device(a, b))
    send(outgoing, mine, partner_receives.at[mine // 2], plane.partner())
    at = lax.broadcasted_iota(jnp.int32, (128, 512), 0)
    lane = lanes_of((128, 512))
    number = at & 63
    row = (number >> 1) * 16 + (number & 1) * 2 + (at >> 6)
    selections = [jnp.where(lane == row + 4 * k, 1.0, 0.0).astype(BF16) for k in range(4)]
    for a, b in others:
        slot = plane.slot(a, b)
        remote(
            outgoing, gathered.at[slot], sends.at[0], receives.at[slot // 2], plane.partner()
        ).wait_recv()
        send(gathered.at[slot], slot, partner_receives.at[slot // 2], plane.partner())
    for at in range(16):
        slot = plane.partner_slot(at // 4, at % 4)
        remote(
            outgoing, gathered.at[slot], sends.at[0], partner_receives.at[at], plane.partner()
        ).wait_recv()
    flat = jnp.concatenate([gathered[i] for i in range(32)], axis=0)
    pieces = [nn(chosen, flat) for chosen in selections]
    everyone = jnp.concatenate([p[:, :896] for p in pieces], axis=1).astype(BF16)
    target = pieces[0][:64, 896:960]
    logits = nt(everyone[:64], everyone[64:]) * (1.0 / sharpness_divisor)
    weights = jnp.exp(logits)
    odds = weights / jnp.sum(weights, axis=-1, keepdims=True)
    column = lanes_of((64, 64))
    hit = jnp.where(target == column.astype(F32), 1.0, 0.0)
    coefficient = (odds - hit) * (objective_coefficient / sharpness_divisor)
    turned_coefficient = coefficient.T
    line = lax.broadcasted_iota(jnp.int32, (64, 64), 0)
    blank = jnp.zeros((1, 64), F32)
    replica = mine
    chosen_rows = []
    for m in range(4):
        source = turned_coefficient if m % 2 else coefficient
        one = jnp.sum(
            jnp.where(line == replica * 2 + m // 2, source, 0.0), axis=0, keepdims=True
        )
        chosen_rows.append(jnp.concatenate([one, blank] if m % 2 else [blank, one], axis=1))
    exact = jnp.concatenate(chosen_rows, axis=0)
    top = exact.astype(BF16)
    rest = exact - top.astype(F32)
    middle = rest.astype(BF16)
    low = (rest - middle.astype(F32)).astype(BF16)
    parts = nn(jnp.concatenate([top, middle, low], axis=0), everyone)
    embed_grad = parts[0:4] + parts[4:8] + parts[8:12]
    pooled_grad = embed_grad * scale - pooled * (
        scale * scale * scale * jnp.sum(embed_grad * pooled, axis=-1, keepdims=True)
    )
    gained = pooled_grad * gain
    row_grad = gained * inverse - rows * (
        inverse * inverse * inverse * jnp.mean(gained * rows, axis=-1, keepdims=True)
    )
    for m in range(4):
        last_grad[m] = row_grad[m : m + 1]
    for copy in started:
        copy.wait_send()


def step_kernel(
    lengths, positive, entry, gain, wq_own, wo_own, cosine, sine, final_gain,
    grad_out,
    wq, wo_spaced, wo, hidden, saved, prob, inverses, last_rows, last_grad, embeds, embed_own,
    outbox, grads,
    wq_send, wq_recv, wq_cross, wo_send, wo_recv, wo_cross, e_send, e_recv, e_cross,
    f_send, f_recv, b_send, b_recv, f_turn, b_turn, entry_sem,
):
    me = lax.axis_index("section")
    count = lax.axis_size("section")
    micros = entry.shape[0]
    plane = Plane()
    mine = plane.slot(0, 0)
    barrier, greetings = start_meeting(plane)
    wq[pl.ds(pl.multiple_of(mine * 112, 16), 112)] = wq_own[...]
    wo_spaced[pl.ds(pl.multiple_of(mine * 32, 16), 32)] = jnp.concatenate(
        [wo_own[...], jnp.zeros((4, wo_own.shape[1]), BF16)], axis=0
    )
    pl.semaphore_wait(barrier, greetings)
    gathers = (
        Gather(plane, wq, 112, 64, wq_send, wq_recv, wq_cross),
        Gather(Plane(flipped=True), wo_spaced, 32, 16, wo_send, wo_recv, wo_cross),
    )
    for gather in gathers:
        gather.begin()

    @pl.when(me == 0)
    def _():
        copy = pltpu.make_async_copy(entry, hidden, entry_sem)
        copy.start()
        copy.wait()

    for gather in gathers:
        gather.first_near()
    for gather in gathers:
        gather.second_near(0)
    for gather in gathers:
        gather.first_far()
    for first in (-1, 1, 2):
        for gather in gathers:
            gather.second_near(first)
    for gather in gathers:
        for first in (0, -1, 1, 2):
            gather.second_far(first)
    for b in range(4):
        gathers[1].from_partner(b)
        wo[224 * b : 224 * (b + 1)] = jnp.concatenate(
            [wo_spaced[256 * b + 32 * i : 256 * b + 32 * i + 28] for i in range(8)], axis=0
        )
    for b in range(4):
        gathers[0].from_partner(b)
    for gather in gathers:
        gather.drain()

    def hop(m, k):
        low, size = CHUNKS[k]
        return remote(
            outbox.at[m, :, pl.ds(low, size)], hidden.at[m, :, pl.ds(low, size)],
            f_send.at[m, k], f_recv.at[m, k], {"section": lax.rem(me + 1, count)},
        )

    def back_hop(m, k):
        low, size = BACK_CHUNKS[k]
        return remote(
            grad_out.at[m, :, pl.ds(low, size)], grads.at[m, :, pl.ds(low, size)],
            b_send.at[m, k], b_recv.at[m, k], {"section": lax.rem(me + count - 1, count)},
        )

    def take_turn(sending, turn, m):
        @pl.when(jnp.logical_and(sending, plane.core + m > 0))
        def _():
            pl.semaphore_wait(turn, 1)

    def give_turn(sending, turn, m, copies):
        @pl.when(sending)
        def _():
            for k in range(EARLY):
                copies(m, k).wait_send()

        @pl.when(jnp.logical_and(sending, m + plane.core < micros))
        def _():
            pl.semaphore_signal(
                turn, inc=1, device_id=plane.partner(), device_id_type=pl.DeviceIdType.MESH
            )

    def forward(m, carry):
        length = lengths[m]

        def chunk_of(low, size):
            k = [c[0] for c in CHUNKS].index(low)

            @pl.when(me > 0)
            def _():
                hop(m, k).wait_recv()

            return hidden[m, :, low : low + size]

        projected, inverse = project(chunk_of, gain, wq)
        inverses[m] = inverse
        context, kept, probabilities = attend(
            projected, length, cosine[...], sine[...], tpu_roll
        )
        last = is_last(length)
        for k, (low, size) in enumerate(CHUNKS):
            wide = hidden[m, :, low : low + size].astype(F32)
            following = (wide + nn(context, wo[:, low : low + size])).astype(BF16)
            outbox[m, :, low : low + size] = following
            if k == 0:
                take_turn(me < count - 1, f_turn, m)

            @pl.when(me < count - 1)
            def _():
                hop(m, k).start()

            last_rows[m, :, low : low + size] = jnp.sum(
                jnp.where(last, following.astype(F32), 0.0), axis=0, keepdims=True
            )
        saved[m] = kept
        prob[m] = probabilities
        give_turn(me < count - 1, f_turn, m, hop)
        return carry

    lax.fori_loop(0, micros, forward, 0)

    @pl.when(me < count - 1)
    def _():
        for m in range(micros):
            for k in range(EARLY, len(CHUNKS)):
                hop(m, k).wait_send()

    @pl.when(me == count - 1)
    def _():
        contrast(plane, last_rows, final_gain, positive, embeds, embed_own, e_send, e_recv,
                 e_cross, last_grad)

    def backward(m, carry):
        length = lengths[m]

        @pl.when(me == count - 1)
        def _():
            grads[m] = jnp.where(is_last(length), last_grad[m], 0.0).astype(BF16)

        def chunk_of(low, size):
            k = [c[0] for c in BACK_CHUNKS].index(low)

            @pl.when(me < count - 1)
            def _():
                back_hop(m, k).wait_recv()

            return grads[m, :, low : low + size]

        forms = forms_of(saved[m], tpu_roll)
        context_grad = context_gradient(chunk_of, wo)
        projected_grad, product = attend_back(
            context_grad, saved[m], forms, prob[m], cosine[...], sine[...], tpu_roll
        )
        inverse = inverses[m]
        lean = inverse * inverse * product * (1.0 / 3584)
        for k, (low, size) in enumerate(BACK_CHUNKS):
            normed_grad = nt(projected_grad, wq[low : low + size, :])
            grad_out[m, :, low : low + size] = (
                grads[m, :, low : low + size].astype(F32)
                + normed_grad * gain[:, low : low + size] * inverse
                - hidden[m, :, low : low + size].astype(F32) * lean
            ).astype(BF16)
            if k == 0:
                take_turn(me > 0, b_turn, m)

            @pl.when(me > 0)
            def _():
                back_hop(m, k).start()

        give_turn(me > 0, b_turn, m, back_hop)
        return carry

    lax.fori_loop(0, micros, backward, 0)

    @pl.when(me > 0)
    def _():
        for m in range(micros):
            for k in range(EARLY, len(BACK_CHUNKS)):
                back_hop(m, k).wait_send()


def whole():
    return pl.BlockSpec(memory_space=pltpu.VMEM)


def turning(length):
    half = HEAD_DIM // 2
    frequency = rope_base ** (-np.arange(half, dtype=np.float32) * np.float32(2.0 / HEAD_DIM))
    angles = np.arange(length, dtype=np.float32)[:, None] * frequency[None, :].astype(np.float32)
    cosine, sine = np.cos(angles), np.sin(angles)
    return (
        np.concatenate([cosine] * 4, axis=1).astype(np.float32),
        np.concatenate([-sine, sine] * 2, axis=1).astype(np.float32),
    )


def handed_on(source, target, held, come, go):
    pieces = held.shape[0]
    copies_in = [
        pltpu.make_async_copy(source.at[i], held.at[i], come.at[i]) for i in range(pieces)
    ]
    copies_out = [
        pltpu.make_async_copy(held.at[i], target.at[i], go.at[i]) for i in range(pieces)
    ]
    for copy in copies_in:
        copy.start()
    for coming, going in zip(copies_in, copies_out):
        coming.wait()
        going.start()
    for copy in copies_out:
        copy.wait()


def per_device(entry, norm_gain, w_qkv, w_out, final_gain, lengths, positive):
    width = entry.shape[1]
    seqs = lengths.shape[0]
    length = entry.shape[0] // seqs
    cosine, sine = turning(length)
    block = (seqs, length, width)
    dma = pltpu.SemaphoreType.DMA
    args = (
        lengths, positive,
        entry.reshape(block), norm_gain, w_qkv[0], w_out[0],
        jnp.asarray(cosine), jnp.asarray(sine), final_gain,
    )
    small = pl.BlockSpec(memory_space=pltpu.SMEM)
    chunks, back_chunks = len(CHUNKS), len(BACK_CHUNKS)
    grads = pl.pallas_call(
        step_kernel,
        out_shape=jax.ShapeDtypeStruct(block, BF16),
        in_specs=[small] * 2
        + [pl.BlockSpec(memory_space=pl.ANY)]
        + [whole()] * (len(args) - 3),
        out_specs=whole(),
        scratch_shapes=[
            pltpu.VMEM((width, 1152), BF16),
            pltpu.VMEM((1024, width), BF16),
            pltpu.VMEM((896, width), BF16),
            pltpu.VMEM(block, BF16),
            pltpu.VMEM((seqs, length, 1152), BF16),
            pltpu.VMEM((seqs, PAIRS * length, 2 * length), BF16),
            pltpu.VMEM((seqs, length, 1), F32),
            pltpu.VMEM((seqs, 1, width), F32),
            pltpu.VMEM((seqs, 1, width), F32),
            pltpu.VMEM((32, 16, 1024), BF16),
            pltpu.VMEM((16, 1024), BF16),
            pltpu.VMEM(block, BF16),
            pltpu.VMEM(block, BF16),
            dma((GATHER_SENDS,)), dma((16, 2)), dma((16,)),
            dma((GATHER_SENDS,)), dma((16, 2)), dma((16,)),
            dma((31,)), dma((16,)), dma((16,)),
            dma((seqs, chunks)), dma((seqs, chunks)),
            dma((seqs, back_chunks)), dma((seqs, back_chunks)),
            pltpu.SemaphoreType.REGULAR, pltpu.SemaphoreType.REGULAR, dma,
        ],
        compiler_params=pltpu.CompilerParams(
            collective_id=0, has_side_effects=True, vmem_limit_bytes=64000 * 1024
        ),
    )(*args)
    result = pl.pallas_call(
        handed_on,
        out_shape=jax.ShapeDtypeStruct(block, BF16),
        in_specs=[pl.BlockSpec(memory_space=pl.ANY)],
        out_specs=pl.BlockSpec(memory_space=pl.ANY),
        scratch_shapes=[pltpu.VMEM(block, BF16), dma((seqs,)), dma((seqs,))],
    )(grads)
    return result.reshape(1, seqs * length, width)


def solution(mesh):
    finer = Mesh(
        mesh.devices.reshape(mesh.shape["section"], 4, 4, 2), ("section", "dp_0", "dp_1", "dp_2")
    )
    in_specs = (
        P(DP, None),
        P("section", None),
        P("section", DP, None),
        P("section", DP, None),
        P(),
        P(DP),
        P(DP),
    )
    return jax.shard_map(
        per_device, mesh=finer, in_specs=in_specs, out_specs=P("section", DP, None),
        check_vma=False,
    )
```

```python
import jax
import jax.numpy as jnp
import numpy as np
from jax import lax
from jax.experimental import pallas as pl
from jax.experimental.pallas import tpu as pltpu
from jax.sharding import Mesh
from jax.sharding import PartitionSpec as P

HEAD_DIM = 64
GROUP_HEADS = 7
KV_GROUPS = 2
DP = ("dp_0", "dp_1", "dp_2")

rope_base = 1000000.0
norm_eps = 1e-06
sharpness_divisor = 0.05
objective_coefficient = 256.0

LENGTH = 48
EARLY = 2
PAIRS = 7
F32 = jnp.float32
BF16 = jnp.bfloat16


def nn(a, b):
    return lax.dot_general(a, b, (((1,), (0,)), ((), ())), preferred_element_type=F32)


def nt(a, b):
    return lax.dot_general(a, b, (((1,), (1,)), ((), ())), preferred_element_type=F32)


def tn(a, b):
    return lax.dot_general(a, b, (((0,), (0,)), ((), ())), preferred_element_type=F32)


def lanes_of(shape):
    return lax.broadcasted_iota(jnp.int32, shape, 1)


def turned(block, cosine, sine, roll):
    lane = lanes_of(block.shape)
    swapped = jnp.where(lane % 64 < 32, roll(block, 96), roll(block, 32))
    return block * cosine + swapped * sine


def paired(rows, roll):
    lane = lanes_of(rows.shape)
    other = roll(rows, 64)
    zero = jnp.zeros_like(rows)
    low = lane < 64
    first = jnp.where(low, rows, zero)
    second = jnp.where(low, zero, rows)
    return tuple(
        jnp.concatenate(two, axis=0).astype(BF16)
        for two in (
            (first, jnp.where(low, zero, other)),
            (first, second),
            (jnp.where(low, other, zero), second),
        )
    )


SPANS = ((0, 3), (3, 4), (4, 7))


def stacked(blocks, span):
    chosen = blocks[span[0] : span[1]]
    return chosen[0] if len(chosen) == 1 else jnp.concatenate(chosen, axis=0)


CHUNKS = ((0, 512), (512, 2048), (2560, 1024))
BACK_CHUNKS = ((0, 512), (512, 1024), (1536, 1280), (2816, 768))


def live_lanes(shape, length):
    lane = lanes_of(shape)
    return jnp.where(lane < LENGTH, lane, lane - LENGTH) < length


def is_last(length):
    return lax.broadcasted_iota(jnp.int32, (LENGTH, 1), 0) == length - 1


def project(chunk_of, gain, wq):
    squares, projected = 0.0, 0.0
    for low, size in CHUNKS:
        wide = chunk_of(low, size).astype(F32)
        squares = squares + jnp.sum(wide * wide, axis=-1, keepdims=True)
        gained = (wide * gain[:, low : low + size]).astype(BF16)
        projected = projected + nn(gained, wq[low : low + size, :])
    inverse = lax.rsqrt(squares * (1.0 / 3584) + norm_eps)
    return projected * inverse, inverse


def attend(projected, length, cosine, sine, roll):
    blocks = [projected[:, 128 * b : 128 * (b + 1)] for b in range(9)]
    turned_blocks = [turned(b, cosine, sine, roll) for b in blocks[:8]]
    queries = [b.astype(BF16) for b in turned_blocks[:PAIRS]]
    keys = turned_blocks[PAIRS].astype(BF16)
    values = blocks[8].astype(BF16)
    key_forms = paired(keys.astype(F32), roll)
    value_forms = paired(values.astype(F32), roll)
    probabilities = []
    context = []
    for span, key_form, value_form in zip(SPANS, key_forms, value_forms):
        scores = nt(stacked(queries, span), key_form) * HEAD_DIM ** (-0.5)
        weights = jnp.where(live_lanes(scores.shape, length), jnp.exp(scores), 0.0)
        low = lanes_of(weights.shape) < LENGTH
        sum_low = jnp.sum(jnp.where(low, weights, 0.0), axis=-1, keepdims=True)
        sum_high = jnp.sum(jnp.where(low, 0.0, weights), axis=-1, keepdims=True)
        probability = (weights / jnp.where(low, sum_low, sum_high)).astype(BF16)
        probabilities.append(probability)
        result = nn(probability, value_form).astype(BF16)
        for i in range(span[1] - span[0]):
            context.append(result[LENGTH * i : LENGTH * (i + 1)])
    saved = jnp.concatenate(queries + [keys, values], axis=1)
    return jnp.concatenate(context, axis=1), saved, jnp.concatenate(probabilities, axis=0)


def context_gradient(chunk_of, wo):
    total = 0.0
    for low, size in BACK_CHUNKS:
        total = total + nt(chunk_of(low, size), wo[:, low : low + size])
    return total.astype(BF16)


def forms_of(saved, roll):
    return (
        paired(saved[:, 896:1024].astype(F32), roll),
        paired(saved[:, 1024:1152].astype(F32), roll),
    )


def attend_back(context_grad, saved, forms, probabilities, cosine, sine, roll):
    context_grads = [context_grad[:, 128 * b : 128 * (b + 1)] for b in range(PAIRS)]
    queries = [saved[:, 128 * b : 128 * (b + 1)] for b in range(PAIRS)]
    key_forms, value_forms = forms
    query_grads = []
    key_parts = []
    value_parts = []
    for span, key_form, value_form in zip(SPANS, key_forms, value_forms):
        chosen = stacked(context_grads, span)
        probability = probabilities[LENGTH * span[0] : LENGTH * span[1]]
        wide_p = probability.astype(F32)
        prob_grad = nt(chosen, value_form)
        product = prob_grad * wide_p
        low = lanes_of(product.shape) < LENGTH
        sum_low = jnp.sum(jnp.where(low, product, 0.0), axis=-1, keepdims=True)
        sum_high = jnp.sum(jnp.where(low, 0.0, product), axis=-1, keepdims=True)
        score_grad = (
            wide_p * (prob_grad - jnp.where(low, sum_low, sum_high)) * HEAD_DIM ** (-0.5)
        ).astype(BF16)
        query_grad = nn(score_grad, key_form)
        for i in range(span[1] - span[0]):
            query_grads.append(query_grad[LENGTH * i : LENGTH * (i + 1)])
        key_parts.append(tn(score_grad, stacked(queries, span)))
        value_parts.append(tn(probability, chosen))

    def folded(parts):
        both, mixed, last = parts
        low_part = both[:LENGTH] + roll(both[LENGTH:], 64) + mixed[:LENGTH]
        high_part = mixed[LENGTH:] + last[LENGTH:] + roll(last[:LENGTH], 64)
        return jnp.where(lanes_of(low_part.shape) < 64, low_part, high_part)

    grads = [
        block.astype(BF16).astype(F32)
        for block in query_grads + [folded(key_parts), folded(value_parts)]
    ]
    product = 0.0
    for b, block in enumerate(grads):
        product = product + block * saved[:, 128 * b : 128 * (b + 1)].astype(F32)
    turned_back = [turned(block, cosine, -sine, roll).astype(BF16) for block in grads[:8]]
    projected_grad = jnp.concatenate(turned_back + [grads[8].astype(BF16)], axis=1)
    return projected_grad, jnp.sum(product, axis=-1, keepdims=True)


def tpu_roll(x, shift):
    return pltpu.roll(x, shift, axis=1)


def remote(source, target, send, receive, place):
    return pltpu.make_async_remote_copy(
        src_ref=source,
        dst_ref=target,
        send_sem=send,
        recv_sem=receive,
        device_id=place,
        device_id_type=pl.DeviceIdType.MESH,
    )


class Plane:
    def __init__(self, flipped=False):
        self.x = lax.axis_index("dp_0")
        self.y = lax.axis_index("dp_1")
        self.core = lax.axis_index("dp_2")
        self.turned = 1 - self.core if flipped else self.core

    def spot(self, first, second):
        other = 1 - self.turned
        return (
            lax.rem(self.x + first * other + second * self.turned, 4),
            lax.rem(self.y + first * self.turned + second * other, 4),
        )

    def slot(self, first, second, mine=True):
        x, y = self.spot(first % 4, second % 4)
        core = self.core if mine else 1 - self.core
        return (x * 4 + y) * 2 + core

    def device(self, first, second):
        x, y = self.spot(first % 4, second % 4)
        return {"dp_0": x, "dp_1": y}

    def partner_slot(self, x, y):
        return (x * 4 + y) * 2 + (1 - self.core)

    def partner(self):
        return {"dp_2": 1 - self.core}


def start_meeting(plane):
    me = lax.axis_index("section")
    count = lax.axis_size("section")
    barrier = pltpu.get_barrier_semaphore()
    places = [{"section": lax.rem(me + step, count)} for step in (1, count - 1)]
    places.append(plane.partner())
    places += [plane.device(a, b) for a, b in ((1, 0), (3, 0), (0, 1), (0, 3))]
    for place in places:
        pl.semaphore_signal(
            barrier, inc=1, device_id=place, device_id_type=pl.DeviceIdType.MESH
        )
    return barrier, len(places)


class Gather:
    def __init__(self, plane, whole, rows, cut, sends, receives, partner_receives):
        self.plane, self.whole = plane, whole
        self.rows, self.cut = rows, cut
        self.sends, self.receives = sends, receives
        self.partner_receives = partner_receives
        self.started = []

    def part(self, slot, half):
        low, size = ((0, self.rows), (0, self.cut), (self.cut, self.rows - self.cut))[half]
        return self.whole.at[pl.ds(pl.multiple_of(slot * self.rows + low, 16), size)]

    def send(self, slot, half, place, receives=None):
        target = self.part(slot, half)
        receives = self.receives.at[slot // 2, max(half - 1, 0)] if receives is None else receives
        copy = remote(
            target,
            target,
            self.sends.at[len(self.started)],
            receives,
            place,
        )
        copy.start()
        self.started.append(copy)

    def hand_over(self, slot):
        self.send(slot, 0, self.plane.partner(), self.partner_receives.at[slot // 2])

    def arrived(self, slot, half):
        part = self.part(slot, half)
        remote(
            part, part, self.sends.at[0], self.receives.at[slot // 2, max(half - 1, 0)],
            self.plane.partner(),
        ).wait_recv()

    def begin(self):
        plane = self.plane
        slot = plane.slot(0, 0)
        for step in (1, -1):
            self.send(slot, 0, plane.device(step, 0))
            self.send(slot, 0, plane.device(0, step))
        self.hand_over(slot)

    def first_near(self):
        plane = self.plane
        for step, half in ((-1, 1), (1, 2)):
            slot = plane.slot(step, 0)
            self.arrived(slot, 0)
            self.send(slot, half, plane.device(-step, 0))
            self.spread(slot)

    def first_far(self):
        slot = self.plane.slot(2, 0)
        self.arrived(slot, 1)
        self.arrived(slot, 2)
        self.spread(slot)

    def spread(self, slot):
        for step in (1, -1):
            self.send(slot, 0, self.plane.device(0, step))
        self.hand_over(slot)

    def second_near(self, first):
        plane = self.plane
        for step, half in ((-1, 1), (1, 2)):
            slot = plane.slot(first, step)
            self.arrived(slot, 0)
            self.send(slot, half, plane.device(0, -step))
            self.hand_over(slot)

    def second_far(self, first):
        slot = self.plane.slot(first, 2)
        self.arrived(slot, 1)
        self.arrived(slot, 2)
        self.hand_over(slot)

    def from_partner(self, b):
        for at in range(4 * b, 4 * b + 4):
            part = self.part(self.plane.partner_slot(at // 4, at % 4), 0)
            remote(
                part, part, self.sends.at[0], self.partner_receives.at[at],
                self.plane.partner(),
            ).wait_recv()

    def drain(self):
        for copy in self.started:
            copy.wait_send()


GATHER_SENDS = 36


def contrast(plane, last_rows, final_gain, positive, gathered, outgoing, sends, receives,
             partner_receives, last_grad):
    rows = jnp.concatenate([last_rows[m] for m in range(4)], axis=0)
    gain = final_gain[...].reshape(1, -1)
    inverse = lax.rsqrt(jnp.mean(rows * rows, axis=-1, keepdims=True) + norm_eps)
    pooled = rows * inverse * gain
    scale = lax.rsqrt(jnp.sum(pooled * pooled, axis=-1, keepdims=True))
    embedding = pooled * scale
    spot = lax.broadcasted_iota(jnp.int32, (4, 128), 0)
    tail = jnp.where(spot < 2, positive[0], positive[1]).astype(F32)
    packed = jnp.concatenate(
        [
            jnp.concatenate([embedding[:, 896 * k : 896 * (k + 1)], tail], axis=1)
            for k in range(4)
        ],
        axis=0,
    ).astype(BF16)
    outgoing[...] = packed
    mine = plane.slot(0, 0)
    gathered[mine] = packed
    started = []

    def send(source, slot, receive, place):
        copy = remote(source, gathered.at[slot], sends.at[len(started)], receive, place)
        copy.start()
        started.append(copy)

    others = [(a, b) for a in range(4) for b in range(4) if a or b]
    others.sort(key=lambda ab: min(ab[0], 4 - ab[0]) + min(ab[1], 4 - ab[1]))
    for a, b in reversed(others):
        send(outgoing, mine, receives.at[mine // 2], plane.device(a, b))
    send(outgoing, mine, partner_receives.at[mine // 2], plane.partner())
    at = lax.broadcasted_iota(jnp.int32, (128, 512), 0)
    lane = lanes_of((128, 512))
    number = at & 63
    row = (number >> 1) * 16 + (number & 1) * 2 + (at >> 6)
    selections = [jnp.where(lane == row + 4 * k, 1.0, 0.0).astype(BF16) for k in range(4)]
    for a, b in others:
        slot = plane.slot(a, b)
        remote(
            outgoing, gathered.at[slot], sends.at[0], receives.at[slot // 2], plane.partner()
        ).wait_recv()
        send(gathered.at[slot], slot, partner_receives.at[slot // 2], plane.partner())
    for at in range(16):
        slot = plane.partner_slot(at // 4, at % 4)
        remote(
            outgoing, gathered.at[slot], sends.at[0], partner_receives.at[at], plane.partner()
        ).wait_recv()
    flat = jnp.concatenate([gathered[i] for i in range(32)], axis=0)
    pieces = [nn(chosen, flat) for chosen in selections]
    everyone = jnp.concatenate([p[:, :896] for p in pieces], axis=1).astype(BF16)
    target = pieces[0][:64, 896:960]
    logits = nt(everyone[:64], everyone[64:]) * (1.0 / sharpness_divisor)
    weights = jnp.exp(logits)
    odds = weights / jnp.sum(weights, axis=-1, keepdims=True)
    column = lanes_of((64, 64))
    hit = jnp.where(target == column.astype(F32), 1.0, 0.0)
    coefficient = (odds - hit) * (objective_coefficient / sharpness_divisor)
    turned_coefficient = coefficient.T
    line = lax.broadcasted_iota(jnp.int32, (64, 64), 0)
    blank = jnp.zeros((1, 64), F32)
    replica = mine
    chosen_rows = []
    for m in range(4):
        source = turned_coefficient if m % 2 else coefficient
        one = jnp.sum(
            jnp.where(line == replica * 2 + m // 2, source, 0.0), axis=0, keepdims=True
        )
        chosen_rows.append(jnp.concatenate([one, blank] if m % 2 else [blank, one], axis=1))
    exact = jnp.concatenate(chosen_rows, axis=0)
    top = exact.astype(BF16)
    rest = exact - top.astype(F32)
    middle = rest.astype(BF16)
    low = (rest - middle.astype(F32)).astype(BF16)
    parts = nn(jnp.concatenate([top, middle, low], axis=0), everyone)
    embed_grad = parts[0:4] + parts[4:8] + parts[8:12]
    pooled_grad = embed_grad * scale - pooled * (
        scale * scale * scale * jnp.sum(embed_grad * pooled, axis=-1, keepdims=True)
    )
    gained = pooled_grad * gain
    row_grad = gained * inverse - rows * (
        inverse * inverse * inverse * jnp.mean(gained * rows, axis=-1, keepdims=True)
    )
    for m in range(4):
        last_grad[m] = row_grad[m : m + 1]
    for copy in started:
        copy.wait_send()


def step_kernel(
    lengths, positive, entry, gain, wq_own, wo_own, cosine, sine, final_gain,
    grad_out,
    wq, wo_folded, wo, hidden, saved, prob, inverses, last_rows, last_grad, embeds, embed_own,
    outbox, grads,
    wq_send, wq_recv, wq_cross, wo_send, wo_recv, wo_cross, e_send, e_recv, e_cross,
    f_send, f_recv, b_send, b_recv, f_turn, b_turn, entry_sem,
):
    me = lax.axis_index("section")
    count = lax.axis_size("section")
    micros = entry.shape[0]
    plane = Plane()
    mine = plane.slot(0, 0)
    barrier, greetings = start_meeting(plane)
    wq[pl.ds(pl.multiple_of(mine * 112, 16), 112)] = wq_own[...]
    wo_folded[pl.ds(pl.multiple_of(mine * 112, 16), 112)] = jnp.concatenate(
        [wo_own[:, 896 * k : 896 * (k + 1)] for k in range(4)], axis=0
    )
    pl.semaphore_wait(barrier, greetings)
    gathers = (
        Gather(plane, wq, 112, 64, wq_send, wq_recv, wq_cross),
        Gather(Plane(flipped=True), wo_folded, 112, 64, wo_send, wo_recv, wo_cross),
    )
    for gather in gathers:
        gather.begin()

    @pl.when(me == 0)
    def _():
        copy = pltpu.make_async_copy(entry, hidden, entry_sem)
        copy.start()
        copy.wait()

    for gather in gathers:
        gather.first_near()
    for gather in gathers:
        gather.second_near(0)
    for gather in gathers:
        gather.first_far()
    for first in (-1, 1, 2):
        for gather in gathers:
            gather.second_near(first)
    for gather in gathers:
        for first in (0, -1, 1, 2):
            gather.second_far(first)
    for b in range(4):
        gathers[1].from_partner(b)
        for k in range(4):
            wo[224 * b : 224 * (b + 1), 896 * k : 896 * (k + 1)] = jnp.concatenate(
                [
                    wo_folded[112 * i + 28 * k : 112 * i + 28 * (k + 1)]
                    for i in range(8 * b, 8 * (b + 1))
                ],
                axis=0,
            )
    for b in range(4):
        gathers[0].from_partner(b)
    for gather in gathers:
        gather.drain()

    def hop(m, k):
        low, size = CHUNKS[k]
        return remote(
            outbox.at[m, :, pl.ds(low, size)], hidden.at[m, :, pl.ds(low, size)],
            f_send.at[m, k], f_recv.at[m, k], {"section": lax.rem(me + 1, count)},
        )

    def back_hop(m, k):
        low, size = BACK_CHUNKS[k]
        return remote(
            grad_out.at[m, :, pl.ds(low, size)], grads.at[m, :, pl.ds(low, size)],
            b_send.at[m, k], b_recv.at[m, k], {"section": lax.rem(me + count - 1, count)},
        )

    def take_turn(sending, turn, m):
        @pl.when(jnp.logical_and(sending, plane.core + m > 0))
        def _():
            pl.semaphore_wait(turn, 1)

    def give_turn(sending, turn, m, copies):
        @pl.when(sending)
        def _():
            for k in range(EARLY):
                copies(m, k).wait_send()

        @pl.when(jnp.logical_and(sending, m + plane.core < micros))
        def _():
            pl.semaphore_signal(
                turn, inc=1, device_id=plane.partner(), device_id_type=pl.DeviceIdType.MESH
            )

    def forward(m, carry):
        length = lengths[m]

        def chunk_of(low, size):
            k = [c[0] for c in CHUNKS].index(low)

            @pl.when(me > 0)
            def _():
                hop(m, k).wait_recv()

            return hidden[m, :, low : low + size]

        projected, inverse = project(chunk_of, gain, wq)
        inverses[m] = inverse
        context, kept, probabilities = attend(
            projected, length, cosine[...], sine[...], tpu_roll
        )
        last = is_last(length)
        for k, (low, size) in enumerate(CHUNKS):
            wide = hidden[m, :, low : low + size].astype(F32)
            following = (wide + nn(context, wo[:, low : low + size])).astype(BF16)
            outbox[m, :, low : low + size] = following
            if k == 0:
                take_turn(me < count - 1, f_turn, m)

            @pl.when(me < count - 1)
            def _():
                hop(m, k).start()

            last_rows[m, :, low : low + size] = jnp.sum(
                jnp.where(last, following.astype(F32), 0.0), axis=0, keepdims=True
            )
        saved[m] = kept
        prob[m] = probabilities
        give_turn(me < count - 1, f_turn, m, hop)
        return carry

    lax.fori_loop(0, micros, forward, 0)

    @pl.when(me < count - 1)
    def _():
        for m in range(micros):
            for k in range(EARLY, len(CHUNKS)):
                hop(m, k).wait_send()

    @pl.when(me == count - 1)
    def _():
        contrast(plane, last_rows, final_gain, positive, embeds, embed_own, e_send, e_recv,
                 e_cross, last_grad)

    def backward(m, carry):
        length = lengths[m]

        @pl.when(me == count - 1)
        def _():
            grads[m] = jnp.where(is_last(length), last_grad[m], 0.0).astype(BF16)

        def chunk_of(low, size):
            k = [c[0] for c in BACK_CHUNKS].index(low)

            @pl.when(me < count - 1)
            def _():
                back_hop(m, k).wait_recv()

            return grads[m, :, low : low + size]

        forms = forms_of(saved[m], tpu_roll)
        context_grad = context_gradient(chunk_of, wo)
        projected_grad, product = attend_back(
            context_grad, saved[m], forms, prob[m], cosine[...], sine[...], tpu_roll
        )
        inverse = inverses[m]
        lean = inverse * inverse * product * (1.0 / 3584)
        for k, (low, size) in enumerate(BACK_CHUNKS):
            normed_grad = nt(projected_grad, wq[low : low + size, :])
            grad_out[m, :, low : low + size] = (
                grads[m, :, low : low + size].astype(F32)
                + normed_grad * gain[:, low : low + size] * inverse
                - hidden[m, :, low : low + size].astype(F32) * lean
            ).astype(BF16)
            if k == 0:
                take_turn(me > 0, b_turn, m)

            @pl.when(me > 0)
            def _():
                back_hop(m, k).start()

        give_turn(me > 0, b_turn, m, back_hop)
        return carry

    lax.fori_loop(0, micros, backward, 0)

    @pl.when(me > 0)
    def _():
        for m in range(micros):
            for k in range(EARLY, len(BACK_CHUNKS)):
                back_hop(m, k).wait_send()


def whole():
    return pl.BlockSpec(memory_space=pltpu.VMEM)


def turning(length):
    half = HEAD_DIM // 2
    frequency = rope_base ** (-np.arange(half, dtype=np.float32) * np.float32(2.0 / HEAD_DIM))
    angles = np.arange(length, dtype=np.float32)[:, None] * frequency[None, :].astype(np.float32)
    cosine, sine = np.cos(angles), np.sin(angles)
    return (
        np.concatenate([cosine] * 4, axis=1).astype(np.float32),
        np.concatenate([-sine, sine] * 2, axis=1).astype(np.float32),
    )


def handed_on(source, target, held, come, go):
    pieces = held.shape[0]
    copies_in = [
        pltpu.make_async_copy(source.at[i], held.at[i], come.at[i]) for i in range(pieces)
    ]
    copies_out = [
        pltpu.make_async_copy(held.at[i], target.at[i], go.at[i]) for i in range(pieces)
    ]
    for copy in copies_in:
        copy.start()
    for coming, going in zip(copies_in, copies_out):
        coming.wait()
        going.start()
    for copy in copies_out:
        copy.wait()


def per_device(entry, norm_gain, w_qkv, w_out, final_gain, lengths, positive):
    width = entry.shape[1]
    seqs = lengths.shape[0]
    length = entry.shape[0] // seqs
    cosine, sine = turning(length)
    block = (seqs, length, width)
    dma = pltpu.SemaphoreType.DMA
    args = (
        lengths, positive,
        entry.reshape(block), norm_gain, w_qkv[0], w_out[0],
        jnp.asarray(cosine), jnp.asarray(sine), final_gain,
    )
    small = pl.BlockSpec(memory_space=pltpu.SMEM)
    chunks, back_chunks = len(CHUNKS), len(BACK_CHUNKS)
    grads = pl.pallas_call(
        step_kernel,
        out_shape=jax.ShapeDtypeStruct(block, BF16),
        in_specs=[small] * 2
        + [pl.BlockSpec(memory_space=pl.ANY)]
        + [whole()] * (len(args) - 3),
        out_specs=whole(),
        scratch_shapes=[
            pltpu.VMEM((width, 1152), BF16),
            pltpu.VMEM((3584, 896), BF16),
            pltpu.VMEM((896, width), BF16),
            pltpu.VMEM(block, BF16),
            pltpu.VMEM((seqs, length, 1152), BF16),
            pltpu.VMEM((seqs, PAIRS * length, 2 * length), BF16),
            pltpu.VMEM((seqs, length, 1), F32),
            pltpu.VMEM((seqs, 1, width), F32),
            pltpu.VMEM((seqs, 1, width), F32),
            pltpu.VMEM((32, 16, 1024), BF16),
            pltpu.VMEM((16, 1024), BF16),
            pltpu.VMEM(block, BF16),
            pltpu.VMEM(block, BF16),
            dma((GATHER_SENDS,)), dma((16, 2)), dma((16,)),
            dma((GATHER_SENDS,)), dma((16, 2)), dma((16,)),
            dma((31,)), dma((16,)), dma((16,)),
            dma((seqs, chunks)), dma((seqs, chunks)),
            dma((seqs, back_chunks)), dma((seqs, back_chunks)),
            pltpu.SemaphoreType.REGULAR, pltpu.SemaphoreType.REGULAR, dma,
        ],
        compiler_params=pltpu.CompilerParams(
            collective_id=0, has_side_effects=True, vmem_limit_bytes=64000 * 1024
        ),
    )(*args)
    result = pl.pallas_call(
        handed_on,
        out_shape=jax.ShapeDtypeStruct(block, BF16),
        in_specs=[pl.BlockSpec(memory_space=pl.ANY)],
        out_specs=pl.BlockSpec(memory_space=pl.ANY),
        scratch_shapes=[pltpu.VMEM(block, BF16), dma((seqs,)), dma((seqs,))],
    )(grads)
    return result.reshape(1, seqs * length, width)


def solution(mesh):
    finer = Mesh(
        mesh.devices.reshape(mesh.shape["section"], 4, 4, 2), ("section", "dp_0", "dp_1", "dp_2")
    )
    in_specs = (
        P(DP, None),
        P("section", None),
        P("section", DP, None),
        P("section", DP, None),
        P(),
        P(DP),
        P(DP),
    )
    return jax.shard_map(
        per_device, mesh=finer, in_specs=in_specs, out_specs=P("section", DP, None),
        check_vma=False,
    )
```

```python
import jax
import jax.numpy as jnp
import numpy as np
from jax import lax
from jax.experimental import pallas as pl
from jax.experimental.pallas import tpu as pltpu
from jax.sharding import Mesh
from jax.sharding import PartitionSpec as P

HEAD_DIM = 64
GROUP_HEADS = 7
KV_GROUPS = 2
DP = ("dp_0", "dp_1", "dp_2")

rope_base = 1000000.0
norm_eps = 1e-06
sharpness_divisor = 0.05
objective_coefficient = 256.0

LENGTH = 48
EARLY = 2
PAIRS = 7
F32 = jnp.float32
BF16 = jnp.bfloat16


def nn(a, b):
    return lax.dot_general(a, b, (((1,), (0,)), ((), ())), preferred_element_type=F32)


def nt(a, b):
    return lax.dot_general(a, b, (((1,), (1,)), ((), ())), preferred_element_type=F32)


def tn(a, b):
    return lax.dot_general(a, b, (((0,), (0,)), ((), ())), preferred_element_type=F32)


def lanes_of(shape):
    return lax.broadcasted_iota(jnp.int32, shape, 1)


def turned(block, cosine, sine, roll):
    lane = lanes_of(block.shape)
    swapped = jnp.where(lane % 64 < 32, roll(block, 96), roll(block, 32))
    return block * cosine + swapped * sine


def paired(rows, roll):
    lane = lanes_of(rows.shape)
    other = roll(rows, 64)
    zero = jnp.zeros_like(rows)
    low = lane < 64
    first = jnp.where(low, rows, zero)
    second = jnp.where(low, zero, rows)
    return tuple(
        jnp.concatenate(two, axis=0).astype(BF16)
        for two in (
            (first, jnp.where(low, zero, other)),
            (first, second),
            (jnp.where(low, other, zero), second),
        )
    )


SPANS = ((0, 3), (3, 4), (4, 7))


def stacked(blocks, span):
    chosen = blocks[span[0] : span[1]]
    return chosen[0] if len(chosen) == 1 else jnp.concatenate(chosen, axis=0)


CHUNKS = ((0, 512), (512, 2048), (2560, 1024))
BACK_CHUNKS = ((0, 512), (512, 1024), (1536, 1280), (2816, 768))


def live_lanes(shape, length):
    lane = lanes_of(shape)
    return jnp.where(lane < LENGTH, lane, lane - LENGTH) < length


def is_last(length):
    return lax.broadcasted_iota(jnp.int32, (LENGTH, 1), 0) == length - 1


def project(chunk_of, gain, wq):
    squares, projected = 0.0, 0.0
    for low, size in CHUNKS:
        wide = chunk_of(low, size).astype(F32)
        squares = squares + jnp.sum(wide * wide, axis=-1, keepdims=True)
        gained = (wide * gain[:, low : low + size]).astype(BF16)
        projected = projected + nn(gained, wq[low : low + size, :])
    inverse = lax.rsqrt(squares * (1.0 / 3584) + norm_eps)
    return projected * inverse, inverse


def attend(projected, length, cosine, sine, roll):
    blocks = [projected[:, 128 * b : 128 * (b + 1)] for b in range(9)]
    turned_blocks = [turned(b, cosine, sine, roll) for b in blocks[:8]]
    queries = [b.astype(BF16) for b in turned_blocks[:PAIRS]]
    keys = turned_blocks[PAIRS].astype(BF16)
    values = blocks[8].astype(BF16)
    key_forms = paired(keys.astype(F32), roll)
    value_forms = paired(values.astype(F32), roll)
    probabilities = []
    context = []
    for span, key_form, value_form in zip(SPANS, key_forms, value_forms):
        scores = nt(stacked(queries, span), key_form) * HEAD_DIM ** (-0.5)
        weights = jnp.where(live_lanes(scores.shape, length), jnp.exp(scores), 0.0)
        low = lanes_of(weights.shape) < LENGTH
        sum_low = jnp.sum(jnp.where(low, weights, 0.0), axis=-1, keepdims=True)
        sum_high = jnp.sum(jnp.where(low, 0.0, weights), axis=-1, keepdims=True)
        probability = (weights / jnp.where(low, sum_low, sum_high)).astype(BF16)
        probabilities.append(probability)
        result = nn(probability, value_form).astype(BF16)
        for i in range(span[1] - span[0]):
            context.append(result[LENGTH * i : LENGTH * (i + 1)])
    saved = jnp.concatenate(queries + [keys, values], axis=1)
    return jnp.concatenate(context, axis=1), saved, jnp.concatenate(probabilities, axis=0)


def context_gradient(chunk_of, wo):
    total = 0.0
    for low, size in BACK_CHUNKS:
        total = total + nt(chunk_of(low, size), wo[:, low : low + size])
    return total.astype(BF16)


def forms_of(saved, roll):
    return (
        paired(saved[:, 896:1024].astype(F32), roll),
        paired(saved[:, 1024:1152].astype(F32), roll),
    )


def attend_back(context_grad, saved, forms, probabilities, cosine, sine, roll):
    context_grads = [context_grad[:, 128 * b : 128 * (b + 1)] for b in range(PAIRS)]
    queries = [saved[:, 128 * b : 128 * (b + 1)] for b in range(PAIRS)]
    key_forms, value_forms = forms
    query_grads = []
    key_parts = []
    value_parts = []
    for span, key_form, value_form in zip(SPANS, key_forms, value_forms):
        chosen = stacked(context_grads, span)
        probability = probabilities[LENGTH * span[0] : LENGTH * span[1]]
        wide_p = probability.astype(F32)
        prob_grad = nt(chosen, value_form)
        product = prob_grad * wide_p
        low = lanes_of(product.shape) < LENGTH
        sum_low = jnp.sum(jnp.where(low, product, 0.0), axis=-1, keepdims=True)
        sum_high = jnp.sum(jnp.where(low, 0.0, product), axis=-1, keepdims=True)
        score_grad = (
            wide_p * (prob_grad - jnp.where(low, sum_low, sum_high)) * HEAD_DIM ** (-0.5)
        ).astype(BF16)
        query_grad = nn(score_grad, key_form)
        for i in range(span[1] - span[0]):
            query_grads.append(query_grad[LENGTH * i : LENGTH * (i + 1)])
        key_parts.append(tn(score_grad, stacked(queries, span)))
        value_parts.append(tn(probability, chosen))

    def folded(parts):
        both, mixed, last = parts
        low_part = both[:LENGTH] + roll(both[LENGTH:], 64) + mixed[:LENGTH]
        high_part = mixed[LENGTH:] + last[LENGTH:] + roll(last[:LENGTH], 64)
        return jnp.where(lanes_of(low_part.shape) < 64, low_part, high_part)

    grads = [
        block.astype(BF16).astype(F32)
        for block in query_grads + [folded(key_parts), folded(value_parts)]
    ]
    product = 0.0
    for b, block in enumerate(grads):
        product = product + block * saved[:, 128 * b : 128 * (b + 1)].astype(F32)
    turned_back = [turned(block, cosine, -sine, roll).astype(BF16) for block in grads[:8]]
    projected_grad = jnp.concatenate(turned_back + [grads[8].astype(BF16)], axis=1)
    return projected_grad, jnp.sum(product, axis=-1, keepdims=True)


def tpu_roll(x, shift):
    return pltpu.roll(x, shift, axis=1)


def remote(source, target, send, receive, place):
    return pltpu.make_async_remote_copy(
        src_ref=source,
        dst_ref=target,
        send_sem=send,
        recv_sem=receive,
        device_id=place,
        device_id_type=pl.DeviceIdType.MESH,
    )


class Plane:
    def __init__(self, flipped=False):
        self.x = lax.axis_index("dp_0")
        self.y = lax.axis_index("dp_1")
        self.core = lax.axis_index("dp_2")
        self.turned = 1 - self.core if flipped else self.core

    def spot(self, first, second):
        other = 1 - self.turned
        return (
            lax.rem(self.x + first * other + second * self.turned, 4),
            lax.rem(self.y + first * self.turned + second * other, 4),
        )

    def slot(self, first, second, mine=True):
        x, y = self.spot(first % 4, second % 4)
        core = self.core if mine else 1 - self.core
        return (x * 4 + y) * 2 + core

    def device(self, first, second):
        x, y = self.spot(first % 4, second % 4)
        return {"dp_0": x, "dp_1": y}

    def partner_slot(self, x, y):
        return (x * 4 + y) * 2 + (1 - self.core)

    def partner(self):
        return {"dp_2": 1 - self.core}


def start_meeting(plane):
    me = lax.axis_index("section")
    count = lax.axis_size("section")
    barrier = pltpu.get_barrier_semaphore()
    places = [{"section": lax.rem(me + step, count)} for step in (1, count - 1)]
    places.append(plane.partner())
    places += [plane.device(a, b) for a, b in ((1, 0), (3, 0), (0, 1), (0, 3))]
    for place in places:
        pl.semaphore_signal(
            barrier, inc=1, device_id=place, device_id_type=pl.DeviceIdType.MESH
        )
    return barrier, len(places)


class Gather:
    def __init__(self, plane, whole, rows, cut, sends, receives, partner_receives):
        self.plane, self.whole = plane, whole
        self.rows, self.cut = rows, cut
        self.sends, self.receives = sends, receives
        self.partner_receives = partner_receives
        self.started = []

    def part(self, slot, half):
        low, size = ((0, self.rows), (0, self.cut), (self.cut, self.rows - self.cut))[half]
        return self.whole.at[pl.ds(pl.multiple_of(slot * self.rows + low, 16), size)]

    def send(self, slot, half, place, receives=None):
        target = self.part(slot, half)
        receives = self.receives.at[slot // 2, max(half - 1, 0)] if receives is None else receives
        copy = remote(
            target,
            target,
            self.sends.at[len(self.started)],
            receives,
            place,
        )
        copy.start()
        self.started.append(copy)

    def hand_over(self, slot):
        self.send(slot, 0, self.plane.partner(), self.partner_receives.at[slot // 2])

    def arrived(self, slot, half):
        part = self.part(slot, half)
        remote(
            part, part, self.sends.at[0], self.receives.at[slot // 2, max(half - 1, 0)],
            self.plane.partner(),
        ).wait_recv()

    def begin(self):
        plane = self.plane
        slot = plane.slot(0, 0)
        for step in (1, -1):
            self.send(slot, 0, plane.device(step, 0))
            self.send(slot, 0, plane.device(0, step))
        self.hand_over(slot)

    def first_near(self):
        plane = self.plane
        for step, half in ((-1, 1), (1, 2)):
            slot = plane.slot(step, 0)
            self.arrived(slot, 0)
            self.send(slot, half, plane.device(-step, 0))
            self.spread(slot)

    def first_far(self):
        slot = self.plane.slot(2, 0)
        self.arrived(slot, 1)
        self.arrived(slot, 2)
        self.spread(slot)

    def spread(self, slot):
        for step in (1, -1):
            self.send(slot, 0, self.plane.device(0, step))
        self.hand_over(slot)

    def second_near(self, first):
        plane = self.plane
        for step, half in ((-1, 1), (1, 2)):
            slot = plane.slot(first, step)
            self.arrived(slot, 0)
            self.send(slot, half, plane.device(0, -step))
            self.hand_over(slot)

    def second_far(self, first):
        slot = self.plane.slot(first, 2)
        self.arrived(slot, 1)
        self.arrived(slot, 2)
        self.hand_over(slot)

    def from_partner(self, b):
        for at in range(4 * b, 4 * b + 4):
            part = self.part(self.plane.partner_slot(at // 4, at % 4), 0)
            remote(
                part, part, self.sends.at[0], self.partner_receives.at[at],
                self.plane.partner(),
            ).wait_recv()

    def drain(self):
        for copy in self.started:
            copy.wait_send()


GATHER_SENDS = 36


class Exchange:
    def __init__(self, plane, pair, gathered, outgoing, sends, receives, partner_receives):
        self.plane, self.pair = plane, pair
        self.gathered, self.outgoing = gathered.at[pair], outgoing.at[pair]
        self.sends, self.receives = sends.at[pair], receives.at[pair]
        self.partner_receives = partner_receives.at[pair]
        others = [(a, b) for a in range(4) for b in range(4) if a or b]
        others.sort(key=lambda ab: min(ab[0], 4 - ab[0]) + min(ab[1], 4 - ab[1]))
        self.others = others

    def copy(self, source, slot, at, receive, place):
        return remote(source, self.gathered.at[slot], self.sends.at[at], receive, place)

    def own_copies(self):
        plane, mine = self.plane, self.plane.slot(0, 0)
        found = [
            self.copy(self.outgoing, mine, at, self.receives.at[mine // 2], plane.device(*place))
            for at, place in enumerate(reversed(self.others))
        ]
        found.append(
            self.copy(
                self.outgoing, mine, 15, self.partner_receives.at[mine // 2], plane.partner()
            )
        )
        return found

    def passed_copies(self):
        plane = self.plane
        slots = [plane.slot(*place) for place in self.others]
        return [
            (
                self.copy(self.outgoing, slot, 0, self.receives.at[slot // 2], plane.partner()),
                self.copy(
                    self.gathered.at[slot], slot, 16 + at,
                    self.partner_receives.at[slot // 2], plane.partner(),
                ),
            )
            for at, slot in enumerate(slots)
        ]

    def offer(self, last_rows, gain, positive):
        rows = jnp.concatenate([last_rows[2 * self.pair], last_rows[2 * self.pair + 1]], axis=0)
        inverse = lax.rsqrt(jnp.mean(rows * rows, axis=-1, keepdims=True) + norm_eps)
        pooled = rows * inverse * gain
        embedding = pooled * lax.rsqrt(jnp.sum(pooled * pooled, axis=-1, keepdims=True))
        pieces = [
            embedding[m : m + 1, 512 * k : 512 * (k + 1)] for m in range(2) for k in range(7)
        ]
        spot = lanes_of((2, 512))
        pieces.append(jnp.where(spot >= 0, positive[self.pair], 0).astype(F32))
        packed = jnp.concatenate(pieces, axis=0).astype(BF16)
        self.outgoing[...] = packed
        self.gathered[self.plane.slot(0, 0)] = packed
        for copy in self.own_copies():
            copy.start()

    def pass_on(self):
        for arriving, passing in self.passed_copies():
            arriving.wait_recv()
            passing.start()

    def from_partner(self):
        for at in range(16):
            slot = self.plane.partner_slot(at // 4, at % 4)
            self.copy(
                self.outgoing, slot, 0, self.partner_receives.at[at], self.plane.partner()
            ).wait_recv()

    def drain(self):
        for copy in self.own_copies():
            copy.wait_send()
        for _, passing in self.passed_copies():
            passing.wait_send()


def contrast(plane, exchanges, last_rows, gain, last_grad):
    at = lax.broadcasted_iota(jnp.int32, (480, 512), 0)
    chosen = jnp.where(
        lanes_of((480, 512)) == (at & 31) * 16 + (at >> 5), 1.0, 0.0
    ).astype(BF16)
    for exchange in exchanges:
        exchange.pass_on()
    for exchange in exchanges:
        exchange.from_partner()
    questions, passages, targets = [], [], []
    for exchange in exchanges:
        flat = jnp.concatenate([exchange.gathered[i] for i in range(32)], axis=0)
        found = nn(chosen, flat)
        pieces = [found[32 * k : 32 * (k + 1)] for k in range(15)]
        questions.append(jnp.concatenate(pieces[:7], axis=1))
        passages.append(jnp.concatenate(pieces[7:14], axis=1))
        targets.append(pieces[14][:, :64])
    everyone = jnp.concatenate(questions + passages, axis=0).astype(BF16)
    target = jnp.concatenate(targets, axis=0)
    rows = jnp.concatenate([last_rows[m] for m in range(4)], axis=0)
    inverse = lax.rsqrt(jnp.mean(rows * rows, axis=-1, keepdims=True) + norm_eps)
    pooled = rows * inverse * gain
    scale = lax.rsqrt(jnp.sum(pooled * pooled, axis=-1, keepdims=True))
    logits = nt(everyone[:64], everyone[64:]) * (1.0 / sharpness_divisor)
    weights = jnp.exp(logits)
    odds = weights / jnp.sum(weights, axis=-1, keepdims=True)
    column = lanes_of((64, 64))
    number = (column & 31) * 2 + (column >> 5)
    hit = jnp.where(target == number.astype(F32), 1.0, 0.0)
    coefficient = (odds - hit) * (objective_coefficient / sharpness_divisor)
    turned_coefficient = coefficient.T
    line = lax.broadcasted_iota(jnp.int32, (64, 64), 0)
    blank = jnp.zeros((1, 64), F32)
    replica = plane.slot(0, 0)
    chosen_rows = []
    for m in range(4):
        source = turned_coefficient if m % 2 else coefficient
        one = jnp.sum(
            jnp.where(line == replica + 32 * (m // 2), source, 0.0), axis=0, keepdims=True
        )
        chosen_rows.append(jnp.concatenate([one, blank] if m % 2 else [blank, one], axis=1))
    exact = jnp.concatenate(chosen_rows, axis=0)
    top = exact.astype(BF16)
    rest = exact - top.astype(F32)
    middle = rest.astype(BF16)
    low = (rest - middle.astype(F32)).astype(BF16)
    parts = nn(jnp.concatenate([top, middle, low], axis=0), everyone)
    embed_grad = parts[0:4] + parts[4:8] + parts[8:12]
    pooled_grad = embed_grad * scale - pooled * (
        scale * scale * scale * jnp.sum(embed_grad * pooled, axis=-1, keepdims=True)
    )
    gained = pooled_grad * gain
    row_grad = gained * inverse - rows * (
        inverse * inverse * inverse * jnp.mean(gained * rows, axis=-1, keepdims=True)
    )
    for m in range(4):
        last_grad[m] = row_grad[m : m + 1]
    for exchange in exchanges:
        exchange.drain()


def step_kernel(
    lengths, positive, entry, gain, wq_own, wo_own, cosine, sine, final_gain,
    grad_out,
    wq, wo_folded, wo, hidden, saved, prob, inverses, last_rows, last_grad, embeds, embed_own,
    outbox, grads,
    wq_send, wq_recv, wq_cross, wo_send, wo_recv, wo_cross, e_send, e_recv, e_cross,
    f_send, f_recv, b_send, b_recv, f_turn, b_turn, entry_sem,
):
    me = lax.axis_index("section")
    count = lax.axis_size("section")
    micros = entry.shape[0]
    plane = Plane()
    mine = plane.slot(0, 0)
    barrier, greetings = start_meeting(plane)
    wq[pl.ds(pl.multiple_of(mine * 112, 16), 112)] = wq_own[...]
    wo_folded[pl.ds(pl.multiple_of(mine * 112, 16), 112)] = jnp.concatenate(
        [wo_own[:, 896 * k : 896 * (k + 1)] for k in range(4)], axis=0
    )
    pl.semaphore_wait(barrier, greetings)
    gathers = (
        Gather(plane, wq, 112, 64, wq_send, wq_recv, wq_cross),
        Gather(Plane(flipped=True), wo_folded, 112, 64, wo_send, wo_recv, wo_cross),
    )
    for gather in gathers:
        gather.begin()

    @pl.when(me == 0)
    def _():
        copy = pltpu.make_async_copy(entry, hidden, entry_sem)
        copy.start()
        copy.wait()

    for gather in gathers:
        gather.first_near()
    for gather in gathers:
        gather.second_near(0)
    for gather in gathers:
        gather.first_far()
    for first in (-1, 1, 2):
        for gather in gathers:
            gather.second_near(first)
    for gather in gathers:
        for first in (0, -1, 1, 2):
            gather.second_far(first)
    for b in range(4):
        gathers[1].from_partner(b)
        for k in range(4):
            wo[224 * b : 224 * (b + 1), 896 * k : 896 * (k + 1)] = jnp.concatenate(
                [
                    wo_folded[112 * i + 28 * k : 112 * i + 28 * (k + 1)]
                    for i in range(8 * b, 8 * (b + 1))
                ],
                axis=0,
            )
    for b in range(4):
        gathers[0].from_partner(b)
    for gather in gathers:
        gather.drain()

    def hop(m, k):
        low, size = CHUNKS[k]
        return remote(
            outbox.at[m, :, pl.ds(low, size)], hidden.at[m, :, pl.ds(low, size)],
            f_send.at[m, k], f_recv.at[m, k], {"section": lax.rem(me + 1, count)},
        )

    def back_hop(m, k):
        low, size = BACK_CHUNKS[k]
        return remote(
            grad_out.at[m, :, pl.ds(low, size)], grads.at[m, :, pl.ds(low, size)],
            b_send.at[m, k], b_recv.at[m, k], {"section": lax.rem(me + count - 1, count)},
        )

    def take_turn(sending, turn, m):
        @pl.when(jnp.logical_and(sending, plane.core + m > 0))
        def _():
            pl.semaphore_wait(turn, 1)

    def give_turn(sending, turn, m, copies):
        @pl.when(sending)
        def _():
            for k in range(EARLY):
                copies(m, k).wait_send()

        @pl.when(jnp.logical_and(sending, m + plane.core < micros))
        def _():
            pl.semaphore_signal(
                turn, inc=1, device_id=plane.partner(), device_id_type=pl.DeviceIdType.MESH
            )

    exchanges = [
        Exchange(plane, pair, embeds, embed_own, e_send, e_recv, e_cross) for pair in range(2)
    ]
    pool_gain = final_gain[...].reshape(1, -1)

    def forward(m, carry):
        length = lengths[m]

        def chunk_of(low, size):
            k = [c[0] for c in CHUNKS].index(low)

            @pl.when(me > 0)
            def _():
                hop(m, k).wait_recv()

            return hidden[m, :, low : low + size]

        projected, inverse = project(chunk_of, gain, wq)
        inverses[m] = inverse
        context, kept, probabilities = attend(
            projected, length, cosine[...], sine[...], tpu_roll
        )
        last = is_last(length)
        for k, (low, size) in enumerate(CHUNKS):
            wide = hidden[m, :, low : low + size].astype(F32)
            following = (wide + nn(context, wo[:, low : low + size])).astype(BF16)
            outbox[m, :, low : low + size] = following
            if k == 0:
                take_turn(me < count - 1, f_turn, m)

            @pl.when(me < count - 1)
            def _():
                hop(m, k).start()

            last_rows[m, :, low : low + size] = jnp.sum(
                jnp.where(last, following.astype(F32), 0.0), axis=0, keepdims=True
            )
        saved[m] = kept
        prob[m] = probabilities
        give_turn(me < count - 1, f_turn, m, hop)

        @pl.when(jnp.logical_and(me == count - 1, m == 1))
        def _():
            exchanges[0].offer(last_rows, pool_gain, positive)

        return carry

    lax.fori_loop(0, micros, forward, 0)

    @pl.when(me < count - 1)
    def _():
        for m in range(micros):
            for k in range(EARLY, len(CHUNKS)):
                hop(m, k).wait_send()

    @pl.when(me == count - 1)
    def _():
        exchanges[1].offer(last_rows, pool_gain, positive)
        contrast(plane, exchanges, last_rows, pool_gain, last_grad)

    def backward(m, carry):
        length = lengths[m]

        @pl.when(me == count - 1)
        def _():
            grads[m] = jnp.where(is_last(length), last_grad[m], 0.0).astype(BF16)

        def chunk_of(low, size):
            k = [c[0] for c in BACK_CHUNKS].index(low)

            @pl.when(me < count - 1)
            def _():
                back_hop(m, k).wait_recv()

            return grads[m, :, low : low + size]

        forms = forms_of(saved[m], tpu_roll)
        context_grad = context_gradient(chunk_of, wo)
        projected_grad, product = attend_back(
            context_grad, saved[m], forms, prob[m], cosine[...], sine[...], tpu_roll
        )
        inverse = inverses[m]
        lean = inverse * inverse * product * (1.0 / 3584)
        for k, (low, size) in enumerate(BACK_CHUNKS):
            normed_grad = nt(projected_grad, wq[low : low + size, :])
            grad_out[m, :, low : low + size] = (
                grads[m, :, low : low + size].astype(F32)
                + normed_grad * gain[:, low : low + size] * inverse
                - hidden[m, :, low : low + size].astype(F32) * lean
            ).astype(BF16)
            if k == 0:
                take_turn(me > 0, b_turn, m)

            @pl.when(me > 0)
            def _():
                back_hop(m, k).start()

        give_turn(me > 0, b_turn, m, back_hop)
        return carry

    lax.fori_loop(0, micros, backward, 0)

    @pl.when(me > 0)
    def _():
        for m in range(micros):
            for k in range(EARLY, len(BACK_CHUNKS)):
                back_hop(m, k).wait_send()


def whole():
    return pl.BlockSpec(memory_space=pltpu.VMEM)


def turning(length):
    half = HEAD_DIM // 2
    frequency = rope_base ** (-np.arange(half, dtype=np.float32) * np.float32(2.0 / HEAD_DIM))
    angles = np.arange(length, dtype=np.float32)[:, None] * frequency[None, :].astype(np.float32)
    cosine, sine = np.cos(angles), np.sin(angles)
    return (
        np.concatenate([cosine] * 4, axis=1).astype(np.float32),
        np.concatenate([-sine, sine] * 2, axis=1).astype(np.float32),
    )


def handed_on(source, target, held, come, go):
    pieces = held.shape[0]
    copies_in = [
        pltpu.make_async_copy(source.at[i], held.at[i], come.at[i]) for i in range(pieces)
    ]
    copies_out = [
        pltpu.make_async_copy(held.at[i], target.at[i], go.at[i]) for i in range(pieces)
    ]
    for copy in copies_in:
        copy.start()
    for coming, going in zip(copies_in, copies_out):
        coming.wait()
        going.start()
    for copy in copies_out:
        copy.wait()


def per_device(entry, norm_gain, w_qkv, w_out, final_gain, lengths, positive):
    width = entry.shape[1]
    seqs = lengths.shape[0]
    length = entry.shape[0] // seqs
    cosine, sine = turning(length)
    block = (seqs, length, width)
    dma = pltpu.SemaphoreType.DMA
    args = (
        lengths, positive,
        entry.reshape(block), norm_gain, w_qkv[0], w_out[0],
        jnp.asarray(cosine), jnp.asarray(sine), final_gain,
    )
    small = pl.BlockSpec(memory_space=pltpu.SMEM)
    chunks, back_chunks = len(CHUNKS), len(BACK_CHUNKS)
    grads = pl.pallas_call(
        step_kernel,
        out_shape=jax.ShapeDtypeStruct(block, BF16),
        in_specs=[small] * 2
        + [pl.BlockSpec(memory_space=pl.ANY)]
        + [whole()] * (len(args) - 3),
        out_specs=whole(),
        scratch_shapes=[
            pltpu.VMEM((width, 1152), BF16),
            pltpu.VMEM((3584, 896), BF16),
            pltpu.VMEM((896, width), BF16),
            pltpu.VMEM(block, BF16),
            pltpu.VMEM((seqs, length, 1152), BF16),
            pltpu.VMEM((seqs, PAIRS * length, 2 * length), BF16),
            pltpu.VMEM((seqs, length, 1), F32),
            pltpu.VMEM((seqs, 1, width), F32),
            pltpu.VMEM((seqs, 1, width), F32),
            pltpu.VMEM((2, 32, 16, 512), BF16),
            pltpu.VMEM((2, 16, 512), BF16),
            pltpu.VMEM(block, BF16),
            pltpu.VMEM(block, BF16),
            dma((GATHER_SENDS,)), dma((16, 2)), dma((16,)),
            dma((GATHER_SENDS,)), dma((16, 2)), dma((16,)),
            dma((2, 31)), dma((2, 16)), dma((2, 16)),
            dma((seqs, chunks)), dma((seqs, chunks)),
            dma((seqs, back_chunks)), dma((seqs, back_chunks)),
            pltpu.SemaphoreType.REGULAR, pltpu.SemaphoreType.REGULAR, dma,
        ],
        compiler_params=pltpu.CompilerParams(
            collective_id=0, has_side_effects=True, vmem_limit_bytes=64000 * 1024
        ),
    )(*args)
    result = pl.pallas_call(
        handed_on,
        out_shape=jax.ShapeDtypeStruct(block, BF16),
        in_specs=[pl.BlockSpec(memory_space=pl.ANY)],
        out_specs=pl.BlockSpec(memory_space=pl.ANY),
        scratch_shapes=[pltpu.VMEM(block, BF16), dma((seqs,)), dma((seqs,))],
    )(grads)
    return result.reshape(1, seqs * length, width)


def solution(mesh):
    finer = Mesh(
        mesh.devices.reshape(mesh.shape["section"], 4, 4, 2), ("section", "dp_0", "dp_1", "dp_2")
    )
    in_specs = (
        P(DP, None),
        P("section", None),
        P("section", DP, None),
        P("section", DP, None),
        P(),
        P(DP),
        P(DP),
    )
    return jax.shard_map(
        per_device, mesh=finer, in_specs=in_specs, out_specs=P("section", DP, None),
        check_vma=False,
    )
```

```python
import jax
import jax.numpy as jnp
import numpy as np
from jax import lax
from jax.experimental import pallas as pl
from jax.experimental.pallas import tpu as pltpu
from jax.sharding import Mesh
from jax.sharding import PartitionSpec as P

HEAD_DIM = 64
GROUP_HEADS = 7
KV_GROUPS = 2
DP = ("dp_0", "dp_1", "dp_2")

rope_base = 1000000.0
norm_eps = 1e-06
sharpness_divisor = 0.05
objective_coefficient = 256.0

LENGTH = 48
EARLY = 2
BACK_EARLY = 1
PAIRS = 7
F32 = jnp.float32
BF16 = jnp.bfloat16


def nn(a, b):
    return lax.dot_general(a, b, (((1,), (0,)), ((), ())), preferred_element_type=F32)


def nt(a, b):
    return lax.dot_general(a, b, (((1,), (1,)), ((), ())), preferred_element_type=F32)


def tn(a, b):
    return lax.dot_general(a, b, (((0,), (0,)), ((), ())), preferred_element_type=F32)


def lanes_of(shape):
    return lax.broadcasted_iota(jnp.int32, shape, 1)


def turned(block, cosine, sine, roll):
    lane = lanes_of(block.shape)
    swapped = jnp.where(lane % 64 < 32, roll(block, 96), roll(block, 32))
    return block * cosine + swapped * sine


def paired(rows, roll):
    lane = lanes_of(rows.shape)
    other = roll(rows, 64)
    zero = jnp.zeros_like(rows)
    low = lane < 64
    first = jnp.where(low, rows, zero)
    second = jnp.where(low, zero, rows)
    return tuple(
        jnp.concatenate(two, axis=0).astype(BF16)
        for two in (
            (first, jnp.where(low, zero, other)),
            (first, second),
            (jnp.where(low, other, zero), second),
        )
    )


SPANS = ((0, 3), (3, 4), (4, 7))


def stacked(blocks, span):
    chosen = blocks[span[0] : span[1]]
    return chosen[0] if len(chosen) == 1 else jnp.concatenate(chosen, axis=0)


CHUNKS = ((0, 512), (512, 2048), (2560, 1024))
BACK_CHUNKS = ((0, 512), (512, 1024), (1536, 1280), (2816, 768))


def live_lanes(shape, length):
    lane = lanes_of(shape)
    return jnp.where(lane < LENGTH, lane, lane - LENGTH) < length


def is_last(length):
    return lax.broadcasted_iota(jnp.int32, (LENGTH, 1), 0) == length - 1


def project(chunk_of, gain, wq):
    squares, projected = 0.0, 0.0
    for low, size in CHUNKS:
        wide = chunk_of(low, size).astype(F32)
        squares = squares + jnp.sum(wide * wide, axis=-1, keepdims=True)
        gained = (wide * gain[:, low : low + size]).astype(BF16)
        projected = projected + nn(gained, wq[low : low + size, :])
    inverse = lax.rsqrt(squares * (1.0 / 3584) + norm_eps)
    return projected * inverse, inverse


def attend(projected, length, cosine, sine, roll):
    blocks = [projected[:, 128 * b : 128 * (b + 1)] for b in range(9)]
    turned_blocks = [turned(b, cosine, sine, roll) for b in blocks[:8]]
    queries = [b.astype(BF16) for b in turned_blocks[:PAIRS]]
    keys = turned_blocks[PAIRS].astype(BF16)
    values = blocks[8].astype(BF16)
    key_forms = paired(keys.astype(F32), roll)
    value_forms = paired(values.astype(F32), roll)
    probabilities = []
    context = []
    for span, key_form, value_form in zip(SPANS, key_forms, value_forms):
        scores = nt(stacked(queries, span), key_form) * HEAD_DIM ** (-0.5)
        weights = jnp.where(live_lanes(scores.shape, length), jnp.exp(scores), 0.0)
        low = lanes_of(weights.shape) < LENGTH
        sum_low = jnp.sum(jnp.where(low, weights, 0.0), axis=-1, keepdims=True)
        sum_high = jnp.sum(jnp.where(low, 0.0, weights), axis=-1, keepdims=True)
        probability = (weights / jnp.where(low, sum_low, sum_high)).astype(BF16)
        probabilities.append(probability)
        result = nn(probability, value_form).astype(BF16)
        for i in range(span[1] - span[0]):
            context.append(result[LENGTH * i : LENGTH * (i + 1)])
    saved = jnp.concatenate(queries + [keys, values], axis=1)
    return jnp.concatenate(context, axis=1), saved, jnp.concatenate(probabilities, axis=0)


def context_gradient(chunk_of, wo):
    total = 0.0
    for low, size in BACK_CHUNKS:
        total = total + nt(chunk_of(low, size), wo[:, low : low + size])
    return total.astype(BF16)


def forms_of(saved, roll):
    return (
        paired(saved[:, 896:1024].astype(F32), roll),
        paired(saved[:, 1024:1152].astype(F32), roll),
    )


def attend_back(context_grad, saved, forms, probabilities, cosine, sine, roll):
    context_grads = [context_grad[:, 128 * b : 128 * (b + 1)] for b in range(PAIRS)]
    queries = [saved[:, 128 * b : 128 * (b + 1)] for b in range(PAIRS)]
    key_forms, value_forms = forms
    query_grads = []
    key_parts = []
    value_parts = []
    for span, key_form, value_form in zip(SPANS, key_forms, value_forms):
        chosen = stacked(context_grads, span)
        probability = probabilities[LENGTH * span[0] : LENGTH * span[1]]
        wide_p = probability.astype(F32)
        prob_grad = nt(chosen, value_form)
        product = prob_grad * wide_p
        low = lanes_of(product.shape) < LENGTH
        sum_low = jnp.sum(jnp.where(low, product, 0.0), axis=-1, keepdims=True)
        sum_high = jnp.sum(jnp.where(low, 0.0, product), axis=-1, keepdims=True)
        score_grad = (
            wide_p * (prob_grad - jnp.where(low, sum_low, sum_high)) * HEAD_DIM ** (-0.5)
        ).astype(BF16)
        query_grad = nn(score_grad, key_form)
        for i in range(span[1] - span[0]):
            query_grads.append(query_grad[LENGTH * i : LENGTH * (i + 1)])
        key_parts.append(tn(score_grad, stacked(queries, span)))
        value_parts.append(tn(probability, chosen))

    def folded(parts):
        both, mixed, last = parts
        low_part = both[:LENGTH] + roll(both[LENGTH:], 64) + mixed[:LENGTH]
        high_part = mixed[LENGTH:] + last[LENGTH:] + roll(last[:LENGTH], 64)
        return jnp.where(lanes_of(low_part.shape) < 64, low_part, high_part)

    grads = [
        block.astype(BF16).astype(F32)
        for block in query_grads + [folded(key_parts), folded(value_parts)]
    ]
    product = 0.0
    for b, block in enumerate(grads):
        product = product + block * saved[:, 128 * b : 128 * (b + 1)].astype(F32)
    turned_back = [turned(block, cosine, -sine, roll).astype(BF16) for block in grads[:8]]
    projected_grad = jnp.concatenate(turned_back + [grads[8].astype(BF16)], axis=1)
    return projected_grad, jnp.sum(product, axis=-1, keepdims=True)


def tpu_roll(x, shift):
    return pltpu.roll(x, shift, axis=1)


def remote(source, target, send, receive, place):
    return pltpu.make_async_remote_copy(
        src_ref=source,
        dst_ref=target,
        send_sem=send,
        recv_sem=receive,
        device_id=place,
        device_id_type=pl.DeviceIdType.MESH,
    )


class Plane:
    def __init__(self, flipped=False):
        self.x = lax.axis_index("dp_0")
        self.y = lax.axis_index("dp_1")
        self.core = lax.axis_index("dp_2")
        self.turned = 1 - self.core if flipped else self.core

    def spot(self, first, second):
        other = 1 - self.turned
        return (
            lax.rem(self.x + first * other + second * self.turned, 4),
            lax.rem(self.y + first * self.turned + second * other, 4),
        )

    def slot(self, first, second, mine=True):
        x, y = self.spot(first % 4, second % 4)
        core = self.core if mine else 1 - self.core
        return (x * 4 + y) * 2 + core

    def device(self, first, second):
        x, y = self.spot(first % 4, second % 4)
        return {"dp_0": x, "dp_1": y}

    def partner_slot(self, x, y):
        return (x * 4 + y) * 2 + (1 - self.core)

    def partner(self):
        return {"dp_2": 1 - self.core}


def start_meeting(plane):
    me = lax.axis_index("section")
    count = lax.axis_size("section")
    barrier = pltpu.get_barrier_semaphore()
    places = [{"section": lax.rem(me + step, count)} for step in (1, count - 1)]
    places.append(plane.partner())
    places += [plane.device(a, b) for a, b in ((1, 0), (3, 0), (0, 1), (0, 3))]
    for place in places:
        pl.semaphore_signal(
            barrier, inc=1, device_id=place, device_id_type=pl.DeviceIdType.MESH
        )
    return barrier, len(places)


class Gather:
    def __init__(self, plane, whole, rows, cut, sends, receives, partner_receives):
        self.plane, self.whole = plane, whole
        self.rows, self.cut = rows, cut
        self.sends, self.receives = sends, receives
        self.partner_receives = partner_receives
        self.started = []

    def part(self, slot, half):
        low, size = ((0, self.rows), (0, self.cut), (self.cut, self.rows - self.cut))[half]
        return self.whole.at[pl.ds(pl.multiple_of(slot * self.rows + low, 16), size)]

    def send(self, slot, half, place, receives=None):
        target = self.part(slot, half)
        receives = self.receives.at[slot // 2, max(half - 1, 0)] if receives is None else receives
        copy = remote(
            target,
            target,
            self.sends.at[len(self.started)],
            receives,
            place,
        )
        copy.start()
        self.started.append(copy)

    def hand_over(self, slot):
        self.send(slot, 0, self.plane.partner(), self.partner_receives.at[slot // 2])

    def arrived(self, slot, half):
        part = self.part(slot, half)
        remote(
            part, part, self.sends.at[0], self.receives.at[slot // 2, max(half - 1, 0)],
            self.plane.partner(),
        ).wait_recv()

    def begin(self):
        plane = self.plane
        slot = plane.slot(0, 0)
        for step in (1, -1):
            self.send(slot, 0, plane.device(step, 0))
            self.send(slot, 0, plane.device(0, step))
        self.hand_over(slot)

    def first_near(self):
        plane = self.plane
        for step, half in ((-1, 1), (1, 2)):
            slot = plane.slot(step, 0)
            self.arrived(slot, 0)
            self.send(slot, half, plane.device(-step, 0))
            self.spread(slot)

    def first_far(self):
        slot = self.plane.slot(2, 0)
        self.arrived(slot, 1)
        self.arrived(slot, 2)
        self.spread(slot)

    def spread(self, slot):
        for step in (1, -1):
            self.send(slot, 0, self.plane.device(0, step))
        self.hand_over(slot)

    def second_near(self, first):
        plane = self.plane
        for step, half in ((-1, 1), (1, 2)):
            slot = plane.slot(first, step)
            self.arrived(slot, 0)
            self.send(slot, half, plane.device(0, -step))
            self.hand_over(slot)

    def second_far(self, first):
        slot = self.plane.slot(first, 2)
        self.arrived(slot, 1)
        self.arrived(slot, 2)
        self.hand_over(slot)

    def from_partner(self, b):
        for at in range(4 * b, 4 * b + 4):
            part = self.part(self.plane.partner_slot(at // 4, at % 4), 0)
            remote(
                part, part, self.sends.at[0], self.partner_receives.at[at],
                self.plane.partner(),
            ).wait_recv()

    def drain(self):
        for copy in self.started:
            copy.wait_send()


GATHER_SENDS = 36


def contrast(plane, last_rows, final_gain, positive, gathered, outgoing, sends, receives,
             partner_receives, last_grad):
    rows = jnp.concatenate([last_rows[m] for m in range(4)], axis=0)
    gain = final_gain[...].reshape(1, -1)
    inverse = lax.rsqrt(jnp.mean(rows * rows, axis=-1, keepdims=True) + norm_eps)
    pooled = rows * inverse * gain
    scale = lax.rsqrt(jnp.sum(pooled * pooled, axis=-1, keepdims=True))
    embedding = pooled * scale
    spot = lax.broadcasted_iota(jnp.int32, (4, 128), 0)
    tail = jnp.where(spot < 2, positive[0], positive[1]).astype(F32)
    packed = jnp.concatenate(
        [
            jnp.concatenate([embedding[:, 896 * k : 896 * (k + 1)], tail], axis=1)
            for k in range(4)
        ],
        axis=0,
    ).astype(BF16)
    outgoing[...] = packed
    mine = plane.slot(0, 0)
    gathered[mine] = packed
    started = []

    def send(source, slot, receive, place):
        copy = remote(source, gathered.at[slot], sends.at[len(started)], receive, place)
        copy.start()
        started.append(copy)

    others = [(a, b) for a in range(4) for b in range(4) if a or b]
    others.sort(key=lambda ab: min(ab[0], 4 - ab[0]) + min(ab[1], 4 - ab[1]))
    for a, b in reversed(others):
        send(outgoing, mine, receives.at[mine // 2], plane.device(a, b))
    send(outgoing, mine, partner_receives.at[mine // 2], plane.partner())
    at = lax.broadcasted_iota(jnp.int32, (128, 512), 0)
    lane = lanes_of((128, 512))
    number = at & 63
    row = (number >> 1) * 16 + (number & 1) * 2 + (at >> 6)
    selections = [jnp.where(lane == row + 4 * k, 1.0, 0.0).astype(BF16) for k in range(4)]
    for a, b in others:
        slot = plane.slot(a, b)
        remote(
            outgoing, gathered.at[slot], sends.at[0], receives.at[slot // 2], plane.partner()
        ).wait_recv()
        send(gathered.at[slot], slot, partner_receives.at[slot // 2], plane.partner())
    for at in range(16):
        slot = plane.partner_slot(at // 4, at % 4)
        remote(
            outgoing, gathered.at[slot], sends.at[0], partner_receives.at[at], plane.partner()
        ).wait_recv()
    flat = jnp.concatenate([gathered[i] for i in range(32)], axis=0)
    pieces = [nn(chosen, flat) for chosen in selections]
    everyone = jnp.concatenate([p[:, :896] for p in pieces], axis=1).astype(BF16)
    target = pieces[0][:64, 896:960]
    logits = nt(everyone[:64], everyone[64:]) * (1.0 / sharpness_divisor)
    weights = jnp.exp(logits)
    odds = weights / jnp.sum(weights, axis=-1, keepdims=True)
    column = lanes_of((64, 64))
    hit = jnp.where(target == column.astype(F32), 1.0, 0.0)
    coefficient = (odds - hit) * (objective_coefficient / sharpness_divisor)
    turned_coefficient = coefficient.T
    line = lax.broadcasted_iota(jnp.int32, (64, 64), 0)
    blank = jnp.zeros((1, 64), F32)
    replica = mine
    chosen_rows = []
    for m in range(4):
        source = turned_coefficient if m % 2 else coefficient
        one = jnp.sum(
            jnp.where(line == replica * 2 + m // 2, source, 0.0), axis=0, keepdims=True
        )
        chosen_rows.append(jnp.concatenate([one, blank] if m % 2 else [blank, one], axis=1))
    exact = jnp.concatenate(chosen_rows, axis=0)
    top = exact.astype(BF16)
    rest = exact - top.astype(F32)
    middle = rest.astype(BF16)
    low = (rest - middle.astype(F32)).astype(BF16)
    parts = nn(jnp.concatenate([top, middle, low], axis=0), everyone)
    embed_grad = parts[0:4] + parts[4:8] + parts[8:12]
    pooled_grad = embed_grad * scale - pooled * (
        scale * scale * scale * jnp.sum(embed_grad * pooled, axis=-1, keepdims=True)
    )
    gained = pooled_grad * gain
    row_grad = gained * inverse - rows * (
        inverse * inverse * inverse * jnp.mean(gained * rows, axis=-1, keepdims=True)
    )
    for m in range(4):
        last_grad[m] = row_grad[m : m + 1]
    for copy in started:
        copy.wait_send()


def step_kernel(
    lengths, positive, entry, gain, wq_own, wo_own, cosine, sine, final_gain,
    grad_out,
    wq, wo_folded, wo, hidden, saved, prob, inverses, last_rows, last_grad, embeds, embed_own,
    outbox, grads,
    wq_send, wq_recv, wq_cross, wo_send, wo_recv, wo_cross, e_send, e_recv, e_cross,
    f_send, f_recv, b_send, b_recv, f_turn, b_turn, entry_sem,
):
    me = lax.axis_index("section")
    count = lax.axis_size("section")
    micros = entry.shape[0]
    plane = Plane()
    mine = plane.slot(0, 0)
    barrier, greetings = start_meeting(plane)
    wq[pl.ds(pl.multiple_of(mine * 112, 16), 112)] = wq_own[...]
    wo_folded[pl.ds(pl.multiple_of(mine * 112, 16), 112)] = jnp.concatenate(
        [wo_own[:, 896 * k : 896 * (k + 1)] for k in range(4)], axis=0
    )
    pl.semaphore_wait(barrier, greetings)
    gathers = (
        Gather(plane, wq, 112, 64, wq_send, wq_recv, wq_cross),
        Gather(Plane(flipped=True), wo_folded, 112, 64, wo_send, wo_recv, wo_cross),
    )
    for gather in gathers:
        gather.begin()

    @pl.when(me == 0)
    def _():
        copy = pltpu.make_async_copy(entry, hidden, entry_sem)
        copy.start()
        copy.wait()

    for gather in gathers:
        gather.first_near()
    for gather in gathers:
        gather.second_near(0)
    for gather in gathers:
        gather.first_far()
    for first in (-1, 1, 2):
        for gather in gathers:
            gather.second_near(first)
    for gather in gathers:
        for first in (0, -1, 1, 2):
            gather.second_far(first)
    for b in range(4):
        gathers[1].from_partner(b)
        for k in range(4):
            wo[224 * b : 224 * (b + 1), 896 * k : 896 * (k + 1)] = jnp.concatenate(
                [
                    wo_folded[112 * i + 28 * k : 112 * i + 28 * (k + 1)]
                    for i in range(8 * b, 8 * (b + 1))
                ],
                axis=0,
            )
    for b in range(4):
        gathers[0].from_partner(b)
    for gather in gathers:
        gather.drain()

    def hop(m, k):
        low, size = CHUNKS[k]
        return remote(
            outbox.at[m, :, pl.ds(low, size)], hidden.at[m, :, pl.ds(low, size)],
            f_send.at[m, k], f_recv.at[m, k], {"section": lax.rem(me + 1, count)},
        )

    def back_hop(m, k):
        low, size = BACK_CHUNKS[k]
        return remote(
            grad_out.at[m, :, pl.ds(low, size)], grads.at[m, :, pl.ds(low, size)],
            b_send.at[m, k], b_recv.at[m, k], {"section": lax.rem(me + count - 1, count)},
        )

    def take_turn(sending, turn, m):
        @pl.when(jnp.logical_and(sending, plane.core + m > 0))
        def _():
            pl.semaphore_wait(turn, 1)

    def give_turn(sending, turn, m, copies, early):
        @pl.when(sending)
        def _():
            for k in range(early):
                copies(m, k).wait_send()

        @pl.when(jnp.logical_and(sending, m + plane.core < micros))
        def _():
            pl.semaphore_signal(
                turn, inc=1, device_id=plane.partner(), device_id_type=pl.DeviceIdType.MESH
            )

    def forward(m, carry):
        length = lengths[m]

        def chunk_of(low, size):
            k = [c[0] for c in CHUNKS].index(low)

            @pl.when(me > 0)
            def _():
                hop(m, k).wait_recv()

            return hidden[m, :, low : low + size]

        projected, inverse = project(chunk_of, gain, wq)
        inverses[m] = inverse
        context, kept, probabilities = attend(
            projected, length, cosine[...], sine[...], tpu_roll
        )
        last = is_last(length)
        for k, (low, size) in enumerate(CHUNKS):
            wide = hidden[m, :, low : low + size].astype(F32)
            following = (wide + nn(context, wo[:, low : low + size])).astype(BF16)
            outbox[m, :, low : low + size] = following
            if k == 0:
                take_turn(me < count - 1, f_turn, m)

            @pl.when(me < count - 1)
            def _():
                hop(m, k).start()

            last_rows[m, :, low : low + size] = jnp.sum(
                jnp.where(last, following.astype(F32), 0.0), axis=0, keepdims=True
            )
        saved[m] = kept
        prob[m] = probabilities
        give_turn(me < count - 1, f_turn, m, hop, EARLY)
        return carry

    lax.fori_loop(0, micros, forward, 0)

    @pl.when(me < count - 1)
    def _():
        for m in range(micros):
            for k in range(EARLY, len(CHUNKS)):
                hop(m, k).wait_send()

    @pl.when(me == count - 1)
    def _():
        contrast(plane, last_rows, final_gain, positive, embeds, embed_own, e_send, e_recv,
                 e_cross, last_grad)

    def backward(m, carry):
        length = lengths[m]

        @pl.when(me == count - 1)
        def _():
            grads[m] = jnp.where(is_last(length), last_grad[m], 0.0).astype(BF16)

        def chunk_of(low, size):
            k = [c[0] for c in BACK_CHUNKS].index(low)

            @pl.when(me < count - 1)
            def _():
                back_hop(m, k).wait_recv()

            return grads[m, :, low : low + size]

        forms = forms_of(saved[m], tpu_roll)
        context_grad = context_gradient(chunk_of, wo)
        projected_grad, product = attend_back(
            context_grad, saved[m], forms, prob[m], cosine[...], sine[...], tpu_roll
        )
        inverse = inverses[m]
        lean = inverse * inverse * product * (1.0 / 3584)
        for k, (low, size) in enumerate(BACK_CHUNKS):
            normed_grad = nt(projected_grad, wq[low : low + size, :])
            grad_out[m, :, low : low + size] = (
                grads[m, :, low : low + size].astype(F32)
                + normed_grad * gain[:, low : low + size] * inverse
                - hidden[m, :, low : low + size].astype(F32) * lean
            ).astype(BF16)
            if k == 0:
                take_turn(me > 0, b_turn, m)

            @pl.when(me > 0)
            def _():
                back_hop(m, k).start()

        give_turn(me > 0, b_turn, m, back_hop, BACK_EARLY)
        return carry

    lax.fori_loop(0, micros, backward, 0)

    @pl.when(me > 0)
    def _():
        for m in range(micros):
            for k in range(BACK_EARLY, len(BACK_CHUNKS)):
                back_hop(m, k).wait_send()


def whole():
    return pl.BlockSpec(memory_space=pltpu.VMEM)


def turning(length):
    half = HEAD_DIM // 2
    frequency = rope_base ** (-np.arange(half, dtype=np.float32) * np.float32(2.0 / HEAD_DIM))
    angles = np.arange(length, dtype=np.float32)[:, None] * frequency[None, :].astype(np.float32)
    cosine, sine = np.cos(angles), np.sin(angles)
    return (
        np.concatenate([cosine] * 4, axis=1).astype(np.float32),
        np.concatenate([-sine, sine] * 2, axis=1).astype(np.float32),
    )


def handed_on(source, target, held, come, go):
    pieces = held.shape[0]
    copies_in = [
        pltpu.make_async_copy(source.at[i], held.at[i], come.at[i]) for i in range(pieces)
    ]
    copies_out = [
        pltpu.make_async_copy(held.at[i], target.at[i], go.at[i]) for i in range(pieces)
    ]
    for copy in copies_in:
        copy.start()
    for coming, going in zip(copies_in, copies_out):
        coming.wait()
        going.start()
    for copy in copies_out:
        copy.wait()


def per_device(entry, norm_gain, w_qkv, w_out, final_gain, lengths, positive):
    width = entry.shape[1]
    seqs = lengths.shape[0]
    length = entry.shape[0] // seqs
    cosine, sine = turning(length)
    block = (seqs, length, width)
    dma = pltpu.SemaphoreType.DMA
    args = (
        lengths, positive,
        entry.reshape(block), norm_gain, w_qkv[0], w_out[0],
        jnp.asarray(cosine), jnp.asarray(sine), final_gain,
    )
    small = pl.BlockSpec(memory_space=pltpu.SMEM)
    chunks, back_chunks = len(CHUNKS), len(BACK_CHUNKS)
    grads = pl.pallas_call(
        step_kernel,
        out_shape=jax.ShapeDtypeStruct(block, BF16),
        in_specs=[small] * 2
        + [pl.BlockSpec(memory_space=pl.ANY)]
        + [whole()] * (len(args) - 3),
        out_specs=whole(),
        scratch_shapes=[
            pltpu.VMEM((width, 1152), BF16),
            pltpu.VMEM((3584, 896), BF16),
            pltpu.VMEM((896, width), BF16),
            pltpu.VMEM(block, BF16),
            pltpu.VMEM((seqs, length, 1152), BF16),
            pltpu.VMEM((seqs, PAIRS * length, 2 * length), BF16),
            pltpu.VMEM((seqs, length, 1), F32),
            pltpu.VMEM((seqs, 1, width), F32),
            pltpu.VMEM((seqs, 1, width), F32),
            pltpu.VMEM((32, 16, 1024), BF16),
            pltpu.VMEM((16, 1024), BF16),
            pltpu.VMEM(block, BF16),
            pltpu.VMEM(block, BF16),
            dma((GATHER_SENDS,)), dma((16, 2)), dma((16,)),
            dma((GATHER_SENDS,)), dma((16, 2)), dma((16,)),
            dma((31,)), dma((16,)), dma((16,)),
            dma((seqs, chunks)), dma((seqs, chunks)),
            dma((seqs, back_chunks)), dma((seqs, back_chunks)),
            pltpu.SemaphoreType.REGULAR, pltpu.SemaphoreType.REGULAR, dma,
        ],
        compiler_params=pltpu.CompilerParams(
            collective_id=0, has_side_effects=True, vmem_limit_bytes=64000 * 1024
        ),
    )(*args)
    result = pl.pallas_call(
        handed_on,
        out_shape=jax.ShapeDtypeStruct(block, BF16),
        in_specs=[pl.BlockSpec(memory_space=pl.ANY)],
        out_specs=pl.BlockSpec(memory_space=pl.ANY),
        scratch_shapes=[pltpu.VMEM(block, BF16), dma((seqs,)), dma((seqs,))],
    )(grads)
    return result.reshape(1, seqs * length, width)


def solution(mesh):
    finer = Mesh(
        mesh.devices.reshape(mesh.shape["section"], 4, 4, 2), ("section", "dp_0", "dp_1", "dp_2")
    )
    in_specs = (
        P(DP, None),
        P("section", None),
        P("section", DP, None),
        P("section", DP, None),
        P(),
        P(DP),
        P(DP),
    )
    return jax.shard_map(
        per_device, mesh=finer, in_specs=in_specs, out_specs=P("section", DP, None),
        check_vma=False,
    )
```
